128 devices in a mesh: tp: 16 (over z, y), dp: 8 (over x, core).
Axes of the slice: x: 4, y: 4, z: 4, core: 2. Of those that a mesh axis runs over, the one named last changes fastest.
Arguments:
- h_main: bfloat16 [8, 512, 2048], P('dp')
- h_mtp: bfloat16 [8, 512, 2048], P('dp')
- labels_main: int32 [8, 512], P('dp')
- labels_mtp: int32 [8, 512], P('dp')
- weight_main: float32 [8, 512], P('dp')
- weight_mtp: float32 [8, 512], P('dp')
- gain_final: float32 [2048], replicated
- gain_mtp: float32 [2048], replicated
- w_out: bfloat16 [2048, 102400], P(None, 'tp')
Outputs:
- output 1: float32 [], replicated
- output 2: bfloat16 [8, 512, 2048], P('dp')
- output 3: bfloat16 [8, 512, 2048], P('dp')
- output 4: float32 [2048, 102400], P('dp', 'tp')
- output 5: float32 [2048], replicated
- output 6: float32 [2048], replicated
All inputs are finite; a program needn't handle non-finite values.
Results may differ from the reference program's by a relative error of at most 0.00844116.
Values sent between devices are 32-bit elements.
A program may use at most 1 GiB of HBM per device.

```python
import jax
import jax.numpy as jnp
from jax import lax

BATCH_ALL = 8
SEQ_LEN = 512
D_MODEL = 2048
VOCAB_SIZE = 102400
TP_SHARDS = 16
ROW_BLOCK = 256
SHARD_VOCAB = VOCAB_SIZE // TP_SHARDS
ROWS_ALL = BATCH_ALL * SEQ_LEN
NUM_BLOCKS = ROWS_ALL // ROW_BLOCK
NORM_EPS = 1e-6
MTP_LAMBDA = 0.3
LOGIT_SCALE = 3.0


def setup_inputs(seed: int = 0) -> dict:
    key_list = jax.random.split(jax.random.key(seed), 7)
    h_main = jax.random.normal(key_list[0], (BATCH_ALL, SEQ_LEN, D_MODEL), jnp.float32).astype(jnp.bfloat16)
    h_mtp = jax.random.normal(key_list[1], (BATCH_ALL, SEQ_LEN, D_MODEL), jnp.float32).astype(jnp.bfloat16)
    tokens = jax.random.randint(key_list[2], (BATCH_ALL, SEQ_LEN + 2), 0, VOCAB_SIZE, jnp.int32)
    tokens = tokens.at[0, 1].set(VOCAB_SIZE - 1).at[0, 2].set(0)
    lengths = jax.random.randint(key_list[3], (BATCH_ALL,), SEQ_LEN // 4, SEQ_LEN + 1, jnp.int32)
    lengths = lengths.at[0].set(SEQ_LEN).at[BATCH_ALL - 1].set(SEQ_LEN // 4)
    positions = jnp.arange(SEQ_LEN, dtype=jnp.int32)[None, :]
    weight_main = (positions < lengths[:, None]).astype(jnp.float32)
    weight_mtp = (positions < lengths[:, None] - 1).astype(jnp.float32)
    gain_final = 1.0 + 0.2 * jax.random.normal(key_list[4], (D_MODEL,), jnp.float32)
    gain_mtp = 1.0 + 0.2 * jax.random.normal(key_list[5], (D_MODEL,), jnp.float32)
    w_out = (jax.random.normal(key_list[6], (D_MODEL, VOCAB_SIZE), jnp.float32) * (LOGIT_SCALE * D_MODEL ** -0.5)).astype(jnp.bfloat16)
    return {"h_main": h_main, "h_mtp": h_mtp, "labels_main": tokens[:, 1:SEQ_LEN + 1], "labels_mtp": tokens[:, 2:], "weight_main": weight_main, "weight_mtp": weight_mtp, "gain_final": gain_final, "gain_mtp": gain_mtp, "w_out": w_out}


def norm_apply(x_rows, gain_vec):
    return x_rows * lax.rsqrt(jnp.mean(x_rows * x_rows, axis=-1, keepdims=True) + NORM_EPS) * gain_vec


def reference(h_main, h_mtp, labels_main, labels_mtp, weight_main, weight_mtp, gain_final, gain_mtp, w_out):
    coef_main = 1.0 / jnp.sum(weight_main)
    coef_mtp = MTP_LAMBDA / jnp.sum(weight_mtp)
    x_blocks = jnp.stack([h_main, h_mtp]).astype(jnp.float32).reshape(2 * NUM_BLOCKS, ROW_BLOCK, D_MODEL)
    label_blocks = jnp.stack([labels_main, labels_mtp]).reshape(2 * NUM_BLOCKS, ROW_BLOCK)
    weight_blocks = jnp.stack([weight_main * coef_main, weight_mtp * coef_mtp]).reshape(2 * NUM_BLOCKS, ROW_BLOCK)
    gain_blocks = jnp.repeat(jnp.stack([gain_final, gain_mtp]), NUM_BLOCKS, axis=0)
    w_shards = w_out.reshape(D_MODEL, TP_SHARDS, SHARD_VOCAB).transpose(1, 0, 2)

    def shard_product(operand_pair):
        grad_shard, w_shard = operand_pair
        return jnp.dot(grad_shard, w_shard.T, preferred_element_type=jnp.float32).astype(jnp.bfloat16)

    def block_step(grad_w, block_data):
        x_rows, labels, row_w, gain_vec = block_data
        u_rows = norm_apply(x_rows, gain_vec).astype(jnp.bfloat16)
        logits = jnp.dot(u_rows, w_out, preferred_element_type=jnp.float32)
        row_max = jnp.max(logits, axis=-1, keepdims=True)
        log_norm = row_max + jnp.log(jnp.sum(jnp.exp(logits - row_max), axis=-1, keepdims=True))
        onehot = jax.nn.one_hot(labels, VOCAB_SIZE, dtype=jnp.float32)
        target = jnp.sum(logits * onehot, axis=-1)
        loss_part = jnp.sum(row_w * (log_norm[:, 0] - target))
        grad_z = (row_w[:, None] * (jnp.exp(logits - log_norm) - onehot)).astype(jnp.bfloat16)
        grad_w = grad_w + lax.dot_general(u_rows, grad_z, (((0,), (0,)), ((), ())), preferred_element_type=jnp.float32)
        grad_split = grad_z.reshape(ROW_BLOCK, TP_SHARDS, SHARD_VOCAB).transpose(1, 0, 2)
        partials = lax.map(shard_product, (grad_split, w_shards))
        grad_u = jnp.sum(partials.astype(jnp.float32), axis=0)
        _, norm_vjp = jax.vjp(norm_apply, x_rows, gain_vec)
        grad_x, grad_gain = norm_vjp(grad_u)
        return grad_w, (loss_part, grad_x.astype(jnp.bfloat16), grad_gain)

    grad_w, outputs = lax.scan(block_step, jnp.zeros((D_MODEL, VOCAB_SIZE), jnp.float32), (x_blocks, label_blocks, weight_blocks, gain_blocks))
    loss_parts, grad_x, grad_gain = outputs
    grad_h = grad_x.reshape(2, BATCH_ALL, SEQ_LEN, D_MODEL)
    gain_grads = grad_gain.reshape(2, NUM_BLOCKS, D_MODEL).sum(axis=1)
    return (jnp.sum(loss_parts), grad_h[0], grad_h[1], grad_w, gain_grads[0], gain_grads[1])
```

```python
import functools

import jax
import jax.numpy as jnp
from jax import lax
from jax.experimental import pallas as pl
from jax.experimental.pallas import tpu as pltpu
from jax.sharding import PartitionSpec as P

NORM_EPS = 1e-6
MTP_LAMBDA = 0.3
MESH = pl.DeviceIdType.MESH
F32 = jnp.float32
BF16 = jnp.bfloat16
ANY = pl.BlockSpec(memory_space=pl.ANY)
VMEM = pl.BlockSpec(memory_space=pltpu.VMEM)


def columns(row, width=128):
    return jnp.broadcast_to(row, (width, row.shape[1])).T


def logits_kernel(n_tp, n_dp, chunk, hm, ht, gain, lab_m, lab_t, wt_m, wt_t, w, z, u_out, st, lpart, h_v, u_v, w_v, z_v, m_v, s_v, t_v,
                  lab_v, send_v, land, wsend, wland, psend, pland, sem_h, sem_u, sem_w, sem_z, ssem, rsem, wssem, wrsem, pssem, prsem):
    seq, depth = hm.shape
    rows, vocab = z.shape
    steps = vocab // chunk
    tp, dp = lax.axis_index("tp"), lax.axis_index("dp")
    partner = lax.rem(dp // 2 + 1, 2) * 2 + (dp // 4) * 4 + lax.rem(dp, 2)

    loads = [pltpu.make_async_copy(src, h_v.at[pl.ds(i * seq, seq), :], sem_h.at[i]) for i, src in enumerate((hm, ht))]

    def w_copy(i, slot):
        return pltpu.make_async_copy(w.at[:, pl.ds(pl.multiple_of(i * chunk, 128), chunk)], w_v.at[slot], sem_w.at[slot])

    def z_copy(i, slot):
        return pltpu.make_async_copy(z_v.at[slot], z.at[:, pl.ds(pl.multiple_of(i * chunk, 128), chunk)], sem_z.at[slot])

    for c in loads:
        c.start()
    w_copy(0, 0).start()
    barrier = pltpu.get_barrier_semaphore()
    for d in range(1, n_tp):
        pl.semaphore_signal(barrier, inc=1, device_id={"tp": lax.rem(tp + d, n_tp), "dp": dp}, device_id_type=MESH)
    for d in range(1, n_dp):
        pl.semaphore_signal(barrier, inc=1, device_id={"tp": tp, "dp": lax.rem(dp + d, n_dp)}, device_id_type=MESH)

    m_v[...] = jnp.full_like(m_v, -jnp.inf)
    s_v[...] = jnp.zeros_like(s_v)
    t_v[...] = jnp.zeros_like(t_v)
    first = (tp * vocab).astype(F32)
    lab_v[pl.ds(0, seq), :] = columns(lab_m[...].astype(F32) - first)
    lab_v[pl.ds(seq, seq), :] = columns(lab_t[...].astype(F32) - first)
    wrow = lax.broadcasted_iota(jnp.int32, (8, 128), 0)
    wsend[...] = jnp.where(wrow == 0, jnp.sum(wt_m[...]), jnp.sum(wt_t[...]))
    wland[dp] = wsend[...]

    for c in loads:
        c.wait()
    for half in range(2):
        g = gain[pl.ds(half, 1), :]

        @pl.loop(0, seq // 128)
        def _(i):
            r = pl.ds(pl.multiple_of(half * seq + i * 128, 128), 128)
            x = h_v[r, :].astype(F32)
            inv = lax.rsqrt(jnp.mean(x * x, axis=-1, keepdims=True) + NORM_EPS)
            u_v[r, :] = (x * inv * g).astype(BF16)

    u_copy = pltpu.make_async_copy(u_v, u_out, sem_u)
    u_copy.start()
    lane = lax.broadcasted_iota(jnp.int32, (rows, 128), 1).astype(F32)

    @pl.loop(0, steps)
    def _(i):
        slot = lax.rem(i, 2)
        w_copy(i, slot).wait()

        @pl.when(i + 1 < steps)
        def _():
            w_copy(i + 1, 1 - slot).start()

        @pl.when(i >= 2)
        def _():
            z_copy(i - 2, slot).wait()

        m, s, t = m_v[...], s_v[...], t_v[...]
        rel = lab_v[...] - (i * chunk).astype(F32)
        for n in range(chunk // 256):
            cols = slice(n * 256, (n + 1) * 256)
            zz = jnp.dot(u_v[...], w_v[slot, :, cols], preferred_element_type=F32)
            z_v[slot, :, cols] = zz
            za, zb = zz[:, :128], zz[:, 128:]
            new = jnp.maximum(m, jnp.maximum(za, zb))
            s = s * jnp.exp(m - new) + (jnp.exp(za - new) + jnp.exp(zb - new))
            t = jnp.where(rel == lane + n * 256, za, t)
            t = jnp.where(rel == lane + (n * 256 + 128), zb, t)
            m = new
        m_v[...], s_v[...], t_v[...] = m, s, t
        z_copy(i, slot).start()

    pl.semaphore_wait(barrier, n_tp + n_dp - 2)
    wcopies = []
    for d in range(1, n_dp):
        peer = lax.rem(dp + d, n_dp)
        c = pltpu.make_async_remote_copy(wsend, wland.at[dp], wssem.at[d], wrsem.at[dp], device_id={"tp": tp, "dp": peer}, device_id_type=MESH)
        c.start()
        wcopies.append(c)
    mt = m_v[...].T
    top = jnp.max(mt, axis=0, keepdims=True)
    total = jnp.sum(s_v[...].T * jnp.exp(mt - top), axis=0, keepdims=True)
    hit = jnp.sum(t_v[...].T, axis=0, keepdims=True)
    srow = lax.broadcasted_iota(jnp.int32, (8, rows), 0)
    mine = jnp.where(srow == 0, top + jnp.log(total), hit)
    send_v[...] = mine
    land[tp] = mine
    copies = []
    for d in range(1, n_tp):
        peer = lax.rem(tp + d, n_tp)
        c = pltpu.make_async_remote_copy(send_v, land.at[tp], ssem.at[d], rsem.at[tp], device_id={"tp": peer, "dp": dp}, device_id_type=MESH)
        c.start()
        copies.append(c)
    for d in range(1, n_dp):
        src = lax.rem(dp + d, n_dp)
        pltpu.make_async_copy(wland.at[src], wland.at[src], wrsem.at[src]).wait()
    sums = wland[0]
    for d in range(1, n_dp):
        sums = sums + wland[d]
    coef_m = 1.0 / sums[0:1, 0:1]
    coef_t = MTP_LAMBDA / sums[1:2, 0:1]
    rw = jnp.concatenate([wt_m[...] * coef_m, wt_t[...] * coef_t], axis=1)
    lab = jnp.concatenate([lab_m[...], lab_t[...]], axis=1).astype(F32)
    for d in range(1, n_tp):
        src = lax.rem(tp + d, n_tp)
        pltpu.make_async_copy(land.at[src], land.at[src], rsem.at[src]).wait()
    top = land[0]
    for d in range(1, n_tp):
        top = jnp.maximum(top, land[d])
    acc = jnp.zeros_like(top)
    hits = jnp.zeros_like(top)
    for d in range(n_tp):
        acc = acc + jnp.exp(land[d] - top)
        hits = hits + land[d]
    lse = (top + jnp.log(acc))[0:1, :]
    hit = hits[1:2, :]
    lpart[...] = jnp.broadcast_to(jnp.sum(rw * (lse - hit)), (8, 128))
    mine = jnp.where(srow == 0, lse, jnp.where(srow == 1, rw, lab - first))
    psend[...] = mine
    st[0] = mine
    c = pltpu.make_async_remote_copy(psend, pland, pssem, prsem, device_id={"tp": tp, "dp": partner}, device_id_type=MESH)
    c.start()
    c.wait()
    st[1] = pland[...]
    for c in wcopies + copies:
        c.wait_send()
    z_copy(steps - 2, (steps - 2) % 2).wait()
    z_copy(steps - 1, (steps - 1) % 2).wait()
    u_copy.wait()


def logits(n_tp, n_dp, hm, ht, gain, lab_m, lab_t, wt_m, wt_t, w):
    seq, depth = hm.shape
    rows, vocab = 2 * seq, w.shape[1]
    chunk = 1280
    dma = pltpu.SemaphoreType.DMA
    return pl.pallas_call(
        functools.partial(logits_kernel, n_tp, n_dp, chunk),
        out_shape=(
            jax.ShapeDtypeStruct((rows, vocab), F32),
            jax.ShapeDtypeStruct((rows, depth), BF16),
            jax.ShapeDtypeStruct((2, 8, rows), F32),
            jax.ShapeDtypeStruct((8, 128), F32),
        ),
        in_specs=[ANY, ANY, VMEM, VMEM, VMEM, VMEM, VMEM, ANY],
        out_specs=(ANY, ANY, VMEM, VMEM),
        scratch_shapes=[
            pltpu.VMEM((rows, depth), BF16),
            pltpu.VMEM((rows, depth), BF16),
            pltpu.VMEM((2, depth, chunk), BF16),
            pltpu.VMEM((2, rows, chunk), F32),
            pltpu.VMEM((rows, 128), F32),
            pltpu.VMEM((rows, 128), F32),
            pltpu.VMEM((rows, 128), F32),
            pltpu.VMEM((rows, 128), F32),
            pltpu.VMEM((8, rows), F32),
            pltpu.VMEM((n_tp, 8, rows), F32),
            pltpu.VMEM((8, 128), F32),
            pltpu.VMEM((n_dp, 8, 128), F32),
            pltpu.VMEM((8, rows), F32),
            pltpu.VMEM((8, rows), F32),
            dma((2,)), dma, dma((2,)), dma((2,)),
            dma((n_tp,)), dma((n_tp,)), dma((n_dp,)), dma((n_dp,)), dma, dma,
        ],
        compiler_params=pltpu.CompilerParams(vmem_limit_bytes=62 * 2**20, collective_id=0, has_side_effects=True),
        cost_estimate=pl.CostEstimate(flops=2 * rows * depth * vocab, bytes_accessed=2 * depth * vocab, transcendentals=0),
        name="logits",
    )(hm, ht, gain, lab_m, lab_t, wt_m, wt_t, w)


def grad_logits(z, lse, rw, lab, col):
    lane = lax.broadcasted_iota(jnp.int32, z.shape, 1).astype(F32)
    p = jnp.exp(z - lse)
    return rw * jnp.where(lab - col == lane, p - 1.0, p)


def du_kernel(chunk, z, w, st, du, z_v, w_v, e_v, acc, lse_v, rw_v, lab_v, sem_z, sem_w, sem_o):
    rows, vocab = z.shape
    steps = vocab // chunk

    def w_copy(i, slot):
        return pltpu.make_async_copy(w.at[:, pl.ds(pl.multiple_of(i * chunk, 128), chunk)], w_v.at[slot], sem_w.at[slot])

    def z_copy(i, slot):
        return pltpu.make_async_copy(z.at[:, pl.ds(pl.multiple_of(i * chunk, 128), chunk)], z_v.at[slot], sem_z.at[slot])

    z_copy(0, 0).start()
    w_copy(0, 0).start()
    lse_v[...] = columns(st[0, 0:1, :])
    rw_v[...] = columns(st[0, 1:2, :])
    lab_v[...] = columns(st[0, 2:3, :])
    acc[...] = jnp.zeros_like(acc)

    @pl.loop(0, steps)
    def _(i):
        slot = lax.rem(i, 2)
        z_copy(i, slot).wait()
        w_copy(i, slot).wait()

        @pl.when(i + 1 < steps)
        def _():
            z_copy(i + 1, 1 - slot).start()
            w_copy(i + 1, 1 - slot).start()

        col = (i * chunk).astype(F32)
        for g in range(chunk // 128):
            cols = slice(g * 128, (g + 1) * 128)
            e_v[:, cols] = grad_logits(z_v[slot, :, cols], lse_v[...], rw_v[...], lab_v[...], col + g * 128).astype(BF16)
        for n in range(acc.shape[1] // 512):
            cols = slice(n * 512, (n + 1) * 512)
            acc[:, cols] += lax.dot_general(e_v[...], w_v[slot, cols, :], (((1,), (1,)), ((), ())), preferred_element_type=F32)

    acc[...] = acc[...].astype(BF16).astype(F32)
    c = pltpu.make_async_copy(acc, du, sem_o)
    c.start()
    c.wait()


def du_partial(z, w, st):
    rows, vocab = z.shape
    depth = w.shape[0]
    chunk = 640
    dma = pltpu.SemaphoreType.DMA
    return pl.pallas_call(
        functools.partial(du_kernel, chunk),
        out_shape=jax.ShapeDtypeStruct((rows, depth), F32),
        in_specs=[ANY, ANY, VMEM],
        out_specs=ANY,
        scratch_shapes=[
            pltpu.VMEM((2, rows, chunk), F32),
            pltpu.VMEM((2, depth, chunk), BF16),
            pltpu.VMEM((rows, chunk), BF16),
            pltpu.VMEM((rows, depth), F32),
            pltpu.VMEM((rows, 128), F32),
            pltpu.VMEM((rows, 128), F32),
            pltpu.VMEM((rows, 128), F32),
            dma((2,)), dma((2,)), dma,
        ],
        compiler_params=pltpu.CompilerParams(vmem_limit_bytes=62 * 2**20),
        cost_estimate=pl.CostEstimate(flops=2 * rows * depth * vocab, bytes_accessed=2 * depth * vocab, transcendentals=0),
        name="du_partial",
    )(z, w, st)


def head_kernel(first, wide, u_own, u_par, z, w, st, after, out, u_v, up_v, w_v, z_v, et_v, g_v, own_v, sum_v, one_v, o_v,
                lse_v, rw_v, lab_v, sem_u, sem_p, sem_w, sem_z, sem_o, d_send, d_recv, b_send, b_recv, f_send, f_recv):
    del after
    rows, depth = u_own.shape
    half = z.shape[1] // 2
    tp, dp = lax.axis_index("tp"), lax.axis_index("dp")
    x, core = dp // 2, lax.rem(dp, 2)
    side = lax.rem((x + 1) // 2, 2)
    mate, far = x + 1 - 2 * lax.rem(x, 2), 3 - x
    far_mate = far + 1 - 2 * lax.rem(far, 2)

    def at(chip, c):
        return {"tp": tp, "dp": 2 * chip + c}

    barrier = pltpu.get_barrier_semaphore()
    for peer in (at(x, 1 - core), at(far, core), at(mate, core)):
        pl.semaphore_signal(barrier, inc=1, device_id=peer, device_id_type=MESH)

    blocks = [2 * j + 1 - core for j in range(4)] + [2 * j + core for j in range(4)]

    def u_copy(i):
        return pltpu.make_async_copy(u_own.at[:, pl.ds(pl.multiple_of(blocks[i] * 256, 256), 256)],
                                     u_v.at[pl.ds(0, rows), pl.ds(i * 256, 256)], sem_u.at[i])

    def p_copy(i, slot):
        return pltpu.make_async_copy(u_par.at[:, pl.ds(pl.multiple_of(blocks[i] * 256, 256), 256)], up_v.at[slot], sem_p.at[slot])

    def w_copies(c0, width, slot):
        cols = pl.ds(pl.multiple_of(side * half + c0, 128), width)
        return [pltpu.make_async_copy(w.at[pl.ds(pl.multiple_of(blocks[i] * 256, 256), 256), cols],
                                      w_v.at[slot, pl.ds(i * 256, 256), pl.ds(0, width)], sem_w.at[slot, i]) for i in range(8)]

    def z_copy(c0, width, slot):
        cols = pl.ds(pl.multiple_of(side * half + c0, 128), width)
        return pltpu.make_async_copy(z.at[:, cols], z_v.at[slot, :, pl.ds(0, width)], sem_z.at[slot])

    def fetch(c0, width, slot):
        for c in w_copies(c0, width, slot) + [z_copy(c0, width, slot)]:
            c.start()

    fetch(0, first, 0)
    for i in range(8):
        u_copy(i).start()
    p_copy(0, 0).start()
    p_copy(1, 1).start()
    for k in range(2):
        r = pl.ds(k * rows, rows)
        lse_v[r, :] = columns(st[k, 0:1, :])
        rw_v[r, :] = columns(st[k, 1:2, :])
        lab_v[r, :] = columns(st[k, 2:3, :])
    for i in range(8):
        p_copy(i, i % 2).wait()
        u_v[pl.ds(rows, rows), pl.ds(i * 256, 256)] = up_v[i % 2].astype(BF16)
        if i + 2 < 8:
            p_copy(i + 2, i % 2).start()
    for i in range(8):
        u_copy(i).wait()

    def d_copy(k, c0, width, slot):
        return pltpu.make_async_remote_copy(g_v.at[slot, pl.ds(0, width), :], sum_v.at[pl.ds(c0, width), :], d_send.at[slot], d_recv.at[k],
                                            device_id=at(x, 1 - core), device_id_type=MESH)

    def b_copy(k, c0, width, which):
        chip = (far_mate, far)[which]
        return pltpu.make_async_remote_copy(sum_v.at[pl.ds(c0, width), pl.ds(pl.multiple_of(chip * 256, 256), 256)],
                                            one_v.at[which, pl.ds(c0, width), :], b_send.at[2 * k + which], b_recv.at[2 * k + which],
                                            device_id=at(far, core), device_id_type=MESH)

    def f_copy(k, c0, width, slot):
        return pltpu.make_async_remote_copy(o_v.at[0, slot, :, pl.ds(0, width)], out.at[:, pl.ds(pl.multiple_of(side * half + c0, 128), width)],
                                            f_send.at[slot], f_recv.at[k], device_id=at(mate, core), device_id_type=MESH)

    def f_arrival(k, c0, width):
        dst = out.at[:, pl.ds(pl.multiple_of((1 - side) * half + c0, 128), width)]
        return pltpu.make_async_copy(dst, dst, f_recv.at[k])

    def o_copy(c0, width, slot):
        return pltpu.make_async_copy(o_v.at[1, slot, :, pl.ds(0, width)], out.at[:, pl.ds(pl.multiple_of(side * half + c0, 128), width)], sem_o.at[slot])

    def make(k, c0, width, slot):
        for c in w_copies(c0, width, slot) + [z_copy(c0, width, slot)]:
            c.wait()
        col = (side * half + c0).astype(F32)
        own, par = pl.ds(0, rows), pl.ds(rows, rows)
        for g in range(width // 128):
            cols = slice(g * 128, (g + 1) * 128)
            e = grad_logits(z_v[slot, :, cols], lse_v[own, :], rw_v[own, :], lab_v[own, :], col + g * 128)
            et_v[cols, own] = e.T.astype(BF16)
        step = min(width, 256)
        for n in range(width // step):
            zz = jnp.dot(u_v[par, :], w_v[slot, :, n * step:(n + 1) * step], preferred_element_type=F32)
            for g in range(step // 128):
                c1 = n * step + g * 128
                e = grad_logits(zz[:, g * 128:(g + 1) * 128], lse_v[par, :], rw_v[par, :], lab_v[par, :], col + c1)
                et_v[c1:c1 + 128, par] = e.T.astype(BF16)
        et = et_v[pl.ds(0, width), :]
        g_v[slot, pl.ds(0, width), :] = jnp.dot(et, u_v[:, :1024], preferred_element_type=F32)
        d_copy(k, c0, width, slot).start()
        own_v[pl.ds(0, width), :] = jnp.dot(et, u_v[:, 1024:], preferred_element_type=F32)

    def add(k, c0, width, slot):
        d_copy(k, c0, width, slot).wait_recv()
        r = pl.ds(c0, width)
        sum_v[r, :] += own_v[pl.ds(0, width), :]
        for which in range(2):
            b_copy(k, c0, width, which).start()

    def close(k, c0, width, slot, free):
        @pl.when(free)
        def _():
            f_copy(k, c0, wide, slot).wait_send()
            o_copy(c0, wide, slot).wait()
        r = pl.ds(c0, width)
        for which, chip in enumerate((mate, x)):
            b_copy(k, c0, width, which).wait_recv()
            total = sum_v[r, pl.ds(pl.multiple_of(chip * 256, 256), 256)] + one_v[which, r, :]
            o_v[which, slot, :, pl.ds(0, width)] = total.T
            (f_copy if which == 0 else lambda k, *a: o_copy(*a))(k, c0, width, slot).start()

    n = (half - first) // wide
    start = lambda k: pl.multiple_of(first + (k - 1) * wide, 128)
    fetch(start(1), wide, 1)
    pl.semaphore_wait(barrier, 3)
    make(0, 0, first, 0)
    add(0, 0, first, 0)

    @pl.loop(1, n + 1)
    def _(k):
        slot = lax.rem(k, 2)

        @pl.when(k < n)
        def _():
            fetch(start(k + 1), wide, 1 - slot)

        @pl.when(k == 2)
        def _():
            d_copy(0, 0, first, 0).wait_send()

        @pl.when(k > 2)
        def _():
            d_copy(k - 2, start(k - 2), wide, slot).wait_send()

        make(k, start(k), wide, slot)
        add(k, start(k), wide, slot)

        @pl.when(k == 1)
        def _():
            close(0, 0, first, 0, False)

        @pl.when(k == 2)
        def _():
            close(1, start(1), wide, 1, False)

        @pl.when(k == 3)
        def _():
            f_copy(0, 0, first, 0).wait_send()
            o_copy(0, first, 0).wait()
            close(2, start(2), wide, 0, False)

        @pl.when(k > 3)
        def _():
            close(k - 1, start(k - 1), wide, 1 - slot, True)

    close(n, start(n), wide, n % 2, True)
    for k in (n - 1, n):
        f_copy(k, start(k), wide, k % 2).wait_send()
        o_copy(start(k), wide, k % 2).wait()
        d_copy(k, start(k), wide, k % 2).wait_send()
    for k in range(n + 1):
        c0, width = (0, first) if k == 0 else (first + (k - 1) * wide, wide)
        f_arrival(k, c0, width).wait()
        for which in range(2):
            b_copy(k, c0, width, which).wait_send()


def head_grad(u_own, u_par, z, w, st, after):
    rows, depth = u_own.shape
    vocab = z.shape[1]
    first, wide = 128, 512
    half = vocab // 2
    n = (half - first) // wide + 1
    dma = pltpu.SemaphoreType.DMA
    return pl.pallas_call(
        functools.partial(head_kernel, first, wide),
        out_shape=jax.ShapeDtypeStruct((256, vocab), F32),
        in_specs=[ANY, ANY, ANY, ANY, VMEM, ANY],
        out_specs=ANY,
        scratch_shapes=[
            pltpu.VMEM((2 * rows, depth), BF16),
            pltpu.VMEM((2, rows, 256), F32),
            pltpu.VMEM((2, depth, wide), BF16),
            pltpu.VMEM((2, rows, wide), F32),
            pltpu.VMEM((wide, 2 * rows), BF16),
            pltpu.VMEM((2, wide, 1024), F32),
            pltpu.VMEM((wide, 1024), F32),
            pltpu.VMEM((half, 1024), F32),
            pltpu.VMEM((2, half, 256), F32),
            pltpu.VMEM((2, 2, 256, wide), F32),
            pltpu.VMEM((2 * rows, 128), F32),
            pltpu.VMEM((2 * rows, 128), F32),
            pltpu.VMEM((2 * rows, 128), F32),
            dma((8,)), dma((2,)), dma((2, 8)), dma((2,)), dma((2,)),
            dma((2,)), dma((n,)), dma((2 * n,)), dma((2 * n,)), dma((2,)), dma((n,)),
        ],
        compiler_params=pltpu.CompilerParams(vmem_limit_bytes=63 * 2**20, collective_id=1, has_side_effects=True),
        cost_estimate=pl.CostEstimate(flops=300 * 10**9, bytes_accessed=2 * depth * vocab, transcendentals=0),
        name="head_grad",
    )(u_own, u_par, z, w, st, after)


def total_kernel(n_dp, part, out, land, ssem, rsem):
    tp, dp = lax.axis_index("tp"), lax.axis_index("dp")
    barrier = pltpu.get_barrier_semaphore()
    for d in range(1, n_dp):
        pl.semaphore_signal(barrier, inc=1, device_id={"tp": tp, "dp": lax.rem(dp + d, n_dp)}, device_id_type=MESH)
    land[dp] = part[...]
    pl.semaphore_wait(barrier, n_dp - 1)
    copies = []
    for d in range(1, n_dp):
        c = pltpu.make_async_remote_copy(part, land.at[dp], ssem.at[d], rsem.at[dp],
                                         device_id={"tp": tp, "dp": lax.rem(dp + d, n_dp)}, device_id_type=MESH)
        c.start()
        copies.append(c)
    for d in range(1, n_dp):
        src = lax.rem(dp + d, n_dp)
        pltpu.make_async_copy(land.at[src], land.at[src], rsem.at[src]).wait()
    total = land[0]
    for d in range(1, n_dp):
        total = total + land[d]
    out[...] = total
    for c in copies:
        c.wait_send()


def dp_total(n_dp, part):
    dma = pltpu.SemaphoreType.DMA
    return pl.pallas_call(
        functools.partial(total_kernel, n_dp),
        out_shape=jax.ShapeDtypeStruct(part.shape, F32),
        in_specs=[VMEM],
        out_specs=VMEM,
        scratch_shapes=[pltpu.VMEM((n_dp,) + part.shape, F32), dma((n_dp,)), dma((n_dp,))],
        compiler_params=pltpu.CompilerParams(collective_id=2, has_side_effects=True),
        name="dp_total",
    )(part)


def solution(mesh):
    n_tp, n_dp = mesh.shape["tp"], mesh.shape["dp"]

    def local_step(h_main, h_mtp, labels_main, labels_mtp, weight_main, weight_mtp, gain_final, gain_mtp, w_out):
        batch_loc, seq_len, depth = h_main.shape
        rows = 2 * seq_len
        share = rows // n_tp
        tp = lax.axis_index("tp")
        hm, ht = h_main[0], h_mtp[0]
        gain = jnp.stack([gain_final, gain_mtp])
        per = seq_len // share
        at = lax.rem(tp, per) * share
        is_main = tp < per
        x = jnp.where(is_main, lax.dynamic_slice_in_dim(hm, at, share), lax.dynamic_slice_in_dim(ht, at, share)).astype(F32)
        g = jnp.where(is_main, gain_final, gain_mtp)[None, :]
        inv = lax.rsqrt(jnp.mean(x * x, axis=-1, keepdims=True) + NORM_EPS)
        normed = x * inv
        u_share = lax.optimization_barrier((normed * g).astype(BF16)).astype(F32)
        swap = [(d, (d // 2 ^ 1) * 2 + d % 2) for d in range(n_dp)]
        u_par = lax.all_gather(lax.ppermute(u_share, "dp", swap), "tp", axis=0, tiled=True)

        z, u_own, st, lpart = logits(n_tp, n_dp, hm, ht, gain, labels_main, labels_mtp, weight_main, weight_mtp, w_out)
        du = du_partial(z, w_out, st)
        grad_w = head_grad(u_own, u_par, z, w_out, st, du)
        gu = lax.psum_scatter(du, "tp", scatter_dimension=0, tiled=True)
        gn = gu * g
        gx = inv * (gn - normed * jnp.mean(gn * normed, axis=-1, keepdims=True))
        gg = jnp.sum(gu * normed, axis=0, keepdims=True)
        gg = jnp.concatenate([jnp.where(is_main, gg, 0.0), jnp.where(is_main, 0.0, gg), jnp.zeros((6, depth), F32)])
        pack = lax.optimization_barrier(jnp.concatenate([gx.astype(BF16).astype(F32), gg]))
        pack = lax.optimization_barrier(lax.all_gather(pack, "tp", axis=0, tiled=False))
        grad_h = pack[:, :share].astype(BF16).reshape(2, batch_loc, seq_len, depth)
        gains = jnp.sum(pack[:, share:], axis=0)
        row = lax.broadcasted_iota(jnp.int32, (8, depth), 0)
        total = dp_total(n_dp, jnp.where(row == 2, lpart[0, 0], gains))
        return total[2, 0], grad_h[0], grad_h[1], grad_w, total[0], total[1]

    row_spec = P("dp", None)
    return jax.shard_map(
        local_step,
        mesh=mesh,
        in_specs=(P("dp", None, None), P("dp", None, None), row_spec, row_spec, row_spec, row_spec, P(None), P(None), P(None, "tp")),
        out_specs=(P(), P("dp", None, None), P("dp", None, None), P("dp", "tp"), P(None), P(None)),
        check_vma=False,
    )
```

```python
import functools

import jax
import jax.numpy as jnp
from jax import lax
from jax.experimental import pallas as pl
from jax.experimental.pallas import tpu as pltpu
from jax.sharding import PartitionSpec as P

NORM_EPS = 1e-6
MTP_LAMBDA = 0.3
MESH = pl.DeviceIdType.MESH
F32 = jnp.float32
BF16 = jnp.bfloat16
ANY = pl.BlockSpec(memory_space=pl.ANY)
VMEM = pl.BlockSpec(memory_space=pltpu.VMEM)


def columns(row, width=128):
    return jnp.broadcast_to(row, (width, row.shape[1])).T


RING = 4


class Torus:
    def __init__(self):
        self.tp, self.dp = lax.axis_index("tp"), lax.axis_index("dp")
        self.y, self.z = lax.rem(self.tp, RING), self.tp // RING
        self.x, self.core = self.dp // 2, lax.rem(self.dp, 2)
        self.mate = self.x + 1 - 2 * lax.rem(self.x, 2)
        self.far = 3 - self.x
        self.far_mate = self.far + 1 - 2 * lax.rem(self.far, 2)
        self.side = lax.rem((self.x + 1) // 2, 2)

    def chip(self, x, core):
        return {"tp": self.tp, "dp": 2 * x + core}

    def step(self, axis, d):
        y = lax.rem(self.y + d + RING, RING) if axis == 0 else self.y
        z = lax.rem(self.z + d + RING, RING) if axis == 1 else self.z
        return {"tp": z * RING + y, "dp": self.dp}

    def coords(self, s):
        return (0, self.y, 1, self.z) if s == 0 else (1, self.z, 0, self.y)


def greet(place, n_tp, n_dp):
    barrier = pltpu.get_barrier_semaphore()
    for d in range(1, n_tp):
        pl.semaphore_signal(barrier, inc=1, device_id={"tp": lax.rem(place.tp + d, n_tp), "dp": place.dp}, device_id_type=MESH)
    for d in range(1, n_dp):
        pl.semaphore_signal(barrier, inc=1, device_id={"tp": place.tp, "dp": lax.rem(place.dp + d, n_dp)}, device_id_type=MESH)
    return lambda: pl.semaphore_wait(barrier, n_tp + n_dp - 2)


def remote(src, dst, send, recv, to):
    return pltpu.make_async_remote_copy(src, dst, send, recv, device_id=to, device_id_type=MESH)


def arrived(dst, sem):
    pltpu.make_async_copy(dst, dst, sem).wait()


def ds(start, size, unit=8):
    return pl.ds(pl.multiple_of(start, unit), size)


def grad_logits(z, lse, rw, lab, col):
    lane = lax.broadcasted_iota(jnp.int32, z.shape, 1).astype(F32)
    p = jnp.exp(z - lse)
    return rw * jnp.where(lab - col == lane, p - 1.0, p)


LEFT = 4096
SLICE = 24
SPREAD = 2 * 16 * SLICE


def logits_kernel(n_tp, n_dp, chunk, left, hm, ht, gain_m, gain_t, lab_m, lab_t, wt_m, wt_t, w, z, u_out, up_out, du_out, st, lpart,
                  h_v, u_v, uf_v, got_v, w_v, z_v, e_v, x_v, m_v, s_v, t_v,
                  lab_v, send_v, land, wsend, wland, psend, pland, sem_h, sem_u, sem_w, sem_z, ssem, rsem, wssem, wrsem, pssem, prsem,
                  gs, gr, xs, xr, sem_d, sem_k):
    seq, depth = hm.shape
    rows, vocab = z.shape
    steps = vocab // chunk
    here = Torus()
    tp, dp = here.tp, here.dp
    mate = here.chip(here.mate, here.core)
    lo, hi = pl.ds(0, depth // 2), pl.ds(depth // 2, depth // 2)

    loads = [pltpu.make_async_copy(src, h_v.at[pl.ds(i * seq, seq), :], sem_h.at[i]) for i, src in enumerate((hm, ht))]

    def w_copy(i, slot):
        return pltpu.make_async_copy(w.at[:, ds(i * chunk, chunk, 128)], w_v.at[slot], sem_w.at[slot])

    def z_copy(i, slot):
        return pltpu.make_async_copy(z_v.at[slot], z.at[:, ds(i * chunk, chunk, 128)], sem_z.at[slot])

    for c in loads:
        c.start()
    w_copy(0, 0).start()
    met = greet(here, n_tp, n_dp)

    m_v[...] = jnp.full_like(m_v, -jnp.inf)
    s_v[...] = jnp.zeros_like(s_v)
    t_v[...] = jnp.zeros_like(t_v)
    first = (tp * vocab).astype(F32)
    lab_v[pl.ds(0, seq), :] = columns(lab_m[...].astype(F32) - first)
    lab_v[pl.ds(seq, seq), :] = columns(lab_t[...].astype(F32) - first)
    wrow = lax.broadcasted_iota(jnp.int32, (8, 128), 0)
    wsend[...] = jnp.where(wrow == 0, jnp.sum(wt_m[...]), jnp.sum(wt_t[...]))
    wland[dp] = wsend[...]

    for half, gain in ((0, gain_m), (1, gain_t)):
        loads[half].wait()
        g = gain[...]

        @pl.loop(0, seq // 128)
        def _(i):
            r = ds(half * seq + i * 128, 128, 128)
            x = h_v[r, :].astype(F32)
            inv = lax.rsqrt(jnp.mean(x * x, axis=-1, keepdims=True) + NORM_EPS)
            u = (x * inv * g).astype(BF16)
            u_v[r, :] = u
            uf_v[r, :] = u.astype(F32)

    u_copy = pltpu.make_async_copy(u_v, u_out, sem_u)
    u_copy.start()
    with jax.named_scope('meet'):
        met()

    def block(s, p1, p2):
        return ds(s * (SPREAD // 2) + (lax.rem(p2 + RING, RING) * RING + lax.rem(p1 + RING, RING)) * SLICE, SLICE)

    def group(s, p2):
        return ds(s * (SPREAD // 2) + lax.rem(p2 + RING, RING) * RING * SLICE, RING * SLICE)

    def hop(s, j, rows_of, lanes, axis, d):
        ref = got_v.at[rows_of, lanes]
        return remote(ref, ref, gs.at[s, j], gr.at[s, j], here.step(axis, d))

    def first_step(s):
        a1, p1, a2, p2 = here.coords(s)
        b = block(s, p1, p2)
        return [remote(uf_v.at[b, :], got_v.at[b, :], gs.at[s, 0], gr.at[s, 0], mate)]

    every = pl.ds(0, depth)

    def hops(s, stage):
        a1, p1, a2, p2 = here.coords(s)
        if stage == 1:
            b = block(s, p1, p2)
            return [hop(s, 1, b, every, a1, 1), hop(s, 2, b, every, a1, -1)]
        if stage == 2:
            return [hop(s, 3, block(s, p1 - 1, p2), lo, a1, 1), hop(s, 4, block(s, p1 + 1, p2), hi, a1, -1)]
        if stage == 3:
            return [hop(s, 5, group(s, p2), lo, a2, 1), hop(s, 6, group(s, p2), lo, a2, -1)]
        if stage == 4:
            return [hop(s, 9, group(s, p2), hi, a2, 1), hop(s, 10, group(s, p2), hi, a2, -1)]
        if stage == 5:
            return [hop(s, 7, group(s, p2 - 1), lo, a2, 1)]
        return [hop(s, 8, group(s, p2 + 1), hi, a2, -1)]

    def landed(s, stage):
        a1, p1, a2, p2 = here.coords(s)
        waits = {
            1: [(block(s, p1, p2), every, 0)],
            2: [(block(s, p1 - 1, p2), every, 1), (block(s, p1 + 1, p2), every, 2)],
            3: [(block(s, p1 - 2, p2), lo, 3), (block(s, p1 + 2, p2), hi, 4)],
            4: [],
            5: [(group(s, p2 - 1), lo, 5)],
            6: [(group(s, p2 + 1), hi, 10)],
            7: [(group(s, p2 + 1), lo, 6), (group(s, p2 - 1), hi, 9), (group(s, p2 - 2), lo, 7), (group(s, p2 + 2), hi, 8)],
        }
        for r, lanes, j in waits[stage]:
            arrived(got_v.at[r, lanes], gr.at[s, j])

    def pass_on(s, stage):
        landed(s, stage)
        for c in hops(s, stage):
            c.start()

    straight = remote(uf_v.at[pl.ds(SPREAD, rows - SPREAD), :], got_v.at[pl.ds(SPREAD, rows - SPREAD), :], xs, xr, mate)
    wcopies = []
    for d in range(1, n_dp):
        peer = lax.rem(dp + d, n_dp)
        c = remote(wsend, wland.at[dp], wssem.at[d], wrsem.at[dp], {"tp": tp, "dp": peer})
        c.start()
        wcopies.append(c)
    for c in first_step(0) + first_step(1) + [straight]:
        c.start()
    when = {(1, 0): (0, 1), (1, 3): (1, 1), (2, 0): (0, 2), (2, 3): (1, 2), (3, 0): (0, 3), (3, 3): (1, 3)}
    lane = lax.broadcasted_iota(jnp.int32, (rows, 128), 1).astype(F32)

    @pl.loop(0, steps)
    def _(i):
        slot = lax.rem(i, 2)
        with jax.named_scope('wwait'):
            w_copy(i, slot).wait()

        @pl.when(i + 1 < steps)
        def _():
            w_copy(i + 1, 1 - slot).start()

        @pl.when(i >= 2)
        def _():
            z_copy(i - 2, slot).wait()

        m, s, t = m_v[...], s_v[...], t_v[...]
        rel = lab_v[...] - (i * chunk).astype(F32)
        for n in range(chunk // 256):
            for (at_i, at_n), (which, stage) in when.items():
                if at_n == n:
                    @pl.when(i == at_i)
                    def _():
                        with jax.named_scope(f'pass{which}{stage}'):
                            pass_on(which, stage)
            cols = slice(n * 256, (n + 1) * 256)
            zz = jnp.dot(u_v[...], w_v[slot, :, cols], preferred_element_type=F32)
            z_v[slot, :, cols] = zz
            za, zb = zz[:, :128], zz[:, 128:]
            new = jnp.maximum(m, jnp.maximum(za, zb))
            s = s * jnp.exp(m - new) + (jnp.exp(za - new) + jnp.exp(zb - new))
            t = jnp.where(rel == lane + n * 256, za, t)
            t = jnp.where(rel == lane + (n * 256 + 128), zb, t)
            m = new
        m_v[...], s_v[...], t_v[...] = m, s, t
        z_copy(i, slot).start()

    mt = m_v[...].T
    top = jnp.max(mt, axis=0, keepdims=True)
    total = jnp.sum(s_v[...].T * jnp.exp(mt - top), axis=0, keepdims=True)
    hit = jnp.sum(t_v[...].T, axis=0, keepdims=True)
    mine = jnp.where(lax.broadcasted_iota(jnp.int32, (2, rows), 0) == 0, top + jnp.log(total), hit)
    send_v[...] = mine
    land[tp] = mine
    copies = []
    for d in range(1, n_tp):
        peer = lax.rem(tp + d, n_tp)
        c = remote(send_v, land.at[tp], ssem.at[d], rsem.at[tp], {"tp": peer, "dp": dp})
        c.start()
        copies.append(c)
    with jax.named_scope('pass45'):
        for stage in (4, 5):
            for which in range(2):
                pass_on(which, stage)
    for d in range(1, n_dp):
        src = lax.rem(dp + d, n_dp)
        arrived(wland.at[src], wrsem.at[src])
    sums = wland[0]
    for d in range(1, n_dp):
        sums = sums + wland[d]
    coef_m = 1.0 / sums[0:1, 0:1]
    coef_t = MTP_LAMBDA / sums[1:2, 0:1]
    rw = jnp.concatenate([wt_m[...] * coef_m, wt_t[...] * coef_t], axis=1)
    lab = jnp.concatenate([lab_m[...], lab_t[...]], axis=1).astype(F32)
    with jax.named_scope('statwait'):
        for d in range(1, n_tp):
            src = lax.rem(tp + d, n_tp)
            arrived(land.at[src], rsem.at[src])
    top = land[0]
    for d in range(1, n_tp):
        top = jnp.maximum(top, land[d])
    acc = jnp.zeros_like(top)
    hits = jnp.zeros_like(top)
    for d in range(n_tp):
        acc = acc + jnp.exp(land[d] - top)
        hits = hits + land[d]
    lse = (top + jnp.log(acc))[0:1, :]
    hit = hits[1:2, :]
    lpart[...] = jnp.broadcast_to(jnp.sum(rw * (lse - hit)), (8, 128))
    srow = lax.broadcasted_iota(jnp.int32, (8, rows), 0)
    mine = jnp.where(srow == 0, lse, jnp.where(srow == 1, rw, lab - first))
    psend[...] = mine
    st[0] = mine
    swap = remote(psend, pland, pssem, prsem, mate)
    swap.start()
    m_v[...] = columns(lse)
    s_v[...] = columns(rw)

    skip = left - (steps - 2) * chunk
    for step, begin, at in ((steps - 1, 0, 0), (steps - 2, skip, chunk)):
        for c in range(begin, chunk, 128):
            e_v[:, at + c - begin:at + c - begin + 128] = grad_logits(
                z_v[step % 2, :, c:c + 128], m_v[...], s_v[...], lab_v[...], float(step * chunk + c)).astype(BF16)

    def e_dot(r, n):
        cols = slice(n * 512, (n + 1) * 512)
        nt = (((1,), (1,)), ((), ()))
        return (lax.dot_general(e_v[r, :chunk], w_v[(steps - 1) % 2, cols, :], nt, preferred_element_type=F32)
                + lax.dot_general(e_v[r, chunk:], w_v[(steps - 2) % 2, cols, skip:], nt, preferred_element_type=F32))

    def du_copy(part, n):
        cols = pl.ds(n * 512, 512)
        src, r = ((uf_v.at[pl.ds(0, SPREAD), cols], pl.ds(0, SPREAD)), (x_v.at[:, cols], pl.ds(SPREAD, rows - SPREAD)))[part]
        return pltpu.make_async_copy(src, du_out.at[r, cols], sem_d.at[part, n])

    with jax.named_scope('sendwait'):
        for c in first_step(0) + first_step(1):
            c.wait_send()
    for n in range(depth // 512):
        cols = slice(n * 512, (n + 1) * 512)
        uf_v[:SPREAD, cols] = e_dot(slice(0, SPREAD), n)
        du_copy(0, n).start()
        if n == 1:
            with jax.named_scope('pass06'):
                pass_on(0, 6)
        if n == 2:
            with jax.named_scope('pass16'):
                pass_on(1, 6)
    for n in range(depth // 512):
        cols = slice(n * 512, (n + 1) * 512)
        x_v[:, cols] = e_dot(slice(SPREAD, rows), n)
        du_copy(1, n).start()
    u_copy.wait()
    with jax.named_scope('swapwait'):
        swap.wait()
    st[1] = pland[...]

    def keep(i, begin, end):
        @pl.loop(begin // 128, end // 128)
        def _(j):
            r = ds(j * 128, 128, 128)
            u_v[r, :] = got_v[r, :].astype(BF16)
        return pltpu.make_async_copy(u_v.at[pl.ds(begin, end - begin), :], up_out.at[pl.ds(begin, end - begin), :], sem_k.at[i])

    kept = []
    parts = [(0, SPREAD // 2, lambda: landed(0, 7)), (SPREAD // 2, SPREAD, lambda: landed(1, 7)),
             (SPREAD, rows, lambda: arrived(got_v.at[pl.ds(SPREAD, rows - SPREAD), :], xr))]
    for i, (begin, end, wait) in enumerate(parts):
        with jax.named_scope(f'land{i}'):
            wait()
        kept.append(keep(i, begin, end))
        kept[-1].start()
    tail = jax.named_scope('tail')
    tail.__enter__()
    for c in wcopies + copies:
        c.wait_send()
    for s in range(2):
        for stage in range(1, 7):
            for c in hops(s, stage):
                c.wait_send()
    z_copy(steps - 2, (steps - 2) % 2).wait()
    z_copy(steps - 1, (steps - 1) % 2).wait()
    straight.wait_send()
    for n in range(depth // 512):
        for part in range(2):
            du_copy(part, n).wait()
    for c in kept:
        c.wait()
    tail.__exit__(None, None, None)


def logits(n_tp, n_dp, hm, ht, gain_m, gain_t, lab_m, lab_t, wt_m, wt_t, w):
    seq, depth = hm.shape
    rows, vocab = 2 * seq, w.shape[1]
    chunk = 1280
    dma = pltpu.SemaphoreType.DMA
    return pl.pallas_call(
        functools.partial(logits_kernel, n_tp, n_dp, chunk, LEFT),
        out_shape=(
            jax.ShapeDtypeStruct((rows, vocab), F32),
            jax.ShapeDtypeStruct((rows, depth), BF16),
            jax.ShapeDtypeStruct((rows, depth), BF16),
            jax.ShapeDtypeStruct((rows, depth), F32),
            jax.ShapeDtypeStruct((2, 8, rows), F32),
            jax.ShapeDtypeStruct((8, 128), F32),
        ),
        in_specs=[ANY, ANY] + [VMEM] * 6 + [ANY],
        out_specs=(ANY, ANY, ANY, ANY, VMEM, VMEM),
        scratch_shapes=[
            pltpu.VMEM((rows, depth), BF16),
            pltpu.VMEM((rows, depth), BF16),
            pltpu.VMEM((rows, depth), F32),
            pltpu.VMEM((rows, depth), F32),
            pltpu.VMEM((2, depth, chunk), BF16),
            pltpu.VMEM((2, rows, chunk), F32),
            pltpu.VMEM((rows, vocab - LEFT), BF16),
            pltpu.VMEM((rows - SPREAD, depth), F32),
            pltpu.VMEM((rows, 128), F32),
            pltpu.VMEM((rows, 128), F32),
            pltpu.VMEM((rows, 128), F32),
            pltpu.VMEM((rows, 128), F32),
            pltpu.VMEM((2, rows), F32),
            pltpu.VMEM((n_tp, 2, rows), F32),
            pltpu.VMEM((8, 128), F32),
            pltpu.VMEM((n_dp, 8, 128), F32),
            pltpu.VMEM((8, rows), F32),
            pltpu.VMEM((8, rows), F32),
            dma((2,)), dma, dma((2,)), dma((2,)),
            dma((n_tp,)), dma((n_tp,)), dma((n_dp,)), dma((n_dp,)), dma, dma,
            dma((2, 11)), dma((2, 11)), dma, dma, dma((2, depth // 512)), dma((3,)),
        ],
        compiler_params=pltpu.CompilerParams(vmem_limit_bytes=67043328, collective_id=0, has_side_effects=True),
        cost_estimate=pl.CostEstimate(flops=2 * rows * depth * vocab, bytes_accessed=2 * depth * vocab, transcendentals=0),
        name="logits",
    )(hm, ht, gain_m, gain_t, lab_m, lab_t, wt_m, wt_t, w)


def head_kernel(n_tp, n_dp, first, wide, task, left, plan, hm, ht, gain_m, gain_t, u_own, u_par, z, w, st, du_in, lpart,
                fin, gh, ghb, du, tot, u_v, w_v, z_v, et_v, g_v, own_v, sum_v, one_v, acc_v, e_v,
                lse_v, rw_v, lab_v, ra_v, rl_v, rb_v, rm_v, ra2_v, rb2_v, rh_v, gg_v, gland, tland, tsend,
                sem_u, sem_p, sem_w, sem_z, sem_a, sem_o, d_send, d_recv, b_send, b_recv, f_send, f_recv,
                rs, rr, sem_l, sem_x, g_s, g_r, t_s, t_r):
    rows, depth = u_own.shape
    seq = rows // 2
    vocab = z.shape[1]
    half = vocab // 2
    here = Torus()
    tp, dp = here.tp, here.dp
    x, core, side, mate, far, far_mate = here.x, here.core, here.side, here.mate, here.far, here.far_mate
    met = greet(here, n_tp, n_dp)

    blocks = [2 * j + 1 - core for j in range(4)] + [2 * j + core for j in range(4)]
    block = [ds(b * 256, 256, 256) for b in blocks]

    def u_copies(k):
        return [pltpu.make_async_copy((u_own, u_par)[k].at[:, block[i]], u_v.at[pl.ds(k * rows, rows), pl.ds(i * 256, 256)], sem_u.at[k, i])
                for i in range(8)]

    def u_wait(k):
        with jax.named_scope('uwait'):
            for c in u_copies(k):
                c.wait()

    def w_copies(col, width, slot):
        return [pltpu.make_async_copy(w.at[block[i], ds(col, width, 128)],
                                      w_v.at[slot, pl.ds(i * 256, 256), pl.ds(0, width)], sem_w.at[slot, i]) for i in range(8)]

    def z_copy(col, width, slot):
        return pltpu.make_async_copy(z.at[:, ds(col, width, 128)], z_v.at[slot, :, pl.ds(0, width)], sem_z.at[slot])

    def fetch(c0, width, slot):
        for c in w_copies(side * half + c0, width, slot) + [z_copy(side * half + c0, width, slot)]:
            c.start()

    n = (half - first) // wide
    start = lambda k: pl.multiple_of(first + (k - 1) * wide, 128)
    fetch(0, first, 0)
    for c in u_copies(1):
        c.start()
    for k in range(2):
        r = pl.ds(k * rows, rows)
        lse_v[r, :] = columns(st[k, 0:1, :])
        rw_v[r, :] = columns(st[k, 1:2, :])
        lab_v[r, :] = columns(st[k, 2:3, :])
    def d_copy(k, c0, width, part):
        lanes = pl.ds(part * 512, 512)
        return remote(g_v.at[lax.rem(k, 2), pl.ds(0, width), lanes], sum_v.at[pl.ds(c0, width), lanes], d_send.at[lax.rem(k, 2), part],
                      d_recv.at[k, part], here.chip(x, 1 - core))

    def b_copy(k, c0, width, which):
        chip = (far_mate, far)[which]
        return remote(sum_v.at[pl.ds(c0, width), ds(chip * 256, 256, 256)], one_v.at[which, pl.ds(c0, width), :],
                      b_send.at[2 * k + which], b_recv.at[2 * k + which], here.chip(far, core))

    def f_copy(k, c0, width):
        return remote(sum_v.at[pl.ds(c0, width), ds(mate * 256, 256, 256)], fin.at[1, pl.ds(c0, width), :],
                      f_send.at[k], f_recv.at[k], here.chip(mate, core))

    def o_copy(k, c0, width):
        return pltpu.make_async_copy(sum_v.at[pl.ds(c0, width), ds(x * 256, 256, 256)], fin.at[0, pl.ds(c0, width), :], sem_o.at[k])

    def make(k, c0, width, slot, begin=lambda: None, early=lambda: None, middle=lambda: None):
        with jax.named_scope('wzwait'):
            for c in w_copies(side * half + c0, width, slot) + [z_copy(side * half + c0, width, slot)]:
                c.wait()
        begin()
        col = (side * half + c0).astype(F32)
        own, par = pl.ds(0, rows), pl.ds(rows, rows)
        for g in range(width // 128):
            cols = slice(g * 128, (g + 1) * 128)
            e = grad_logits(z_v[slot, :, cols], lse_v[own, :], rw_v[own, :], lab_v[own, :], col + g * 128)
            et_v[cols, own] = e.T.astype(BF16)
        early()
        for n in range(0, width, 256):
            step = min(width - n, 256)
            zz = jnp.dot(u_v[par, :], w_v[slot, :, n:n + step], preferred_element_type=F32)
            for c1 in range(n, n + step, 128):
                e = grad_logits(zz[:, c1 - n:c1 - n + 128], lse_v[par, :], rw_v[par, :], lab_v[par, :], col + c1)
                et_v[c1:c1 + 128, par] = e.T.astype(BF16)
        middle()
        et = et_v[pl.ds(0, width), :]
        for part in range(2):
            g_v[lax.rem(k, 2), pl.ds(0, width), part * 512:(part + 1) * 512] = jnp.dot(et, u_v[:, part * 512:(part + 1) * 512], preferred_element_type=F32)
            d_copy(k, c0, width, part).start()
        own_v[pl.ds(0, width), :] = jnp.dot(et, u_v[:, 1024:], preferred_element_type=F32)

    def add(k, c0, width):
        with jax.named_scope('dwait'):
            for part in range(2):
                d_copy(k, c0, width, part).wait_recv()
        r = pl.ds(c0, width)
        sum_v[r, :] += own_v[pl.ds(0, width), :]
        for which in range(2):
            b_copy(k, c0, width, which).start()

    def close(k, c0, width):
        r = pl.ds(c0, width)
        for which, chip in enumerate((mate, x)):
            with jax.named_scope('bwait'):
                b_copy(k, c0, width, which).wait_recv()
            sum_v[r, ds(chip * 256, 256, 256)] += one_v[which, r, :]
            (f_copy if which == 0 else o_copy)(k, c0, width).start()

    per = left // task

    def acc_copies(h, back):
        out = []
        for i in range(8):
            mine, there = acc_v.at[:, pl.ds(i * 256, 256)], (du if back else du_in).at[ds(h * seq, seq, 256), block[i]]
            out.append(pltpu.make_async_copy(*((mine, there) if back else (there, mine)), sem_a.at[i]))
        return out

    def du_fetch(t, slot):
        h, i = t // per, lax.rem(t, per)
        for c in w_copies(i * task, task, slot):
            c.start()
        pltpu.make_async_copy(z.at[ds(h * seq, seq, 256), ds(i * task, task, 128)], z_v.at[slot, pl.ds(0, seq), :], sem_z.at[slot]).start()

    def du_wait(slot):
        for c in w_copies(0, task, slot):
            c.wait()
        pltpu.make_async_copy(z.at[pl.ds(0, seq), pl.ds(0, task)], z_v.at[slot, pl.ds(0, seq), :], sem_z.at[slot]).wait()

    def du_run(k, lo, hi):
        @pl.loop(lo, hi)
        def _(t):
            slot = lax.rem(k + 1 + t, 2)
            h, i = t // per, lax.rem(t, per)
            at_point(t, "task")

            @pl.when(t + 1 < hi)
            def _():
                du_fetch(t + 1, 1 - slot)

            @pl.when((t + 1 == hi) & (k < n))
            def _():
                fetch(start(k + 1), wide, 1 - slot)

            du_wait(slot)

            @pl.when(i == 0)
            def _():
                for c in acc_copies(h, False):
                    c.wait()

            r = ds(h * seq, seq, 256)
            col = (i * task).astype(F32)
            for g in range(task // 128):
                cols = slice(g * 128, (g + 1) * 128)
                e_v[:, cols] = grad_logits(z_v[slot, :seq, cols], lse_v[r, :], rw_v[r, :], lab_v[r, :], col + g * 128).astype(BF16)
            for m in range(depth // 512):
                cols = slice(m * 512, (m + 1) * 512)
                acc_v[:, cols] += lax.dot_general(e_v[...], w_v[slot, cols, :], (((1,), (1,)), ((), ())), preferred_element_type=F32)

            @pl.when(i == per - 1)
            def _():
                acc_v[...] = acc_v[...].astype(BF16).astype(F32)
                for c in acc_copies(h, True):
                    c.start()
                for c in acc_copies(h, True):
                    c.wait()

            @pl.when((i == per - 1) & (h == 0))
            def _():
                for c in acc_copies(1, False):
                    c.start()

    lo, hi, every = pl.ds(0, depth // 2), pl.ds(depth // 2, depth // 2), pl.ds(0, depth)

    def mod(p):
        return lax.rem(p + RING, RING)

    def ring(h, s):
        q = 2 * h + s
        a1, p1, a2, p2 = here.coords(s)
        base = h * seq + s * (seq // 2)

        def rows1(p):
            return ds(base + mod(p) * 64, 64, 64)

        def rows2(p):
            return ds(base + p1 * 64 + mod(p) * 16, 16, 16)

        def sub(p):
            return ds(mod(p) * 16, 16, 16)

        def go(j, src, dst, axis, d):
            return lambda: remote(src, dst, rs.at[q, j], rr.at[q, j], here.step(axis, d))

        def near(src, dst, j):
            return lambda: pltpu.make_async_copy(src, dst, sem_l.at[q, j])

        sends = {
            0: [go(0, du.at[rows1(p1 + 2), lo], ra_v.at[q, 0], a1, 1), go(1, du.at[rows1(p1 + 2), hi], ra_v.at[q, 1], a1, -1),
                go(2, du.at[rows1(p1 + 1), hi], rb_v.at[q, 0, :, hi], a1, 1), go(3, du.at[rows1(p1 - 1), lo], rb_v.at[q, 1, :, lo], a1, -1)],
            1: [go(4, ra_v.at[q, 0], rb_v.at[q, 0, :, lo], a1, 1), go(5, ra_v.at[q, 1], rb_v.at[q, 1, :, hi], a1, -1)],
            2: [go(6, rm_v.at[q, sub(p2 + 2), lo], ra2_v.at[q, 0], a2, 1), go(7, rm_v.at[q, sub(p2 + 2), hi], ra2_v.at[q, 1], a2, -1),
                go(8, rm_v.at[q, sub(p2 + 1), hi], rb2_v.at[q, 0, :, hi], a2, 1), go(9, rm_v.at[q, sub(p2 - 1), lo], rb2_v.at[q, 1, :, lo], a2, -1)],
            3: [go(10, ra2_v.at[q, 0], rb2_v.at[q, 0, :, lo], a2, 1), go(11, ra2_v.at[q, 1], rb2_v.at[q, 1, :, hi], a2, -1)],
            4: [go(12, rm_v.at[q, sub(p2), :], gh.at[rows2(p2), :], a2, 1), go(13, rm_v.at[q, sub(p2), :], gh.at[rows2(p2), :], a2, -1)],
            5: [go(14, gh.at[rows2(p2 - 1), lo], gh.at[rows2(p2 - 1), lo], a2, 1), go(15, gh.at[rows2(p2 + 1), hi], gh.at[rows2(p2 + 1), hi], a2, -1)],
            6: [go(16, gh.at[rows1(p1), :], gh.at[rows1(p1), :], a1, 1), go(17, gh.at[rows1(p1), :], gh.at[rows1(p1), :], a1, -1)],
            7: [go(18, gh.at[rows1(p1 - 1), lo], gh.at[rows1(p1 - 1), lo], a1, 1), go(19, gh.at[rows1(p1 + 1), hi], gh.at[rows1(p1 + 1), hi], a1, -1)],
        }
        lands = {
            0: [(ra_v.at[q, 0], 0), (ra_v.at[q, 1], 1)],
            1: [(rb_v.at[q, 0, :, hi], 2), (rb_v.at[q, 1, :, lo], 3), (rb_v.at[q, 0, :, lo], 4), (rb_v.at[q, 1, :, hi], 5)],
            2: [(ra2_v.at[q, 0], 6), (ra2_v.at[q, 1], 7)],
            3: [(rb2_v.at[q, 0, :, hi], 8), (rb2_v.at[q, 1, :, lo], 9), (rb2_v.at[q, 0, :, lo], 10), (rb2_v.at[q, 1, :, hi], 11)],
            4: [(gh.at[rows2(p2 - 1), :], 12), (gh.at[rows2(p2 + 1), :], 13)],
            5: [(gh.at[rows2(p2 - 2), lo], 14), (gh.at[rows2(p2 + 2), hi], 15)],
            6: [(gh.at[rows1(p1 - 1), :], 16), (gh.at[rows1(p1 + 1), :], 17)],
            7: [(gh.at[rows1(p1 - 2), lo], 18), (gh.at[rows1(p1 + 2), hi], 19)],
        }
        local = [near(du.at[rows1(p1 + 1), lo], rl_v.at[s, 0], 0), near(du.at[rows1(p1 - 1), hi], rl_v.at[s, 1], 1),
                 near(du.at[rows1(p1), :], rm_v.at[q], 2),
                 near((hm, ht)[h].at[ds(s * (seq // 2) + p1 * 64 + p2 * 16, 16, 16), :], rh_v.at[q], 3)]

        def keep():
            return pltpu.make_async_copy(rm_v.at[q, sub(p2), :], gh.at[rows2(p2), :], sem_x.at[q])

        return q, sub, p2, sends, lands, local, keep

    def event(h, stage):
        for s in range(2):
            q, sub, p2, sends, lands, local, keep = ring(h, s)
            if stage == 0:
                for c in sends[0] + local:
                    c().start()
                continue
            if stage == 1:
                for c in local:
                    c().wait()
            if stage == 6:
                keep().wait()
            for ref, j in lands[stage - 1]:
                arrived(ref, rr.at[q, j])
            if stage == 1:
                ra_v[q] += rl_v[s]
            if stage == 2:
                rm_v[q] += rb_v[q, 0] + rb_v[q, 1]
            if stage == 3:
                ra2_v[q, 0] += rm_v[q, sub(p2 + 1), lo]
                ra2_v[q, 1] += rm_v[q, sub(p2 - 1), hi]
            if stage == 4:
                gu = rm_v[q, sub(p2), :] + (rb2_v[q, 0] + rb2_v[q, 1])
                xr = rh_v[q].astype(F32)
                inv = lax.rsqrt(jnp.mean(xr * xr, axis=-1, keepdims=True) + NORM_EPS)
                normed = xr * inv
                gn = gu * (gain_m, gain_t)[h][...]
                gx = inv * (gn - normed * jnp.mean(gn * normed, axis=-1, keepdims=True))
                rm_v[q, sub(p2), :] = gx.astype(BF16).astype(F32)
                part = jnp.sum(gu * normed, axis=0, keepdims=True)
                if s == 0:
                    gg_v[h:h + 1, :] = part
                else:
                    gg_v[h:h + 1, :] += part
                keep().start()
            if stage < 8:
                for c in sends[stage]:
                    c().start()

    def narrow(h):
        r = pl.ds(h * seq, seq)
        c = pltpu.make_async_copy(gh.at[r, :], acc_v, sem_a.at[0])
        c.start()
        c.wait()
        u_v[r, :] = acc_v[...].astype(BF16)
        pltpu.make_async_copy(u_v.at[r, :], ghb.at[r, :], sem_u.at[0, h]).start()

    def g_copy(d):
        return remote(gg_v, gland.at[tp], g_s.at[d], g_r.at[tp], {"tp": lax.rem(tp + d, n_tp), "dp": dp})

    def t_copy(d):
        return remote(tsend, tland.at[dp], t_s.at[d], t_r.at[dp], {"tp": tp, "dp": lax.rem(dp + d, n_dp)})

    def gains(stage):
        if stage == 0:
            gland[tp] = gg_v[...]
            for d in range(1, n_tp):
                g_copy(d).start()
        if stage == 1:
            for d in range(1, n_tp):
                src = lax.rem(tp + d, n_tp)
                arrived(gland.at[src], g_r.at[src])
            total = gland[0]
            for d in range(1, n_tp):
                total = total + gland[d]
            total = jnp.concatenate([total, jnp.broadcast_to(lpart[0:1, 0:1], total.shape)])
            tsend[...] = total
            tland[dp] = total
            for d in range(1, n_dp):
                t_copy(d).start()
        if stage == 2:
            for d in range(1, n_dp):
                src = lax.rem(dp + d, n_dp)
                arrived(tland.at[src], t_r.at[src])
            total = tland[0]
            for d in range(1, n_dp):
                total = total + tland[d]
            tot[...] = total

    gg_v[...] = jnp.zeros_like(gg_v)

    def where(k):
        return (0, first) if isinstance(k, int) and k == 0 else (start(k), wide)

    def drain():
        for h in range(2):
            for s in range(2):
                for cs in ring(h, s)[3].values():
                    for c in cs:
                        c().wait_send()
        for d in range(1, n_tp):
            g_copy(d).wait_send()
        for d in range(1, n_dp):
            t_copy(d).wait_send()
        for k in range(n):
            c0, width = where(k)
            if k < n - 1:
                f_copy(k, c0, width).wait()
                o_copy(k, c0, width).wait()
            for which in range(2):
                b_copy(k, c0, width, which).wait_send()
            if k >= n - 1:
                for part in range(2):
                    d_copy(k, c0, width, part).wait_send()

    def act(what, *args):
        with jax.named_scope(what + "".join(str(a) for a in args)):
            {"ring": event, "sums": gains, "narrow": narrow, "drain": drain, "add": lambda k: add(k, *where(k)), "close": lambda k: close(k, *where(k))}[what](*args)

    def pick(table, k, default):
        out = jnp.int32(default)
        for at_k, value in table.items():
            out = jnp.where(k == at_k, value, out)
        return out

    def at_point(k, point):
        for (at_k, at_p), todo in plan["acts"].items():
            if at_p == point:
                @pl.when(k == at_k)
                def _():
                    for a in todo:
                        act(*a)

    def more_loads():
        for c in u_copies(0):
            c.start()
        fetch(start(1), wide, 1)
        for c in acc_copies(0, False):
            c.start()

    def before_sends():
        u_wait(0)
        with jax.named_scope('meet'):
            met()

    with jax.named_scope('make0'):
        make(0, 0, first, 0, more_loads, lambda: u_wait(1), before_sends)
    add(0, 0, first)

    @pl.loop(1, n + 1)
    def _(k):
        lo_t = pick({a: v[0] for a, v in plan["du"].items()}, k, 2 * per)
        hi_t = pick({a: v[1] for a, v in plan["du"].items()}, k, 2 * per)
        before = pick(plan["before"], k, 2 * per)
        slot = lax.rem(k + before, 2)

        @pl.when(hi_t > lo_t)
        def _():
            du_fetch(lo_t, 1 - slot)

        @pl.when((hi_t == lo_t) & (k < n))
        def _():
            fetch(start(k + 1), wide, 1 - slot)

        @pl.when(k == 2)
        def _():
            for part in range(2):
                d_copy(0, 0, first, part).wait_send()

        @pl.when(k > 2)
        def _():
            for part in range(2):
                d_copy(k - 2, start(k - 2), wide, part).wait_send()

        with jax.named_scope('make'):
            make(k, start(k), wide, slot, middle=lambda: at_point(k, "middle"))

        @pl.when(k < n)
        def _():
            add(k, start(k), wide)

        at_point(k, "add")
        with jax.named_scope('du_run'):
            du_run(k, lo_t, hi_t)
        at_point(k, "du")
        done = pick(plan["close"], k, -1)

        @pl.when(done == 0)
        def _():
            close(0, 0, first)

        @pl.when(done > 0)
        def _():
            close(done, start(done), wide)

        at_point(k, "close")

    for a in plan["tail"]:
        act(*a)
    tail = jax.named_scope('tail')
    tail.__enter__()
    for k in (n - 1, n):
        c0, width = where(k)
        f_copy(k, c0, width).wait()
        o_copy(k, c0, width).wait()
    for which in range(2):
        b_copy(n, start(n), wide, which).wait_send()
    for part in range(2):
        d_copy(n, start(n), wide, part).wait_send()
    for h in range(2):
        r = pl.ds(h * seq, seq)
        pltpu.make_async_copy(u_v.at[r, :], ghb.at[r, :], sem_u.at[0, h]).wait()
    tail.__exit__(None, None, None)


PLAN = {
    "du": {2: (0, 8), 3: (8, 12), 4: (12, 16)},
    "before": {1: 0, 2: 0, 3: 8, 4: 12},
    "close": {2: 0, 3: 1, 4: 2, 5: 3, 7: 4},
    "acts": {
        (2, "du"): [("ring", 0, 0)], (3, "du"): [("ring", 0, 1)], (4, "add"): [("ring", 0, 2)], (14, "task"): [("ring", 0, 3)],
        (4, "du"): [("ring", 0, 4), ("ring", 1, 0)], (5, "middle"): [("ring", 0, 5)],
        (6, "middle"): [("ring", 1, 1), ("ring", 0, 6)], (7, "middle"): [("ring", 1, 2)], (7, "add"): [("ring", 1, 3)],
        (8, "middle"): [("ring", 1, 4)], (8, "add"): [("ring", 0, 7), ("ring", 1, 5)],
    },
    "tail": [("close", 5), ("sums", 0), ("ring", 1, 6), ("close", 6), ("sums", 1), ("add", 8), ("ring", 0, 8), ("narrow", 0), ("ring", 1, 7),
             ("close", 7), ("ring", 1, 8), ("narrow", 1), ("sums", 2), ("drain",), ("close", 8)],
}


def head_grad(n_tp, n_dp, hm, ht, gain_m, gain_t, u_own, u_par, z, w, st, du_in, lpart):
    rows, depth = u_own.shape
    vocab = z.shape[1]
    first, wide, task = 128, 384, 512
    half = vocab // 2
    n = (half - first) // wide + 1
    dma = pltpu.SemaphoreType.DMA
    return pl.pallas_call(
        functools.partial(head_kernel, n_tp, n_dp, first, wide, task, LEFT, PLAN),
        out_shape=(
            jax.ShapeDtypeStruct((2, half, 256), F32),
            jax.ShapeDtypeStruct((rows, depth), F32),
            jax.ShapeDtypeStruct((rows, depth), BF16),
            jax.ShapeDtypeStruct((rows, depth), F32),
            jax.ShapeDtypeStruct((4, depth), F32),
        ),
        in_specs=[ANY, ANY, VMEM, VMEM, ANY, ANY, ANY, ANY, VMEM, ANY, VMEM],
        out_specs=(ANY, ANY, ANY, ANY, VMEM),
        scratch_shapes=[
            pltpu.VMEM((2 * rows, depth), BF16),
            pltpu.VMEM((2, depth, task), BF16),
            pltpu.VMEM((2, rows, task), F32),
            pltpu.VMEM((wide, 2 * rows), BF16),
            pltpu.VMEM((2, wide, 1024), F32),
            pltpu.VMEM((wide, 1024), F32),
            pltpu.VMEM((half, 1024), F32),
            pltpu.VMEM((2, half, 256), F32),
            pltpu.VMEM((rows // 2, depth), F32),
            pltpu.VMEM((rows // 2, task), BF16),
            pltpu.VMEM((2 * rows, 128), F32),
            pltpu.VMEM((2 * rows, 128), F32),
            pltpu.VMEM((2 * rows, 128), F32),
            pltpu.VMEM((4, 2, 64, depth // 2), F32),
            pltpu.VMEM((2, 2, 64, depth // 2), F32),
            pltpu.VMEM((4, 2, 64, depth), F32),
            pltpu.VMEM((4, 64, depth), F32),
            pltpu.VMEM((4, 2, 16, depth // 2), F32),
            pltpu.VMEM((4, 2, 16, depth), F32),
            pltpu.VMEM((4, 16, depth), BF16),
            pltpu.VMEM((2, depth), F32),
            pltpu.VMEM((n_tp, 2, depth), F32),
            pltpu.VMEM((n_dp, 4, depth), F32),
            pltpu.VMEM((4, depth), F32),
            dma((2, 8)), dma, dma((2, 8)), dma((2,)), dma((8,)), dma((n,)),
            dma((2, 2)), dma((n, 2)), dma((2 * n,)), dma((2 * n,)), dma((n,)), dma((n,)),
            dma((4, 20)), dma((4, 20)), dma((4, 4)), dma((4,)), dma((n_tp,)), dma((n_tp,)), dma((n_dp,)), dma((n_dp,)),
        ],
        compiler_params=pltpu.CompilerParams(vmem_limit_bytes=67043328, collective_id=1, has_side_effects=True),
        cost_estimate=pl.CostEstimate(flops=300 * 10**9, bytes_accessed=2 * depth * vocab, transcendentals=0),
        name="head_grad",
    )(hm, ht, gain_m, gain_t, u_own, u_par, z, w, st, du_in, lpart)


def finish_kernel(span, fin, gh, tot, out, gm, gt, loss, ggm, ggt, f_v, o_v, g_v, sem_f, sem_o, sem_g, sem_b):
    half = fin.shape[1]
    seq = gm.shape[0]
    side = Torus().side
    nf, ng = 2 * half // span, gh.shape[0] // 128

    def f_in(i):
        k, j = divmod(i, half // span)
        return pltpu.make_async_copy(fin.at[k, pl.ds(j * span, span), :], f_v.at[i], sem_f.at[i])

    def f_out(i):
        k, j = divmod(i, half // span)
        col = (side if k == 0 else 1 - side) * half + j * span
        return pltpu.make_async_copy(o_v.at[i], out.at[:, ds(col, span, 128)], sem_o.at[i])

    def g_in(i):
        return pltpu.make_async_copy(gh.at[pl.ds(i * 128, 128), :], g_v.at[i], sem_g.at[i])

    def g_out(i):
        dst = (gm, gt)[i * 128 // seq]
        return pltpu.make_async_copy(g_v.at[i], dst.at[pl.ds(i * 128 % seq, 128), :], sem_b.at[i])

    for i in range(nf):
        f_in(i).start()
    for i in range(ng):
        g_in(i).start()
    loss[...] = tot[2:3, 0:1]
    ggm[...] = tot[0:1, :]
    ggt[...] = tot[1:2, :]
    for i in range(nf):
        f_in(i).wait()
        o_v[i] = f_v[i].T
        f_out(i).start()
    for i in range(ng):
        g_in(i).wait()
        g_out(i).start()
    for i in range(nf):
        f_out(i).wait()
    for i in range(ng):
        g_out(i).wait()


def finish(fin, gh, tot):
    _, half, block = fin.shape
    rows, depth = gh.shape
    span = 640
    nf, ng = 2 * half // span, rows // 128
    dma = pltpu.SemaphoreType.DMA
    return pl.pallas_call(
        functools.partial(finish_kernel, span),
        out_shape=(
            jax.ShapeDtypeStruct((block, 2 * half), F32),
            jax.ShapeDtypeStruct((rows // 2, depth), BF16),
            jax.ShapeDtypeStruct((rows // 2, depth), BF16),
            jax.ShapeDtypeStruct((1, 1), F32),
            jax.ShapeDtypeStruct((1, depth), F32),
            jax.ShapeDtypeStruct((1, depth), F32),
        ),
        in_specs=[ANY, ANY, VMEM],
        out_specs=(ANY, ANY, ANY, VMEM, VMEM, VMEM),
        scratch_shapes=[
            pltpu.VMEM((nf, span, block), F32),
            pltpu.VMEM((nf, block, span), F32),
            pltpu.VMEM((ng, 128, depth), BF16),
            dma((nf,)), dma((nf,)), dma((ng,)), dma((ng,)),
        ],
        compiler_params=pltpu.CompilerParams(vmem_limit_bytes=62 * 2**20),
        name="finish",
    )(fin, gh, tot)


def solution(mesh):
    n_tp, n_dp = mesh.shape["tp"], mesh.shape["dp"]

    def local_step(h_main, h_mtp, labels_main, labels_mtp, weight_main, weight_mtp, gain_final, gain_mtp, w_out):
        hm, ht = h_main[0], h_mtp[0]
        gm, gt = gain_final[None], gain_mtp[None]
        z, u_own, u_par, du_in, st, lpart = logits(n_tp, n_dp, hm, ht, gm, gt, labels_main, labels_mtp, weight_main, weight_mtp, w_out)
        fin, _, gh, _, tot = head_grad(n_tp, n_dp, hm, ht, gm, gt, u_own, u_par, z, w_out, st, du_in, lpart)
        grad_w, gh_m, gh_t, loss, gg_m, gg_t = finish(fin, gh, tot)
        return loss[0, 0], gh_m[None], gh_t[None], grad_w, gg_m[0], gg_t[0]

    row_spec = P("dp", None)
    return jax.shard_map(
        local_step,
        mesh=mesh,
        in_specs=(P("dp", None, None), P("dp", None, None), row_spec, row_spec, row_spec, row_spec, P(None), P(None), P(None, "tp")),
        out_specs=(P(), P("dp", None, None), P("dp", None, None), P("dp", "tp"), P(None), P(None)),
        check_vma=False,
    )
```

```python
import functools

import jax
import jax.numpy as jnp
from jax import lax
from jax.experimental import pallas as pl
from jax.experimental.pallas import tpu as pltpu
from jax.sharding import PartitionSpec as P

NORM_EPS = 1e-6
MTP_LAMBDA = 0.3
F32, BF16 = jnp.float32, jnp.bfloat16
DMA = pltpu.SemaphoreType.DMA
TWO = DMA((2,))
ANY = pl.BlockSpec(memory_space=pl.ANY)
VMEM = pl.BlockSpec(memory_space=pltpu.VMEM)
VMEM_LIMIT = 67043328
WINDOW = 9
LANES, FEATS = 128, 256
RING = 4
WAYS = (1, -1)
BOTH = range(2)
NT = (((1,), (1,)), ((), ()))
CHUNK = 1280
LEFT = 4096
SLICE = 24
SPREAD = 2 * RING * RING * SLICE
FIRST, WIDE = 128, 384
TASK = 512
KINDS = "nnnnnsnsn"
DONE = (0, 5, 8, 16) + 5 * (20,)
ACTS = ("1a:f2,a1", "2t:L0", "3t:f3", "4t:C0", "2a:a2", "2d:L1,r00,u0", "3m:f4", "9t:a3,C1", "13t:L2,r01", "14t:C2", "3d:f5,r10,u1",
        "4m:r02", "18t:L3,a4", "19t:C3,r03", "4d:r11", "5m:r04", "5a:a5", "6m:r12,r05", "6a:a6", "7m:r13,r06", "7a:a7,r14,L4,g0")
TAIL = ("a8,C4,L5,r15,g1,C5,L6,C6,r16,r07,p70,q70,p71,q71,p80,q80", "p81,q81,r17,g2,r08,n,r18,z")


def ds(start, size, unit=8):
    return pl.ds(pl.multiple_of(start, unit), size)


def mod(p):
    return lax.rem(p + RING, RING)


def upto(n):
    return pl.ds(0, n)


def halves(n):
    return upto(n // 2), pl.ds(n // 2, n // 2)


def columns(row):
    return jnp.broadcast_to(row, (LANES, row.shape[1])).T


def near(src, dst, sem):
    return pltpu.make_async_copy(src, dst, sem)


def remote(src, dst, send, recv, to):
    return pltpu.make_async_remote_copy(src, dst, send, recv, device_id=to, device_id_type=pl.DeviceIdType.MESH)


def arrived(ref, sem):
    near(ref, ref, sem).wait()


def begin(copies):
    for c in copies:
        c.start()


def dot(a, b):
    return jnp.dot(a, b, preferred_element_type=F32)


def grad_logits(z, lse, rw, lab, col):
    lane = lax.broadcasted_iota(jnp.int32, z.shape, 1).astype(F32)
    p = jnp.exp(z - lse)
    return rw * jnp.where(lab - col == lane, p - 1.0, p)


class Torus:
    def __init__(self):
        self.tp, self.dp = lax.axis_index("tp"), lax.axis_index("dp")
        self.y, self.z = lax.rem(self.tp, RING), self.tp // RING
        self.x, self.core = self.dp // 2, lax.rem(self.dp, 2)
        self.mate = self.x + 1 - 2 * lax.rem(self.x, 2)
        self.far = RING - 1 - self.x
        self.opposite = RING - 1 - self.mate

    def side(self, swapped):
        return self.x // 2 if swapped else lax.rem((self.x + 1) // 2, 2)

    def chip(self, x, core=None):
        return {"tp": self.tp, "dp": 2 * x + (self.core if core is None else core)}

    def step(self, axis, d):
        y, z = (mod(self.y + d), self.z) if axis == 0 else (self.y, mod(self.z + d))
        return {"tp": z * RING + y, "dp": self.dp}

    def rings(self, s):
        ways = [functools.partial(self.step, a) for a in BOTH]
        return (self.y, ways[0], self.z, ways[1]) if s == 0 else (self.z, ways[1], self.y, ways[0])

    def others(self, axis):
        n, me = (lax.axis_size(axis), lax.axis_index(axis))
        return [{"tp": self.tp, "dp": self.dp, axis: lax.rem(me + d, n)} for d in range(1, n)]

    def greet(self):
        barrier = pltpu.get_barrier_semaphore()
        peers = self.others("tp") + self.others("dp")
        for peer in peers:
            pl.semaphore_signal(barrier, inc=1, device_id=peer, device_id_type=pl.DeviceIdType.MESH)
        return lambda: pl.semaphore_wait(barrier, len(peers))


class Exchange:
    def __init__(self, here, axis, src, land, send, recv):
        self.land, self.recv = land, recv
        me = lax.axis_index(axis)
        self.copies = lambda: [remote(src, land.at[me], send, recv, to) for to in here.others(axis)]
        self.rest = land.at[pl.ds(1, lax.axis_size(axis) - 1)]
        self.send, self.me = send, me

    def start(self, own):
        self.land[self.me] = own
        begin(self.copies())

    def blocks(self):
        arrived(self.rest, self.recv)
        return [self.land[i] for i in range(self.land.shape[0])]

    def drain(self):
        arrived(self.rest, self.send)


class Gather:
    def __init__(self, ref, rows, lanes, to, send, recv, own=None):
        self.ref, self.rows, self.to, self.send, self.recv = ref, rows, to, send, recv
        self.lanes = lanes
        self.own = ref.at[rows(0), lanes] if own is None else own
        self.size = rows(0).size

    def spread(self):
        dst = self.ref.at[self.rows(0), self.lanes]
        begin([remote(self.own, dst, self.send, self.recv.at[0], self.to(d)) for d in WAYS])

    def pass_on(self):
        arrived(self.ref.at[upto(2 * self.size), self.lanes], self.recv.at[0])
        n = self.lanes.size // 2
        for i, d in enumerate(WAYS):
            part = self.ref.at[self.rows(-d), pl.ds(self.lanes.start + i * n, n)]
            remote(part, part, self.send, self.recv.at[1], self.to(d)).start()

    def end(self):
        arrived(self.ref.at[upto(self.size), self.lanes], self.recv.at[1])


class Scatter:
    def __init__(self, src, rows, to, from_a, from_b, send, recv):
        self.src, self.rows, self.to, self.a, self.b, self.send, self.recv = src, rows, to, from_a, from_b, send, recv
        self.lanes = halves(src.shape[-1])

    def start(self):
        for i, d in enumerate(WAYS):
            remote(self.src.at[self.rows(2), self.lanes[i]], self.a.at[i], self.send, self.recv.at[0], self.to(d)).start()

    def rest(self):
        for i, d in enumerate(WAYS):
            other = self.lanes[1 - i]
            remote(self.src.at[self.rows(d), other], self.b.at[i, :, other], self.send, self.recv.at[1], self.to(d)).start()

    def middle(self, own):
        arrived(self.a, self.recv.at[0])
        for i, d in enumerate(WAYS):
            self.a[i] += own(i, d)
            remote(self.a.at[i], self.b.at[i, :, self.lanes[i]], self.send, self.recv.at[1], self.to(d)).start()

    def end(self):
        arrived(self.b, self.recv.at[1])


def slices(here, s):
    p1, _, p2, _ = here.rings(s)
    base = s * (SPREAD // 2)
    return (lambda o: ds(base + (p2 * RING + mod(p1 + o)) * SLICE, SLICE)), (lambda o: ds(base + mod(p2 + o) * RING * SLICE, RING * SLICE))


def plane_gather(here, ref, s, send, recv):
    _, to1, _, to2 = here.rings(s)
    one, many = slices(here, s)
    depth = ref.shape[-1]
    a = Gather(ref, one, upto(depth), to1, send.at[s], recv.at[s, 0])
    b, c = [Gather(ref, many, lanes, to2, send.at[s], recv.at[s, i + 1]) for i, lanes in enumerate(halves(depth))]

    def turn():
        a.end()
        b.spread()

    def end():
        b.end()
        c.end()

    def drain():
        arrived(ref.at[upto(3 * (RING + 1) * SLICE), :], send.at[s])

    return [a.spread, a.pass_on, turn, c.spread, b.pass_on, c.pass_on, end, drain]


def logits_kernel(hm, ht, gain_m, gain_t, lab_m, lab_t, wt_m, wt_t, w, z, u_out, up_out, far_u, du_out, st, lpart,
                  h_v, u_v, uf_v, got_v, w_v, z_v, e_v, x_v, m_v, s_v, t_v, lab_v, send_v, land, wsend, wland, pack,
                  sem_h, sem_u, sem_w, sem_z, sem_d, sem_k, es, er, ps, pr, gs, gr, xs, xr):
    seq, depth = hm.shape
    rows, vocab = z.shape
    steps = vocab // CHUNK
    here = Torus()
    mate, far = here.chip(here.mate), here.chip(here.far)

    def w_copy(i, slot):
        return near(w.at[:, ds(i * CHUNK, CHUNK, LANES)], w_v.at[slot], sem_w.at[slot])

    def z_copy(i, slot):
        return near(z_v.at[slot], z.at[:, ds(i * CHUNK, CHUNK, LANES)], sem_z.at[slot])

    loads = [near(src, h_v.at[pl.ds(i * seq, seq), :], sem_h.at[i]) for i, src in enumerate((hm, ht))]
    begin(loads + [w_copy(0, 0)])
    met = here.greet()
    m_v[:] = jnp.full_like(m_v, -jnp.inf)
    s_v[:] = jnp.zeros_like(s_v)
    t_v[:] = jnp.zeros_like(t_v)
    lab = jnp.concatenate([lab_m[:], lab_t[:]], axis=1).astype(F32) - (here.tp * vocab).astype(F32)
    lab_v[:] = columns(lab)
    top_row = lax.broadcasted_iota(jnp.int32, wsend.shape, 0) == 0
    wsend[:] = jnp.where(top_row, jnp.sum(wt_m[:]), jnp.sum(wt_t[:]))

    for half, gain in enumerate((gain_m, gain_t)):
        loads[half].wait()
        g = gain[:]

        @pl.loop(0, seq // LANES)
        def _(i):
            r = ds(half * seq + i * LANES, LANES)
            x = h_v[r, :].astype(F32)
            inv = lax.rsqrt(jnp.mean(x * x, axis=-1, keepdims=True) + NORM_EPS)
            u = (x * inv * g).astype(BF16)
            u_v[r, :] = u
            uf_v[r, :] = u.astype(F32)

    u_copy = near(u_v, u_out, sem_u)
    u_copy.start()
    with jax.named_scope("meet"):
        met()

    weights = Exchange(here, "dp", wsend, wland, es.at[0], er.at[0])
    weights.start(wsend[:])
    rest = pl.ds(SPREAD, rows - SPREAD)
    parts = [slices(here, s)[0](0) for s in BOTH] + [rest]

    def fetched(k, i):
        return remote(uf_v.at[parts[i], :], (got_v, far_u)[k].at[parts[i], :], xs.at[k, i], xr.at[k, i], (mate, far)[k])

    begin([fetched(k, i) for i in range(3) for k in BOTH])
    spread = [plane_gather(here, got_v, s, gs, gr) for s in BOTH]
    lane = lax.broadcasted_iota(jnp.int32, (rows, LANES), 1).astype(F32)

    @pl.loop(0, steps)
    def _(i):
        slot = lax.rem(i, 2)
        w_copy(i, slot).wait()

        @pl.when(i + 1 < steps)
        def _():
            w_copy(i + 1, 1 - slot).start()

        @pl.when(i >= 2)
        def _():
            z_copy(i - 2, slot).wait()

        m, s, t = m_v[:], s_v[:], t_v[:]
        rel = lab_v[:] - (i * CHUNK).astype(F32)
        for n in range(0, CHUNK, FEATS):
            for which, at in enumerate((0, 3 * FEATS)):
                for stage in range(3):
                    if n == at:
                        @pl.when(i == stage + 1)
                        def _():
                            if stage == 0:
                                arrived(got_v.at[parts[which], :], xr.at[0, which])
                            spread[which][stage]()
            zz = dot(u_v[:], w_v[slot, :, n:n + FEATS])
            z_v[slot, :, n:n + FEATS] = zz
            za, zb = zz[:, :LANES], zz[:, LANES:]
            new = jnp.maximum(m, jnp.maximum(za, zb))
            s = s * jnp.exp(m - new) + (jnp.exp(za - new) + jnp.exp(zb - new))
            t = jnp.where(rel == lane + n, za, t)
            t = jnp.where(rel == lane + (n + LANES), zb, t)
            m = new
        m_v[:], s_v[:], t_v[:] = m, s, t
        z_copy(i, slot).start()

    mt = m_v[:].T
    top = jnp.max(mt, axis=0, keepdims=True)
    total = jnp.sum(s_v[:].T * jnp.exp(mt - top), axis=0, keepdims=True)
    hit = jnp.sum(t_v[:].T, axis=0, keepdims=True)
    send_v[:] = jnp.where(lax.broadcasted_iota(jnp.int32, send_v.shape, 0) == 0, top + jnp.log(total), hit)
    stats = Exchange(here, "tp", send_v, land, es.at[1], er.at[1])
    stats.start(send_v[:])
    for stage in (3, 4):
        for which in BOTH:
            spread[which][stage]()
    sums = functools.reduce(jnp.add, weights.blocks())
    rw = jnp.concatenate([wt_m[:] * (1.0 / sums[0:1, 0:1]), wt_t[:] * (MTP_LAMBDA / sums[1:2, 0:1])], axis=1)
    with jax.named_scope("statwait"):
        blocks = stats.blocks()
    top = functools.reduce(jnp.maximum, blocks)
    lse = (top + jnp.log(functools.reduce(jnp.add, [jnp.exp(b - top) for b in blocks])))[0:1, :]
    hit = functools.reduce(jnp.add, blocks)[1:2, :]
    lpart[:] = jnp.broadcast_to(jnp.sum(rw * (lse - hit)), lpart.shape)
    row = lax.broadcasted_iota(jnp.int32, st.shape[1:], 0)
    st[1] = jnp.where(row == 0, lse, jnp.where(row == 1, rw, lab))
    pack[:] = st[1]
    swaps = [remote(pack, st.at[2 * k], ps.at[k], pr.at[k], to) for k, to in enumerate((mate, far))]
    begin(swaps)
    m_v[:] = columns(lse)
    s_v[:] = columns(rw)
    skip = LEFT - (steps - 2) * CHUNK
    at = 0
    for step, start in ((steps - 1, 0), (steps - 2, skip)):
        for c in range(start, CHUNK, LANES):
            e_v[:, at:at + LANES] = grad_logits(
                z_v[step % 2, :, c:c + LANES], m_v[:], s_v[:], lab_v[:], float(step * CHUNK + c)).astype(BF16)
            at += LANES

    def e_dot(r, cols):
        return (lax.dot_general(e_v[r, :CHUNK], w_v[(steps - 1) % 2, cols, :], NT, preferred_element_type=F32)
                + lax.dot_general(e_v[r, CHUNK:], w_v[(steps - 2) % 2, cols, skip:], NT, preferred_element_type=F32))

    for i in BOTH:
        for k in BOTH:
            fetched(k, i).wait_send()
    saves = []
    for dst, r in ((uf_v, slice(0, SPREAD)), (x_v, slice(SPREAD, rows))):
        for n in range(0, depth, TASK):
            dst[:r.stop - r.start, n:n + TASK] = e_dot(r, slice(n, n + TASK))
            src = dst.at[upto(r.stop - r.start), pl.ds(n, TASK)]
            saves.append(near(src, du_out.at[pl.ds(r.start, r.stop - r.start), pl.ds(n, TASK)], sem_d.at[len(saves)]))
            saves[-1].start()
            if len(saves) in (2, 3):
                spread[len(saves) - 2][5]()
    u_copy.wait()
    waits = [spread[0][6], spread[1][6], lambda: arrived(got_v.at[rest, :], xr.at[0, 2])]
    for i, wait in enumerate(waits):
        start = i * (SPREAD // 2)
        r = pl.ds(start, min(SPREAD // 2, rows - start))
        with jax.named_scope("land"):
            wait()

        @pl.loop(start // LANES, (start + r.size) // LANES)
        def _(j):
            part = ds(j * LANES, LANES)
            u_v[part, :] = got_v[part, :].astype(BF16)

        saves.append(near(u_v.at[r, :], up_out.at[r, :], sem_k.at[i]))
        saves[-1].start()
    for c in swaps:
        c.wait()
    for i in range(3):
        arrived(far_u.at[parts[i], :], xr.at[1, i])
    weights.drain()
    stats.drain()
    for k in BOTH:
        spread[k][7]()
        fetched(k, 2).wait_send()
        z_copy(steps - 2 + k, (steps + k) % 2).wait()
    for c in saves:
        c.wait()


def logits(hm, ht, gain_m, gain_t, lab_m, lab_t, wt_m, wt_t, w):
    seq, depth = hm.shape
    rows, vocab = 2 * seq, w.shape[1]
    n_tp, n_dp = lax.axis_size("tp"), lax.axis_size("dp")
    shape = jax.ShapeDtypeStruct
    stat = pltpu.VMEM((rows, LANES), F32)
    return pl.pallas_call(
        logits_kernel,
        out_shape=(shape((rows, vocab), F32), shape((rows, depth), BF16), shape((rows, depth), BF16), shape((rows, depth), F32),
                   shape((rows, depth), F32), shape((3, 8, rows), F32), shape((8, LANES), F32)),
        in_specs=[ANY, ANY] + [VMEM] * 6 + [ANY],
        out_specs=(ANY,) * 5 + (VMEM, VMEM),
        scratch_shapes=[
            pltpu.VMEM((rows, depth), BF16), pltpu.VMEM((rows, depth), BF16), pltpu.VMEM((rows, depth), F32), pltpu.VMEM((rows, depth), F32),
            pltpu.VMEM((2, depth, CHUNK), BF16), pltpu.VMEM((2, rows, CHUNK), F32), pltpu.VMEM((rows, vocab - LEFT), BF16),
            pltpu.VMEM((rows - SPREAD, depth), F32), stat, stat, stat, stat,
            pltpu.VMEM((2, rows), F32), pltpu.VMEM((n_tp, 2, rows), F32), pltpu.VMEM((8, LANES), F32), pltpu.VMEM((n_dp, 8, LANES), F32),
            pltpu.VMEM((8, rows), F32),
            TWO, DMA, TWO, TWO, DMA((2 * depth // TASK,)), DMA((3,)), TWO, TWO, TWO, TWO,
            TWO, DMA((2, 3, 2)), *[DMA((2, 3))] * 2,
        ],
        compiler_params=pltpu.CompilerParams(vmem_limit_bytes=VMEM_LIMIT, collective_id=0, has_side_effects=True),
        name="logits",
    )(hm, ht, gain_m, gain_t, lab_m, lab_t, wt_m, wt_t, w)


def chunk_table():
    out, at, used = [], 0, [0, 0]
    for i, kind in enumerate(KINDS):
        width, swapped = (WIDE if i else FIRST), int(kind == "s")
        out.append((at, width, swapped, used[swapped]))
        at, used[swapped] = at + width, used[swapped] + width
    return out, used


def column(here, used, swapped, other, offset):
    base = [2 * used[0] * s + abs(here.side(s) - other) * used[s] for s in BOTH]
    return jnp.where(swapped == 1, base[1], base[0]) + offset


def pick(values, k):
    if isinstance(k, int):
        return values[k]
    return functools.reduce(lambda out, i: jnp.where(k == i, values[i], out), range(1, len(values)), jnp.int32(values[0]))


def head_kernel(hm, ht, gain_m, gain_t, u_own, u_par, far_in, z, w, st, du_in, lpart,
                fin, gh, ghb, du, far_u, one, tot, u_v, w_v, z_v, et_v, g_v, own_v, sum_v, one_v, acc_v,
                lse_v, rw_v, lab_v, ra_v, rl_v, rb_v, rm_v, ra2_v, rb2_v, rh_v, gg_v, gland, tland, tsend,
                sem_u, sem_w, sem_z, sem_a, sem_o, sem_1, d_send, d_recv, b_send, b_recv, f_send, f_recv,
                gs, gr, ss, sr, sem_l, sem_x, es, er):
    del far_in
    rows, depth = u_own.shape
    seq = rows // 2
    here = Torus()
    x, core = here.x, here.core
    met = here.greet()
    table, used = chunk_table()
    starts, _, swaps, offsets = (list(t) for t in zip(*table))
    last = len(table) - 1

    def span(k):
        return upto(FIRST) if isinstance(k, int) and k == 0 else ds(FIRST + (k - 1) * WIDE, WIDE, LANES)

    def chips(k):
        s = pick(swaps, k) == 1
        return jnp.where(s, here.far, here.mate), jnp.where(s, here.mate, here.far)

    def block(i):
        return ds((2 * lax.rem(i, RING) + jnp.where(i < RING, 1 - core, core)) * FEATS, FEATS, FEATS)

    def feats(i):
        return pl.ds(i * FEATS, FEATS)

    def w_copies(col, width, slot):
        return [near(w.at[block(i), ds(col, width, LANES)], w_v.at[slot, feats(i), upto(width)], sem_w.at[slot]) for i in range(2 * RING)]

    def u_copies(k):
        src, r = ((u_par, upto(rows)), (u_own, pl.ds(rows, rows)))[k]
        return [near(src.at[:, block(i)], u_v.at[r, feats(i)], sem_u.at[k]) for i in range(2 * RING)]

    def u_wait(k):
        arrived(u_v.at[upto(rows), :], sem_u.at[k])

    def fetch(k, slot):
        width = span(k).size
        col = column(here, used, pick(swaps, k), 0, pick(offsets, k))
        begin(w_copies(col, width, slot) + [near(z.at[:, ds(col, width, LANES)], z_v.at[slot, :, upto(width)], sem_z.at[slot])])

    per = LEFT // TASK

    def piece(t):
        return t < 2 * per, t // per, lax.rem(t, per)

    def acc_copies(h, back):
        refs = [(acc_v.at[:, feats(i)], (du if back else du_in).at[ds(h * seq, seq), block(i)]) for i in range(2 * RING)]
        return [near(*(p if back else p[::-1]), sem_a) for p in refs]

    def task_fetch(t, slot):
        of_du, h, i = piece(t)

        @pl.when(of_du)
        def _():
            begin(w_copies(i * TASK, TASK, slot))
            near(z.at[ds(h * seq, seq), ds(i * TASK, TASK, LANES)], z_v.at[slot, upto(seq), :], sem_z.at[slot]).start()

        @pl.when(~of_du)
        def _():
            begin([near(far_u.at[:, block(2 * i + j)], z_v.at[slot, :, feats(j)], sem_z.at[slot]) for j in BOTH])

    def task(t, slot):
        of_du, h, i = piece(t)

        @pl.when(~of_du)
        def _():
            arrived(z_v.at[slot], sem_z.at[slot])
            u_v[pl.ds(2 * rows, rows), ds(i * TASK, TASK, LANES)] = z_v[slot].astype(BF16)

        @pl.when(of_du)
        def _():
            arrived(w_v.at[slot], sem_w.at[slot])
            arrived(z_v.at[slot, upto(seq), :], sem_z.at[slot])

            @pl.when(i == 0)
            def _():
                arrived(acc_v, sem_a)

            r = ds(rows + h * seq, seq)
            col = (i * TASK).astype(F32)
            for g in range(0, TASK, LANES):
                cols = slice(g, g + LANES)
                et_v[:, cols] = grad_logits(z_v[slot, :seq, cols], lse_v[r, :], rw_v[r, :], lab_v[r, :], col + g).astype(BF16)
            for m in range(0, depth, TASK):
                cols = slice(m, m + TASK)
                acc_v[:, cols] += lax.dot_general(et_v[:, :TASK], w_v[slot, cols, :], NT, preferred_element_type=F32)

            @pl.when(i == per - 1)
            def _():
                acc_v[:] = acc_v[:].astype(BF16).astype(F32)
                begin(acc_copies(h, True))
                arrived(acc_v, sem_a)

            @pl.when((i == per - 1) & (h == 0))
            def _():
                begin(acc_copies(1, False))

    def d_copy(k, part):
        lanes, width = pl.ds(part * TASK, TASK), span(k).size
        return remote(g_v.at[upto(width), lanes], sum_v.at[span(k), lanes], d_send, d_recv.at[k], here.chip(x, 1 - core))

    def b_copy(k, which):
        to = chips(k)[1]
        block_of = ds(jnp.where(which == 0, here.opposite, to) * FEATS, FEATS, FEATS)
        return remote(sum_v.at[span(k), block_of], one.at[which, span(k), :], b_send, b_recv.at[k, which], here.chip(to))

    def f_copy(k):
        mate = chips(k)[0]
        return remote(sum_v.at[span(k), ds(mate * FEATS, FEATS, FEATS)], fin.at[1, span(k), :], f_send, f_recv, here.chip(mate))

    def o_copy(k):
        return near(sum_v.at[span(k), ds(x * FEATS, FEATS, FEATS)], fin.at[0, span(k), :], sem_o)

    def make(k, slot, early=lambda: None, late=lambda: None, middle=lambda: None):
        width = span(k).size
        swapped = pick(swaps, k)
        col = column(here, used, swapped, 0, pick(offsets, k)).astype(F32)
        arrived(w_v.at[slot, :, upto(width)], sem_w.at[slot])
        arrived(z_v.at[slot, :, upto(width)], sem_z.at[slot])
        early()

        def put(zz, r, c, at):
            e = grad_logits(zz, lse_v[r, :], rw_v[r, :], lab_v[r, :], col + c)
            et_v[c:c + LANES, ds(at, rows, rows)] = e.T.astype(BF16)

        for c in range(0, width, LANES):
            put(z_v[slot, :, c:c + LANES], pl.ds(rows, rows), c, rows * (1 - swapped))
        late()
        other = ds(2 * rows * swapped, rows, rows)
        for n in range(0, width, FEATS):
            step = min(width - n, FEATS)
            zz = dot(u_v[other, :], w_v[slot, :, n:n + step])
            for c in range(0, step, LANES):
                put(zz[:, c:c + LANES], other, n + c, rows * swapped)
        middle()
        both = ds(rows * swapped, 2 * rows, rows)
        et = et_v[upto(width), :]
        for part in BOTH:
            lanes = pl.ds(part * TASK, TASK)
            g_v[upto(width), lanes] = dot(et, u_v[both, lanes])
            d_copy(k, part).start()
        own_v[upto(width), :] = dot(et, u_v[both, pl.ds(2 * TASK, 2 * TASK)])

    def add(k):
        arrived(sum_v.at[span(k), :], d_recv.at[k])
        sum_v[span(k), :] += own_v[upto(span(k).size), :]
        begin([b_copy(k, which) for which in BOTH])

    def landing(k, which):
        return near(one.at[which, span(k), :], one_v.at[which, upto(span(k).size), :], sem_1.at[which])

    def land(k, which):
        with jax.named_scope("bwait"):
            arrived(one.at[which, span(k), :], b_recv.at[k, which])
        landing(k, which).start()

    def close(k, which):
        landing(k, which).wait()
        chip = jnp.where(which == 0, chips(k)[0], x)
        sum_v[span(k), ds(chip * FEATS, FEATS, FEATS)] += one_v[which, upto(span(k).size), :]
        (o_copy if which else f_copy)(k).start()

    def ring(h, s):
        q = 2 * h + s
        p1, to1, p2, to2 = here.rings(s)
        big, small = seq // 2 // RING, seq // 2 // RING // RING
        base = h * seq + s * (seq // 2)
        one_of = lambda o: ds(base + mod(p1 + o) * big, big)
        two_of = lambda o: ds(base + p1 * big + mod(p2 + o) * small, small)
        sub = lambda o: ds(mod(p2 + o) * small, small)
        every = upto(depth)
        first = Scatter(du, one_of, to1, ra_v.at[q], rb_v.at[q], ss.at[q], sr.at[q, 0])
        second = Scatter(rm_v.at[q], sub, to2, ra2_v.at[q], rb2_v.at[q], ss.at[q], sr.at[q, 1])
        down = Gather(gh, two_of, every, to2, ss.at[q], sr.at[q, 2], rm_v.at[q, sub(0), :])
        up = Gather(gh, one_of, every, to1, ss.at[q], sr.at[q, 3])
        lanes = halves(depth)
        h_rows = ds(s * (seq // 2) + p1 * big + p2 * small, small)
        loads = lambda: [near(du.at[one_of(WAYS[i]), lanes[i]], rl_v.at[s, i], sem_l.at[s, i]) for i in BOTH] + [
            near(du.at[one_of(0), :], rm_v.at[q], sem_l.at[s, 2]), near((hm, ht)[h].at[h_rows, :], rh_v.at[q], sem_l.at[s, 3])]
        keep = lambda: near(rm_v.at[q, sub(0), :], gh.at[two_of(0), :], sem_x.at[q])
        return q, sub, lanes, first, second, down, up, loads, keep

    def event(h, stage):
        for s in BOTH:
            q, sub, lanes, first, second, down, up, loads, keep = ring(h, s)
            if stage == 0:
                first.start()
                begin(loads())
            if stage == 1:
                for c in loads():
                    c.wait()
                first.middle(lambda i, d: rl_v[s, i])
            if stage == 2:
                first.end()
                rm_v[q] += rb_v[q, 0] + rb_v[q, 1]
                second.start()
                second.rest()
            if stage == 3:
                second.middle(lambda i, d: rm_v[q, sub(d), lanes[i]])
            if stage == 4:
                second.end()
                gu = rm_v[q, sub(0), :] + (rb2_v[q, 0] + rb2_v[q, 1])
                xr = rh_v[q].astype(F32)
                inv = lax.rsqrt(jnp.mean(xr * xr, axis=-1, keepdims=True) + NORM_EPS)
                normed = xr * inv
                gn = gu * (gain_m, gain_t)[h][:]
                gx = inv * (gn - normed * jnp.mean(gn * normed, axis=-1, keepdims=True))
                rm_v[q, sub(0), :] = gx.astype(BF16).astype(F32)
                part = jnp.sum(gu * normed, axis=0, keepdims=True)
                gg_v[pl.ds(h, 1), :] = part if s == 0 else gg_v[pl.ds(h, 1), :] + part
                keep().start()
                down.spread()
            if stage == 5:
                down.pass_on()
            if stage == 6:
                keep().wait()
                down.end()
                up.spread()
            if stage == 7:
                up.pass_on()
            if stage == 8:
                up.end()

    def rest(h):
        for s in BOTH:
            ring(h, s)[3].rest()

    plane = Exchange(here, "tp", gg_v, gland, es.at[0], er.at[0])
    line = Exchange(here, "dp", tsend, tland, es.at[1], er.at[1])

    def sums(stage):
        if stage == 0:
            plane.start(gg_v[:])
        if stage == 1:
            total = functools.reduce(jnp.add, plane.blocks())
            tsend[:] = jnp.concatenate([total, jnp.broadcast_to(lpart[0:1, 0:1], total.shape)])
            line.start(tsend[:])
        if stage == 2:
            tot[:] = functools.reduce(jnp.add, line.blocks())

    def narrow():
        r = upto(seq)
        c = near(gh.at[r, :], acc_v, sem_a)
        c.start()
        c.wait()
        u_v[r, :] = acc_v[:].astype(BF16)
        near(u_v.at[r, :], ghb, sem_a).start()

    far_steps = [plane_gather(here, far_u, s, gs, gr) for s in BOTH]

    def far_event(stage):
        for s in BOTH:
            for i in ((stage - 1,), (2, 3), (4, 5), (6,))[max(stage - 2, 0)]:
                far_steps[s][i]()

    def drain():
        rows_sent = 6 * (seq // 2 // RING + seq // 2 // RING // RING)
        for q in range(4):
            arrived(du.at[upto(rows_sent), :], ss.at[q])
        for s in BOTH:
            far_steps[s][7]()
        plane.drain()
        line.drain()
        arrived(sum_v.at[:, upto(2 * FEATS)], b_send)
        arrived(g_v, d_send)

    def both(act):
        return lambda k: [act(k, which) for which in BOTH]

    verbs = {"r": event, "u": rest, "g": sums, "n": narrow, "f": far_event, "a": add, "L": both(land), "C": both(close), "p": land, "q": close, "z": drain}

    def run(text):
        for word in text.split(","):
            with jax.named_scope(word):
                verbs[word[0]](*(int(c) for c in word[1:]))

    def at_point(k, point):
        for at, text in (a.split(":") for a in ACTS):
            if at[-1] == point:
                @pl.when(k == int(at[:-1]))
                def _():
                    run(text)

    fetch(0, 0)
    begin(u_copies(0))

    def spread_stats(k):
        for i, ref in enumerate((lse_v, rw_v, lab_v)):
            ref[pl.ds(k * rows, rows), :] = columns(st[k, i:i + 1, :])

    spread_stats(1)

    def more_loads():
        begin(u_copies(1))
        fetch(1, 1)
        begin(acc_copies(0, False))

    def before_other():
        spread_stats(0)
        u_wait(0)

    def before_sends():
        spread_stats(2)
        u_wait(1)
        with jax.named_scope("meet"):
            met()
        far_event(1)

    with jax.named_scope("make0"):
        make(0, 0, more_loads, before_other, before_sends)
    add(0)

    @pl.loop(1, last + 1)
    def _(k):
        lo, hi = pick(DONE[:1] + DONE[:-1], k), pick(DONE, k)
        slot = lax.rem(k + lo, 2)

        def more(t):
            @pl.when(t < hi)
            def _():
                task_fetch(t, lax.rem(k + 1 + t, 2))

            @pl.when((t == hi) & (k < last))
            def _():
                fetch(k + 1, lax.rem(k + 1 + t, 2))

        more(lo)

        def middle():
            at_point(k, "m")

            @pl.when(k == 1)
            def _():
                arrived(g_v.at[upto(FIRST), :], d_send)

            @pl.when(k > 1)
            def _():
                arrived(g_v, d_send)

        with jax.named_scope("make"):
            make(k, slot, middle=middle)

        at_point(k, "a")

        @pl.loop(lo, hi)
        def _(t):
            at_point(t, "t")
            more(t + 1)
            with jax.named_scope("task"):
                task(t, lax.rem(k + 1 + t, 2))

        at_point(k, "d")

    for text in TAIL:
        run(text)
    with jax.named_scope("tail"):
        arrived(fin.at[1], f_send)
        arrived(fin.at[1], f_recv)
        arrived(fin.at[0], sem_o)
        arrived(ghb, sem_a)


def head_grad(hm, ht, gain_m, gain_t, u_own, u_par, far_u, z, w, st, du_in, lpart):
    rows, depth = u_own.shape
    seq = rows // 2
    half = z.shape[1] // 2
    n_tp, n_dp, n = lax.axis_size("tp"), lax.axis_size("dp"), len(KINDS)
    big, small = seq // 2 // RING, seq // 2 // RING // RING
    shape = jax.ShapeDtypeStruct
    stat = pltpu.VMEM((3 * rows, LANES), F32)
    return pl.pallas_call(
        head_kernel,
        out_shape=(shape((2, half, FEATS), F32), shape((rows, depth), F32), shape((seq, depth), BF16), shape((rows, depth), F32),
                   shape((rows, depth), F32), shape((2, half, FEATS), F32), shape((4, depth), F32)),
        in_specs=[ANY, ANY, VMEM, VMEM] + [ANY] * 5 + [VMEM, ANY, VMEM],
        out_specs=(ANY,) * 6 + (VMEM,),
        scratch_shapes=[
            pltpu.VMEM((3 * rows, depth), BF16), pltpu.VMEM((2, depth, TASK), BF16), pltpu.VMEM((2, rows, TASK), F32),
            pltpu.VMEM((TASK, 2 * rows), BF16), pltpu.VMEM((WIDE, 2 * TASK), F32), pltpu.VMEM((WIDE, 2 * TASK), F32),
            pltpu.VMEM((half, 2 * TASK), F32), pltpu.VMEM((2, WIDE, FEATS), F32), pltpu.VMEM((seq, depth), F32),
            stat, stat, stat,
            pltpu.VMEM((4, 2, big, depth // 2), F32), pltpu.VMEM((2, 2, big, depth // 2), F32), pltpu.VMEM((4, 2, big, depth), F32),
            pltpu.VMEM((4, big, depth), F32), pltpu.VMEM((4, 2, small, depth // 2), F32), pltpu.VMEM((4, 2, small, depth), F32),
            pltpu.VMEM((4, small, depth), BF16),
            pltpu.VMEM((2, depth), F32), pltpu.VMEM((n_tp, 2, depth), F32), pltpu.VMEM((n_dp, 4, depth), F32), pltpu.VMEM((4, depth), F32),
            TWO, TWO, TWO, DMA, DMA, TWO, DMA, DMA((n,)), DMA, DMA((n, 2)), DMA, DMA,
            TWO, DMA((2, 3, 2)), DMA((4,)), DMA((4, 4, 2)), DMA((2, 4)), DMA((4,)), TWO, TWO,
        ],
        input_output_aliases={6: 4},
        compiler_params=pltpu.CompilerParams(vmem_limit_bytes=VMEM_LIMIT, collective_id=1, has_side_effects=True),
        name="head_grad",
    )(hm, ht, gain_m, gain_t, u_own, u_par, far_u, z, w, st, du_in, lpart)


def finish_kernel(fin, gh, ghb, tot, out, gm, gt, loss, ggm, ggt, f_v, o_v, g_v, m_v, t_v, sem_f, sem_o, sem_g):
    seq = gm.shape[0]
    table, used = chunk_table()
    jobs = [(k, *t) for t in table for k in BOTH]
    here = Torus()

    def f_in(i):
        k, at, width, _, _ = jobs[i]
        return near(fin.at[k, pl.ds(at, width), :], f_v.at[k, pl.ds(at, width), :], sem_f.at[i])

    def f_out(i):
        k, at, width, swapped, offset = jobs[i]
        return near(o_v.at[k, :, pl.ds(at, width)], out.at[:, ds(column(here, used, swapped, k, offset), width, LANES)], sem_o.at[i])

    g_in, m_in = near(gh.at[pl.ds(seq, seq), :], g_v, sem_g.at[0]), near(ghb, m_v, sem_g.at[1])
    begin([f_in(i) for i in range(WINDOW)])
    ggm[:], ggt[:], loss[:] = tot[0:1, :], tot[1:2, :], tot[2:3, 0:1]
    outs = [f_out(i) for i in range(len(jobs))] + [near(t_v, gt, sem_g.at[0]), near(m_v, gm, sem_g.at[1])]
    for i, (k, at, width, _, _) in enumerate(jobs):
        begin([f_in(i + WINDOW)] if i + WINDOW < len(jobs) else [(m_in, g_in)[i % 2]] if i + 2 >= len(jobs) else [])
        f_in(i).wait()
        o_v[k, :, pl.ds(at, width)] = f_v[k, pl.ds(at, width), :].T
        outs[i].start()
    m_in.wait()
    outs[-1].start()
    g_in.wait()
    t_v[:] = g_v[:].astype(BF16)
    outs[-2].start()
    for c in outs:
        c.wait()


def finish(fin, gh, ghb, tot):
    _, half, block = fin.shape
    seq, depth = ghb.shape
    shape, row, jobs = jax.ShapeDtypeStruct, jax.ShapeDtypeStruct((1, depth), F32), DMA((2 * len(KINDS),))
    rows = pltpu.VMEM((seq, depth), BF16)
    return pl.pallas_call(
        finish_kernel,
        out_shape=(shape((block, 2 * half), F32), shape((seq, depth), BF16), shape((seq, depth), BF16), shape((1, 1), F32), row, row),
        in_specs=[ANY, ANY, ANY, VMEM],
        out_specs=(ANY, ANY, ANY, VMEM, VMEM, VMEM),
        scratch_shapes=[pltpu.VMEM((2, half, block), F32), pltpu.VMEM((2, block, half), F32), pltpu.VMEM((seq, depth), F32), rows, rows,
                        jobs, jobs, TWO],
        compiler_params=pltpu.CompilerParams(vmem_limit_bytes=VMEM_LIMIT),
        name="finish",
    )(fin, gh, ghb, tot)


def solution(mesh):
    def local_step(h_main, h_mtp, labels_main, labels_mtp, weight_main, weight_mtp, gain_final, gain_mtp, w_out):
        hm, ht, gm, gt = h_main[0], h_mtp[0], gain_final[None], gain_mtp[None]
        z, u_own, u_par, far_u, du_in, st, lpart = logits(hm, ht, gm, gt, labels_main, labels_mtp, weight_main, weight_mtp, w_out)
        fin, gh, ghb, _, _, _, tot = head_grad(hm, ht, gm, gt, u_own, u_par, far_u, z, w_out, st, du_in, lpart)
        grad_w, gh_m, gh_t, loss, gg_m, gg_t = finish(fin, gh, ghb, tot)
        return loss[0, 0], gh_m[None], gh_t[None], grad_w, gg_m[0], gg_t[0]

    wide, row = P("dp", None, None), P("dp", None)
    return jax.shard_map(
        local_step,
        mesh=mesh,
        in_specs=(wide, wide, row, row, row, row, P(None), P(None), P(None, "tp")),
        out_specs=(P(), wide, wide, P("dp", "tp"), P(None), P(None)),
        check_vma=False,
    )
```

```python
import functools

import jax
import jax.numpy as jnp
from jax import lax
from jax.experimental import pallas as pl
from jax.experimental.pallas import tpu as pltpu
from jax.sharding import PartitionSpec as P

NORM_EPS = 1e-6
MTP_LAMBDA = 0.3
F32, BF16 = jnp.float32, jnp.bfloat16
DMA = pltpu.SemaphoreType.DMA
TWO = DMA((2,))
ANY = pl.BlockSpec(memory_space=pl.ANY)
VMEM = pl.BlockSpec(memory_space=pltpu.VMEM)
VMEM_LIMIT = 67043328
WINDOW = 9
LANES, FEATS = 128, 256
RING = 4
WAYS = (1, -1)
BOTH = range(2)
NT = (((1,), (1,)), ((), ()))
CHUNK = 1280
LEFT = 4096
SLICE = 24
SPREAD = 2 * RING * RING * SLICE
FIRST, WIDE = 128, 384
TASK = 512
KINDS = "nnnnnnnsn"
DONE = (0, 5, 8, 14, 16) + 4 * (20,)
ACTS = ("1m:f2", "1a:a1", "1t:f3", "2t:L0", "4t:C0", "2a:a2", "2d:r00,u0,L1", "3m:C1", "8t:a3", "9t:r01", "13t:f4", "4m:r02,L2", "4a:C2",
        "14t:a4", "4d:r03,f5,r10", "5m:r04,u1,L3", "5a:a5,C3", "5d:r05,r11", "6m:L4", "6a:a6,C4,r06", "7m:r12", "7a:a7", "8m:L5", "8a:a8,C5,r13")
TAIL = ("r14,g0,r15,r07,g1,r16,L7,C7,L6,C6,p80,q80,r08", "r17,p81,q81,n,g2,r18,z")


def ds(start, size, unit=8):
    return pl.ds(pl.multiple_of(start, unit), size)


def mod(p):
    return lax.rem(p + RING, RING)


def upto(n):
    return pl.ds(0, n)


def halves(n):
    return upto(n // 2), pl.ds(n // 2, n // 2)


def columns(row):
    return jnp.broadcast_to(row, (LANES, row.shape[1])).T


def near(src, dst, sem):
    return pltpu.make_async_copy(src, dst, sem)


def remote(src, dst, send, recv, to):
    return pltpu.make_async_remote_copy(src, dst, send, recv, device_id=to, device_id_type=pl.DeviceIdType.MESH)


def arrived(ref, sem):
    near(ref, ref, sem).wait()


def begin(copies):
    for c in copies:
        c.start()


def dot(a, b):
    return jnp.dot(a, b, preferred_element_type=F32)


def grad_logits(z, lse, rw, lab, col):
    lane = lax.broadcasted_iota(jnp.int32, z.shape, 1).astype(F32)
    p = jnp.exp(z - lse)
    return rw * jnp.where(lab - col == lane, p - 1.0, p)


class Torus:
    def __init__(self):
        self.tp, self.dp = lax.axis_index("tp"), lax.axis_index("dp")
        self.y, self.z = lax.rem(self.tp, RING), self.tp // RING
        self.x, self.core = self.dp // 2, lax.rem(self.dp, 2)
        self.mate = self.x + 1 - 2 * lax.rem(self.x, 2)
        self.far = RING - 1 - self.x
        self.opposite = RING - 1 - self.mate

    def side(self, swapped):
        return self.x // 2 if swapped else lax.rem((self.x + 1) // 2, 2)

    def chip(self, x, core=None):
        return {"tp": self.tp, "dp": 2 * x + (self.core if core is None else core)}

    def step(self, axis, d):
        y, z = (mod(self.y + d), self.z) if axis == 0 else (self.y, mod(self.z + d))
        return {"tp": z * RING + y, "dp": self.dp}

    def rings(self, s):
        ways = [functools.partial(self.step, a) for a in BOTH]
        return (self.y, ways[0], self.z, ways[1]) if s == 0 else (self.z, ways[1], self.y, ways[0])

    def others(self, axis):
        n, me = (lax.axis_size(axis), lax.axis_index(axis))
        return [{"tp": self.tp, "dp": self.dp, axis: lax.rem(me + d, n)} for d in range(1, n)]

    def greet(self):
        barrier = pltpu.get_barrier_semaphore()
        peers = self.others("tp") + self.others("dp")
        for peer in peers:
            pl.semaphore_signal(barrier, inc=1, device_id=peer, device_id_type=pl.DeviceIdType.MESH)
        return lambda: pl.semaphore_wait(barrier, len(peers))


class Exchange:
    def __init__(self, here, axis, src, land, send, recv):
        self.land, self.recv = land, recv
        me = lax.axis_index(axis)
        self.copies = lambda: [remote(src, land.at[me], send, recv, to) for to in here.others(axis)]
        self.rest = land.at[pl.ds(1, lax.axis_size(axis) - 1)]
        self.send, self.me = send, me

    def start(self, own):
        self.land[self.me] = own
        begin(self.copies())

    def blocks(self):
        arrived(self.rest, self.recv)
        return [self.land[i] for i in range(self.land.shape[0])]

    def drain(self):
        arrived(self.rest, self.send)


class Gather:
    def __init__(self, ref, rows, lanes, to, send, recv, own=None):
        self.ref, self.rows, self.to, self.send, self.recv = ref, rows, to, send, recv
        self.lanes = lanes
        self.own = ref.at[rows(0), lanes] if own is None else own
        self.size = rows(0).size

    def spread(self):
        dst = self.ref.at[self.rows(0), self.lanes]
        begin([remote(self.own, dst, self.send, self.recv.at[0], self.to(d)) for d in WAYS])

    def pass_on(self):
        arrived(self.ref.at[upto(2 * self.size), self.lanes], self.recv.at[0])
        n = self.lanes.size // 2
        for i, d in enumerate(WAYS):
            part = self.ref.at[self.rows(-d), pl.ds(self.lanes.start + i * n, n)]
            remote(part, part, self.send, self.recv.at[1], self.to(d)).start()

    def end(self):
        arrived(self.ref.at[upto(self.size), self.lanes], self.recv.at[1])


class Scatter:
    def __init__(self, src, rows, to, from_a, from_b, send, recv):
        self.src, self.rows, self.to, self.a, self.b, self.send, self.recv = src, rows, to, from_a, from_b, send, recv
        self.lanes = halves(src.shape[-1])

    def start(self):
        for i, d in enumerate(WAYS):
            remote(self.src.at[self.rows(2), self.lanes[i]], self.a.at[i], self.send, self.recv.at[0], self.to(d)).start()

    def rest(self):
        for i, d in enumerate(WAYS):
            other = self.lanes[1 - i]
            remote(self.src.at[self.rows(d), other], self.b.at[i, :, other], self.send, self.recv.at[1], self.to(d)).start()

    def middle(self, own):
        arrived(self.a, self.recv.at[0])
        for i, d in enumerate(WAYS):
            self.a[i] += own(i, d)
            remote(self.a.at[i], self.b.at[i, :, self.lanes[i]], self.send, self.recv.at[1], self.to(d)).start()

    def end(self):
        arrived(self.b, self.recv.at[1])


def slices(here, s):
    p1, _, p2, _ = here.rings(s)
    base = s * (SPREAD // 2)
    return (lambda o: ds(base + (p2 * RING + mod(p1 + o)) * SLICE, SLICE)), (lambda o: ds(base + mod(p2 + o) * RING * SLICE, RING * SLICE))


def plane_gather(here, ref, s, send, recv):
    _, to1, _, to2 = here.rings(s)
    one, many = slices(here, s)
    depth = ref.shape[-1]
    a = Gather(ref, one, upto(depth), to1, send.at[s], recv.at[s, 0])
    b, c = [Gather(ref, many, lanes, to2, send.at[s], recv.at[s, i + 1]) for i, lanes in enumerate(halves(depth))]

    def turn():
        a.end()
        b.spread()

    def end():
        b.end()
        c.end()

    def drain():
        arrived(ref.at[upto(3 * (RING + 1) * SLICE), :], send.at[s])

    return [a.spread, a.pass_on, turn, c.spread, b.pass_on, c.pass_on, end, drain]


def logits_kernel(hm, ht, gain_m, gain_t, lab_m, lab_t, wt_m, wt_t, w, z, u_out, up_out, far_u, du_out, st, lpart,
                  h_v, u_v, uf_v, got_v, w_v, z_v, e_v, x_v, m_v, s_v, t_v, lab_v, send_v, land, wsend, wland, pack,
                  sem_h, sem_u, sem_w, sem_z, sem_d, sem_k, es, er, ps, pr, gs, gr, xs, xr):
    seq, depth = hm.shape
    rows, vocab = z.shape
    steps = vocab // CHUNK
    here = Torus()
    mate, far = here.chip(here.mate), here.chip(here.far)

    def w_copy(i, slot):
        return near(w.at[:, ds(i * CHUNK, CHUNK, LANES)], w_v.at[slot], sem_w.at[slot])

    def z_copy(i, slot):
        return near(z_v.at[slot], z.at[:, ds(i * CHUNK, CHUNK, LANES)], sem_z.at[slot])

    loads = [near(src, h_v.at[pl.ds(i * seq, seq), :], sem_h.at[i]) for i, src in enumerate((hm, ht))]
    begin(loads + [w_copy(0, 0)])
    met = here.greet()
    m_v[:] = jnp.full_like(m_v, -jnp.inf)
    s_v[:] = jnp.zeros_like(s_v)
    t_v[:] = jnp.zeros_like(t_v)
    lab = jnp.concatenate([lab_m[:], lab_t[:]], axis=1).astype(F32) - (here.tp * vocab).astype(F32)
    lab_v[:] = columns(lab)
    top_row = lax.broadcasted_iota(jnp.int32, wsend.shape, 0) == 0
    wsend[:] = jnp.where(top_row, jnp.sum(wt_m[:]), jnp.sum(wt_t[:]))

    for half, gain in enumerate((gain_m, gain_t)):
        loads[half].wait()
        g = gain[:]

        @pl.loop(0, seq // LANES)
        def _(i):
            r = ds(half * seq + i * LANES, LANES)
            x = h_v[r, :].astype(F32)
            inv = lax.rsqrt(jnp.mean(x * x, axis=-1, keepdims=True) + NORM_EPS)
            u = (x * inv * g).astype(BF16)
            u_v[r, :] = u
            uf_v[r, :] = u.astype(F32)

    u_copy = near(u_v, u_out, sem_u)
    u_copy.start()
    with jax.named_scope("meet"):
        met()

    weights = Exchange(here, "dp", wsend, wland, es.at[0], er.at[0])
    weights.start(wsend[:])
    rest = pl.ds(SPREAD, rows - SPREAD)
    parts = [slices(here, s)[0](0) for s in BOTH] + [rest]

    def fetched(k, i):
        return remote(uf_v.at[parts[i], :], (got_v, far_u)[k].at[parts[i], :], xs.at[k, i], xr.at[k, i], (mate, far)[k])

    begin([fetched(k, i) for i in range(3) for k in BOTH])
    spread = [plane_gather(here, got_v, s, gs, gr) for s in BOTH]
    lane = lax.broadcasted_iota(jnp.int32, (rows, LANES), 1).astype(F32)

    @pl.loop(0, steps)
    def _(i):
        slot = lax.rem(i, 2)
        w_copy(i, slot).wait()

        @pl.when(i + 1 < steps)
        def _():
            w_copy(i + 1, 1 - slot).start()

        @pl.when(i >= 2)
        def _():
            z_copy(i - 2, slot).wait()

        m, s, t = m_v[:], s_v[:], t_v[:]
        rel = lab_v[:] - (i * CHUNK).astype(F32)
        for n in range(0, CHUNK, FEATS):
            for which, at in enumerate((0, 3 * FEATS)):
                for stage in range(3):
                    if n == at:
                        @pl.when(i == stage + 1)
                        def _():
                            if stage == 0:
                                arrived(got_v.at[parts[which], :], xr.at[0, which])
                            spread[which][stage]()
            zz = dot(u_v[:], w_v[slot, :, n:n + FEATS])
            z_v[slot, :, n:n + FEATS] = zz
            za, zb = zz[:, :LANES], zz[:, LANES:]
            new = jnp.maximum(m, jnp.maximum(za, zb))
            s = s * jnp.exp(m - new) + (jnp.exp(za - new) + jnp.exp(zb - new))
            t = jnp.where(rel == lane + n, za, t)
            t = jnp.where(rel == lane + (n + LANES), zb, t)
            m = new
        m_v[:], s_v[:], t_v[:] = m, s, t
        z_copy(i, slot).start()

    mt = m_v[:].T
    top = jnp.max(mt, axis=0, keepdims=True)
    total = jnp.sum(s_v[:].T * jnp.exp(mt - top), axis=0, keepdims=True)
    hit = jnp.sum(t_v[:].T, axis=0, keepdims=True)
    send_v[:] = jnp.where(lax.broadcasted_iota(jnp.int32, send_v.shape, 0) == 0, top + jnp.log(total), hit)
    stats = Exchange(here, "tp", send_v, land, es.at[1], er.at[1])
    stats.start(send_v[:])
    for stage in (3, 4):
        for which in BOTH:
            spread[which][stage]()
    sums = functools.reduce(jnp.add, weights.blocks())
    rw = jnp.concatenate([wt_m[:] * (1.0 / sums[0:1, 0:1]), wt_t[:] * (MTP_LAMBDA / sums[1:2, 0:1])], axis=1)
    with jax.named_scope("statwait"):
        blocks = stats.blocks()
    top = functools.reduce(jnp.maximum, blocks)
    lse = (top + jnp.log(functools.reduce(jnp.add, [jnp.exp(b - top) for b in blocks])))[0:1, :]
    hit = functools.reduce(jnp.add, blocks)[1:2, :]
    lpart[:] = jnp.broadcast_to(jnp.sum(rw * (lse - hit)), lpart.shape)
    row = lax.broadcasted_iota(jnp.int32, st.shape[1:], 0)
    st[1] = jnp.where(row == 0, lse, jnp.where(row == 1, rw, lab))
    pack[:] = st[1]
    swaps = [remote(pack, st.at[2 * k], ps.at[k], pr.at[k], to) for k, to in enumerate((mate, far))]
    begin(swaps)
    m_v[:] = columns(lse)
    s_v[:] = columns(rw)
    skip = LEFT - (steps - 2) * CHUNK
    at = 0
    for step, start in ((steps - 1, 0), (steps - 2, skip)):
        for c in range(start, CHUNK, LANES):
            e_v[:, at:at + LANES] = grad_logits(
                z_v[step % 2, :, c:c + LANES], m_v[:], s_v[:], lab_v[:], float(step * CHUNK + c)).astype(BF16)
            at += LANES

    def e_dot(r, cols):
        return (lax.dot_general(e_v[r, :CHUNK], w_v[(steps - 1) % 2, cols, :], NT, preferred_element_type=F32)
                + lax.dot_general(e_v[r, CHUNK:], w_v[(steps - 2) % 2, cols, skip:], NT, preferred_element_type=F32))

    for i in BOTH:
        for k in BOTH:
            fetched(k, i).wait_send()
    saves = []
    for dst, r in ((uf_v, slice(0, SPREAD)), (x_v, slice(SPREAD, rows))):
        for n in range(0, depth, TASK):
            dst[:r.stop - r.start, n:n + TASK] = e_dot(r, slice(n, n + TASK))
            src = dst.at[upto(r.stop - r.start), pl.ds(n, TASK)]
            saves.append(near(src, du_out.at[pl.ds(r.start, r.stop - r.start), pl.ds(n, TASK)], sem_d.at[len(saves)]))
            saves[-1].start()
            if len(saves) in (2, 3):
                spread[len(saves) - 2][5]()
    u_copy.wait()
    waits = [spread[0][6], spread[1][6], lambda: arrived(got_v.at[rest, :], xr.at[0, 2])]
    for i, wait in enumerate(waits):
        start = i * (SPREAD // 2)
        r = pl.ds(start, min(SPREAD // 2, rows - start))
        with jax.named_scope("land"):
            wait()

        @pl.loop(start // LANES, (start + r.size) // LANES)
        def _(j):
            part = ds(j * LANES, LANES)
            u_v[part, :] = got_v[part, :].astype(BF16)

        saves.append(near(u_v.at[r, :], up_out.at[r, :], sem_k.at[i]))
        saves[-1].start()
    for c in swaps:
        c.wait()
    for i in range(3):
        arrived(far_u.at[parts[i], :], xr.at[1, i])
    weights.drain()
    stats.drain()
    for k in BOTH:
        spread[k][7]()
        fetched(k, 2).wait_send()
        z_copy(steps - 2 + k, (steps + k) % 2).wait()
    for c in saves:
        c.wait()


def logits(hm, ht, gain_m, gain_t, lab_m, lab_t, wt_m, wt_t, w):
    seq, depth = hm.shape
    rows, vocab = 2 * seq, w.shape[1]
    n_tp, n_dp = lax.axis_size("tp"), lax.axis_size("dp")
    shape = jax.ShapeDtypeStruct
    stat = pltpu.VMEM((rows, LANES), F32)
    return pl.pallas_call(
        logits_kernel,
        out_shape=(shape((rows, vocab), F32), shape((rows, depth), BF16), shape((rows, depth), BF16), shape((rows, depth), F32),
                   shape((rows, depth), F32), shape((3, 8, rows), F32), shape((8, LANES), F32)),
        in_specs=[ANY, ANY] + [VMEM] * 6 + [ANY],
        out_specs=(ANY,) * 5 + (VMEM, VMEM),
        scratch_shapes=[
            pltpu.VMEM((rows, depth), BF16), pltpu.VMEM((rows, depth), BF16), pltpu.VMEM((rows, depth), F32), pltpu.VMEM((rows, depth), F32),
            pltpu.VMEM((2, depth, CHUNK), BF16), pltpu.VMEM((2, rows, CHUNK), F32), pltpu.VMEM((rows, vocab - LEFT), BF16),
            pltpu.VMEM((rows - SPREAD, depth), F32), stat, stat, stat, stat,
            pltpu.VMEM((2, rows), F32), pltpu.VMEM((n_tp, 2, rows), F32), pltpu.VMEM((8, LANES), F32), pltpu.VMEM((n_dp, 8, LANES), F32),
            pltpu.VMEM((8, rows), F32),
            TWO, DMA, TWO, TWO, DMA((2 * depth // TASK,)), DMA((3,)), TWO, TWO, TWO, TWO,
            TWO, DMA((2, 3, 2)), *[DMA((2, 3))] * 2,
        ],
        compiler_params=pltpu.CompilerParams(vmem_limit_bytes=VMEM_LIMIT, collective_id=0, has_side_effects=True),
        name="logits",
    )(hm, ht, gain_m, gain_t, lab_m, lab_t, wt_m, wt_t, w)


def chunk_table():
    out, at, used = [], 0, [0, 0]
    for i, kind in enumerate(KINDS):
        width, swapped = (WIDE if i else FIRST), int(kind == "s")
        out.append((at, width, swapped, used[swapped]))
        at, used[swapped] = at + width, used[swapped] + width
    return out, used


def column(here, used, swapped, other, offset):
    base = [2 * used[0] * s + abs(here.side(s) - other) * used[s] for s in BOTH]
    return jnp.where(swapped == 1, base[1], base[0]) + offset


def pick(values, k):
    if isinstance(k, int):
        return values[k]
    return functools.reduce(lambda out, i: jnp.where(k == i, values[i], out), range(1, len(values)), jnp.int32(values[0]))


def head_kernel(hm, ht, gain_m, gain_t, u_own, u_par, far_in, z, w, st, du_in, lpart,
                fin, gh, ghb, du, far_u, one, tot, u_v, w_v, z_v, et_v, g_v, own_v, sum_v, one_v, acc_v,
                lse_v, rw_v, lab_v, ra_v, rl_v, rb_v, rm_v, ra2_v, rb2_v, rh_v, gg_v, gland, tland, tsend,
                sem_u, sem_w, sem_z, sem_a, sem_o, sem_1, d_send, d_recv, b_send, b_recv, f_send, f_recv,
                gs, gr, ss, sr, sem_l, sem_x, es, er):
    del far_in
    rows, depth = u_own.shape
    seq = rows // 2
    here = Torus()
    x, core = here.x, here.core
    met = here.greet()
    table, used = chunk_table()
    starts, _, swaps, offsets = (list(t) for t in zip(*table))
    last = len(table) - 1

    def span(k):
        return upto(FIRST) if isinstance(k, int) and k == 0 else ds(FIRST + (k - 1) * WIDE, WIDE, LANES)

    def chips(k):
        s = pick(swaps, k) == 1
        return jnp.where(s, here.far, here.mate), jnp.where(s, here.mate, here.far)

    def block(i):
        return ds((2 * lax.rem(i, RING) + jnp.where(i < RING, 1 - core, core)) * FEATS, FEATS, FEATS)

    def feats(i):
        return pl.ds(i * FEATS, FEATS)

    def w_copies(col, width, slot):
        return [near(w.at[block(i), ds(col, width, LANES)], w_v.at[slot, feats(i), upto(width)], sem_w.at[slot]) for i in range(2 * RING)]

    def u_copies(k):
        src, r = ((u_par, upto(rows)), (u_own, pl.ds(rows, rows)))[k]
        return [near(src.at[:, block(i)], u_v.at[r, feats(i)], sem_u.at[k]) for i in range(2 * RING)]

    def u_wait(k):
        arrived(u_v.at[upto(rows), :], sem_u.at[k])

    def fetch(k, slot):
        width = span(k).size
        col = column(here, used, pick(swaps, k), 0, pick(offsets, k))
        begin(w_copies(col, width, slot) + [near(z.at[:, ds(col, width, LANES)], z_v.at[slot, :, upto(width)], sem_z.at[slot])])

    per = LEFT // TASK

    def piece(t):
        return t < 2 * per, t // per, lax.rem(t, per)

    def acc_copies(h, back):
        refs = [(acc_v.at[:, feats(i)], (du if back else du_in).at[ds(h * seq, seq), block(i)]) for i in range(2 * RING)]
        return [near(*(p if back else p[::-1]), sem_a) for p in refs]

    def task_fetch(t, slot):
        of_du, h, i = piece(t)

        @pl.when(of_du)
        def _():
            begin(w_copies(i * TASK, TASK, slot))
            near(z.at[ds(h * seq, seq), ds(i * TASK, TASK, LANES)], z_v.at[slot, upto(seq), :], sem_z.at[slot]).start()

        @pl.when(~of_du)
        def _():
            begin([near(far_u.at[:, block(2 * i + j)], z_v.at[slot, :, feats(j)], sem_z.at[slot]) for j in BOTH])

    def task(t, slot):
        of_du, h, i = piece(t)

        @pl.when(~of_du)
        def _():
            arrived(z_v.at[slot], sem_z.at[slot])
            u_v[pl.ds(2 * rows, rows), ds(i * TASK, TASK, LANES)] = z_v[slot].astype(BF16)

        @pl.when(of_du)
        def _():
            arrived(w_v.at[slot], sem_w.at[slot])
            arrived(z_v.at[slot, upto(seq), :], sem_z.at[slot])

            @pl.when(i == 0)
            def _():
                arrived(acc_v, sem_a)

            r = ds(rows + h * seq, seq)
            col = (i * TASK).astype(F32)
            for g in range(0, TASK, LANES):
                cols = slice(g, g + LANES)
                et_v[:, cols] = grad_logits(z_v[slot, :seq, cols], lse_v[r, :], rw_v[r, :], lab_v[r, :], col + g).astype(BF16)
            for m in range(0, depth, TASK):
                cols = slice(m, m + TASK)
                acc_v[:, cols] += lax.dot_general(et_v[:, :TASK], w_v[slot, cols, :], NT, preferred_element_type=F32)

            @pl.when(i == per - 1)
            def _():
                acc_v[:] = acc_v[:].astype(BF16).astype(F32)
                begin(acc_copies(h, True))
                arrived(acc_v, sem_a)

            @pl.when((i == per - 1) & (h == 0))
            def _():
                begin(acc_copies(1, False))

    def d_copy(k, part):
        lanes, width = pl.ds(part * TASK, TASK), span(k).size
        return remote(g_v.at[upto(width), lanes], sum_v.at[span(k), lanes], d_send, d_recv.at[k], here.chip(x, 1 - core))

    def b_copy(k, which):
        to = chips(k)[1]
        block_of = ds(jnp.where(which == 0, here.opposite, to) * FEATS, FEATS, FEATS)
        return remote(sum_v.at[span(k), block_of], one.at[which, span(k), :], b_send, b_recv.at[k, which], here.chip(to))

    def f_copy(k):
        mate = chips(k)[0]
        return remote(sum_v.at[span(k), ds(mate * FEATS, FEATS, FEATS)], fin.at[1, span(k), :], f_send, f_recv, here.chip(mate))

    def o_copy(k):
        return near(sum_v.at[span(k), ds(x * FEATS, FEATS, FEATS)], fin.at[0, span(k), :], sem_o)

    def make(k, slot, early=lambda: None, late=lambda: None, middle=lambda: None):
        width = span(k).size
        swapped = pick(swaps, k)
        col = column(here, used, swapped, 0, pick(offsets, k)).astype(F32)
        arrived(w_v.at[slot, :, upto(width)], sem_w.at[slot])
        arrived(z_v.at[slot, :, upto(width)], sem_z.at[slot])
        early()

        def put(zz, r, c, at):
            e = grad_logits(zz, lse_v[r, :], rw_v[r, :], lab_v[r, :], col + c)
            et_v[c:c + LANES, ds(at, rows, rows)] = e.T.astype(BF16)

        for c in range(0, width, LANES):
            put(z_v[slot, :, c:c + LANES], pl.ds(rows, rows), c, rows * (1 - swapped))
        late()
        other = ds(2 * rows * swapped, rows, rows)
        for n in range(0, width, FEATS):
            step = min(width - n, FEATS)
            zz = dot(u_v[other, :], w_v[slot, :, n:n + step])
            for c in range(0, step, LANES):
                put(zz[:, c:c + LANES], other, n + c, rows * swapped)
        middle()
        both = ds(rows * swapped, 2 * rows, rows)
        et = et_v[upto(width), :]
        for part in BOTH:
            lanes = pl.ds(part * TASK, TASK)
            g_v[upto(width), lanes] = dot(et, u_v[both, lanes])
            d_copy(k, part).start()
        own_v[upto(width), :] = dot(et, u_v[both, pl.ds(2 * TASK, 2 * TASK)])

    def add(k):
        arrived(sum_v.at[span(k), :], d_recv.at[k])
        sum_v[span(k), :] += own_v[upto(span(k).size), :]
        begin([b_copy(k, which) for which in BOTH])

    def landing(k, which):
        return near(one.at[which, span(k), :], one_v.at[which, upto(span(k).size), :], sem_1.at[which])

    def land(k, which):
        with jax.named_scope("bwait"):
            arrived(one.at[which, span(k), :], b_recv.at[k, which])
        landing(k, which).start()

    def close(k, which):
        landing(k, which).wait()
        chip = jnp.where(which == 0, chips(k)[0], x)
        sum_v[span(k), ds(chip * FEATS, FEATS, FEATS)] += one_v[which, upto(span(k).size), :]
        (o_copy if which else f_copy)(k).start()

    def ring(h, s):
        q = 2 * h + s
        p1, to1, p2, to2 = here.rings(s)
        big, small = seq // 2 // RING, seq // 2 // RING // RING
        base = h * seq + s * (seq // 2)
        one_of = lambda o: ds(base + mod(p1 + o) * big, big)
        two_of = lambda o: ds(base + p1 * big + mod(p2 + o) * small, small)
        sub = lambda o: ds(mod(p2 + o) * small, small)
        every = upto(depth)
        first = Scatter(du, one_of, to1, ra_v.at[q], rb_v.at[q], ss.at[q], sr.at[q, 0])
        second = Scatter(rm_v.at[q], sub, to2, ra2_v.at[q], rb2_v.at[q], ss.at[q], sr.at[q, 1])
        down = Gather(gh, two_of, every, to2, ss.at[q], sr.at[q, 2], rm_v.at[q, sub(0), :])
        up = Gather(gh, one_of, every, to1, ss.at[q], sr.at[q, 3])
        lanes = halves(depth)
        h_rows = ds(s * (seq // 2) + p1 * big + p2 * small, small)
        loads = lambda: [near(du.at[one_of(WAYS[i]), lanes[i]], rl_v.at[s, i], sem_l.at[s, i]) for i in BOTH] + [
            near(du.at[one_of(0), :], rm_v.at[q], sem_l.at[s, 2]), near((hm, ht)[h].at[h_rows, :], rh_v.at[q], sem_l.at[s, 3])]
        keep = lambda: near(rm_v.at[q, sub(0), :], gh.at[two_of(0), :], sem_x.at[q])
        return q, sub, lanes, first, second, down, up, loads, keep

    def event(h, stage):
        for s in BOTH:
            q, sub, lanes, first, second, down, up, loads, keep = ring(h, s)
            if stage == 0:
                first.start()
                begin(loads())
            if stage == 1:
                for c in loads():
                    c.wait()
                first.middle(lambda i, d: rl_v[s, i])
            if stage == 2:
                first.end()
                rm_v[q] += rb_v[q, 0] + rb_v[q, 1]
                second.start()
                second.rest()
            if stage == 3:
                second.middle(lambda i, d: rm_v[q, sub(d), lanes[i]])
            if stage == 4:
                second.end()
                gu = rm_v[q, sub(0), :] + (rb2_v[q, 0] + rb2_v[q, 1])
                xr = rh_v[q].astype(F32)
                inv = lax.rsqrt(jnp.mean(xr * xr, axis=-1, keepdims=True) + NORM_EPS)
                normed = xr * inv
                gn = gu * (gain_m, gain_t)[h][:]
                gx = inv * (gn - normed * jnp.mean(gn * normed, axis=-1, keepdims=True))
                rm_v[q, sub(0), :] = gx.astype(BF16).astype(F32)
                part = jnp.sum(gu * normed, axis=0, keepdims=True)
                gg_v[pl.ds(h, 1), :] = part if s == 0 else gg_v[pl.ds(h, 1), :] + part
                keep().start()
                down.spread()
            if stage == 5:
                down.pass_on()
            if stage == 6:
                keep().wait()
                down.end()
                up.spread()
            if stage == 7:
                up.pass_on()
            if stage == 8:
                up.end()

    def rest(h):
        for s in BOTH:
            ring(h, s)[3].rest()

    plane = Exchange(here, "tp", gg_v, gland, es.at[0], er.at[0])
    line = Exchange(here, "dp", tsend, tland, es.at[1], er.at[1])

    def sums(stage):
        if stage == 0:
            plane.start(gg_v[:])
        if stage == 1:
            total = functools.reduce(jnp.add, plane.blocks())
            tsend[:] = jnp.concatenate([total, jnp.broadcast_to(lpart[0:1, 0:1], total.shape)])
            line.start(tsend[:])
        if stage == 2:
            tot[:] = functools.reduce(jnp.add, line.blocks())

    def narrow():
        r = upto(seq)
        c = near(gh.at[r, :], acc_v, sem_a)
        c.start()
        c.wait()
        u_v[r, :] = acc_v[:].astype(BF16)
        near(u_v.at[r, :], ghb, sem_a).start()

    far_steps = [plane_gather(here, far_u, s, gs, gr) for s in BOTH]

    def far_event(stage):
        for s in BOTH:
            for i in ((stage - 1,), (2, 3), (4, 5), (6,))[max(stage - 2, 0)]:
                far_steps[s][i]()

    def drain():
        rows_sent = 6 * (seq // 2 // RING + seq // 2 // RING // RING)
        for q in range(4):
            arrived(du.at[upto(rows_sent), :], ss.at[q])
        for s in BOTH:
            far_steps[s][7]()
        plane.drain()
        line.drain()
        arrived(sum_v.at[:, upto(2 * FEATS)], b_send)
        arrived(g_v, d_send)

    def both(act):
        return lambda k: [act(k, which) for which in BOTH]

    verbs = {"r": event, "u": rest, "g": sums, "n": narrow, "f": far_event, "a": add, "L": both(land), "C": both(close), "p": land, "q": close, "z": drain}

    def run(text):
        for word in text.split(","):
            with jax.named_scope(word):
                verbs[word[0]](*(int(c) for c in word[1:]))

    def at_point(k, point):
        for at, text in (a.split(":") for a in ACTS):
            if at[-1] == point:
                @pl.when(k == int(at[:-1]))
                def _():
                    run(text)

    fetch(0, 0)
    begin(u_copies(0))

    def spread_stats(k):
        for i, ref in enumerate((lse_v, rw_v, lab_v)):
            ref[pl.ds(k * rows, rows), :] = columns(st[k, i:i + 1, :])

    spread_stats(1)

    def more_loads():
        begin(u_copies(1))
        fetch(1, 1)
        begin(acc_copies(0, False))

    def before_other():
        spread_stats(0)
        u_wait(0)

    def before_sends():
        u_wait(1)
        with jax.named_scope("meet"):
            met()
        far_event(1)

    with jax.named_scope("make0"):
        make(0, 0, more_loads, before_other, before_sends)
    add(0)
    spread_stats(2)

    @pl.loop(1, last + 1)
    def _(k):
        lo, hi = pick(DONE[:1] + DONE[:-1], k), pick(DONE, k)
        slot = lax.rem(k + lo, 2)

        def more(t):
            @pl.when(t < hi)
            def _():
                task_fetch(t, lax.rem(k + 1 + t, 2))

            @pl.when((t == hi) & (k < last))
            def _():
                fetch(k + 1, lax.rem(k + 1 + t, 2))

        more(lo)

        def middle():
            at_point(k, "m")

            @pl.when(k == 1)
            def _():
                arrived(g_v.at[upto(FIRST), :], d_send)

            @pl.when(k > 1)
            def _():
                arrived(g_v, d_send)

        with jax.named_scope("make"):
            make(k, slot, middle=middle)

        at_point(k, "a")

        @pl.loop(lo, hi)
        def _(t):
            at_point(t, "t")
            more(t + 1)
            with jax.named_scope("task"):
                task(t, lax.rem(k + 1 + t, 2))

        at_point(k, "d")

    for text in TAIL:
        run(text)
    with jax.named_scope("tail"):
        arrived(fin.at[1], f_send)
        arrived(fin.at[1], f_recv)
        arrived(fin.at[0], sem_o)
        arrived(ghb, sem_a)


def head_grad(hm, ht, gain_m, gain_t, u_own, u_par, far_u, z, w, st, du_in, lpart):
    rows, depth = u_own.shape
    seq = rows // 2
    half = z.shape[1] // 2
    n_tp, n_dp, n = lax.axis_size("tp"), lax.axis_size("dp"), len(KINDS)
    big, small = seq // 2 // RING, seq // 2 // RING // RING
    shape = jax.ShapeDtypeStruct
    stat = pltpu.VMEM((3 * rows, LANES), F32)
    return pl.pallas_call(
        head_kernel,
        out_shape=(shape((2, half, FEATS), F32), shape((rows, depth), F32), shape((seq, depth), BF16), shape((rows, depth), F32),
                   shape((rows, depth), F32), shape((2, half, FEATS), F32), shape((4, depth), F32)),
        in_specs=[ANY, ANY, VMEM, VMEM] + [ANY] * 5 + [VMEM, ANY, VMEM],
        out_specs=(ANY,) * 6 + (VMEM,),
        scratch_shapes=[
            pltpu.VMEM((3 * rows, depth), BF16), pltpu.VMEM((2, depth, TASK), BF16), pltpu.VMEM((2, rows, TASK), F32),
            pltpu.VMEM((TASK, 2 * rows), BF16), pltpu.VMEM((WIDE, 2 * TASK), F32), pltpu.VMEM((WIDE, 2 * TASK), F32),
            pltpu.VMEM((half, 2 * TASK), F32), pltpu.VMEM((2, WIDE, FEATS), F32), pltpu.VMEM((seq, depth), F32),
            stat, stat, stat,
            pltpu.VMEM((4, 2, big, depth // 2), F32), pltpu.VMEM((2, 2, big, depth // 2), F32), pltpu.VMEM((4, 2, big, depth), F32),
            pltpu.VMEM((4, big, depth), F32), pltpu.VMEM((4, 2, small, depth // 2), F32), pltpu.VMEM((4, 2, small, depth), F32),
            pltpu.VMEM((4, small, depth), BF16),
            pltpu.VMEM((2, depth), F32), pltpu.VMEM((n_tp, 2, depth), F32), pltpu.VMEM((n_dp, 4, depth), F32), pltpu.VMEM((4, depth), F32),
            TWO, TWO, TWO, DMA, DMA, TWO, DMA, DMA((n,)), DMA, DMA((n, 2)), DMA, DMA,
            TWO, DMA((2, 3, 2)), DMA((4,)), DMA((4, 4, 2)), DMA((2, 4)), DMA((4,)), TWO, TWO,
        ],
        input_output_aliases={6: 4},
        compiler_params=pltpu.CompilerParams(vmem_limit_bytes=VMEM_LIMIT, collective_id=1, has_side_effects=True),
        name="head_grad",
    )(hm, ht, gain_m, gain_t, u_own, u_par, far_u, z, w, st, du_in, lpart)


def finish_kernel(fin, gh, ghb, tot, out, gm, gt, loss, ggm, ggt, f_v, o_v, g_v, m_v, t_v, sem_f, sem_o, sem_g):
    seq = gm.shape[0]
    table, used = chunk_table()
    jobs = [(k, *t) for t in table for k in BOTH]
    here = Torus()

    def f_in(i):
        k, at, width, _, _ = jobs[i]
        return near(fin.at[k, pl.ds(at, width), :], f_v.at[k, pl.ds(at, width), :], sem_f.at[i])

    def f_out(i):
        k, at, width, swapped, offset = jobs[i]
        return near(o_v.at[k, :, pl.ds(at, width)], out.at[:, ds(column(here, used, swapped, k, offset), width, LANES)], sem_o.at[i])

    g_in, m_in = near(gh.at[pl.ds(seq, seq), :], g_v, sem_g.at[0]), near(ghb, m_v, sem_g.at[1])
    begin([f_in(i) for i in range(WINDOW)])
    ggm[:], ggt[:], loss[:] = tot[0:1, :], tot[1:2, :], tot[2:3, 0:1]
    outs = [f_out(i) for i in range(len(jobs))] + [near(t_v, gt, sem_g.at[0]), near(m_v, gm, sem_g.at[1])]
    for i, (k, at, width, _, _) in enumerate(jobs):
        begin([f_in(i + WINDOW)] if i + WINDOW < len(jobs) else [(m_in, g_in)[i % 2]] if i + 2 >= len(jobs) else [])
        f_in(i).wait()
        o_v[k, :, pl.ds(at, width)] = f_v[k, pl.ds(at, width), :].T
        outs[i].start()
    m_in.wait()
    outs[-1].start()
    g_in.wait()
    t_v[:] = g_v[:].astype(BF16)
    outs[-2].start()
    for c in outs:
        c.wait()


def finish(fin, gh, ghb, tot):
    _, half, block = fin.shape
    seq, depth = ghb.shape
    shape, row, jobs = jax.ShapeDtypeStruct, jax.ShapeDtypeStruct((1, depth), F32), DMA((2 * len(KINDS),))
    rows = pltpu.VMEM((seq, depth), BF16)
    return pl.pallas_call(
        finish_kernel,
        out_shape=(shape((block, 2 * half), F32), shape((seq, depth), BF16), shape((seq, depth), BF16), shape((1, 1), F32), row, row),
        in_specs=[ANY, ANY, ANY, VMEM],
        out_specs=(ANY, ANY, ANY, VMEM, VMEM, VMEM),
        scratch_shapes=[pltpu.VMEM((2, half, block), F32), pltpu.VMEM((2, block, half), F32), pltpu.VMEM((seq, depth), F32), rows, rows,
                        jobs, jobs, TWO],
        compiler_params=pltpu.CompilerParams(vmem_limit_bytes=VMEM_LIMIT),
        name="finish",
    )(fin, gh, ghb, tot)


def solution(mesh):
    def local_step(h_main, h_mtp, labels_main, labels_mtp, weight_main, weight_mtp, gain_final, gain_mtp, w_out):
        hm, ht, gm, gt = h_main[0], h_mtp[0], gain_final[None], gain_mtp[None]
        z, u_own, u_par, far_u, du_in, st, lpart = logits(hm, ht, gm, gt, labels_main, labels_mtp, weight_main, weight_mtp, w_out)
        fin, gh, ghb, _, _, _, tot = head_grad(hm, ht, gm, gt, u_own, u_par, far_u, z, w_out, st, du_in, lpart)
        grad_w, gh_m, gh_t, loss, gg_m, gg_t = finish(fin, gh, ghb, tot)
        return loss[0, 0], gh_m[None], gh_t[None], grad_w, gg_m[0], gg_t[0]

    wide, row = P("dp", None, None), P("dp", None)
    return jax.shard_map(
        local_step,
        mesh=mesh,
        in_specs=(wide, wide, row, row, row, row, P(None), P(None), P(None, "tp")),
        out_specs=(P(), wide, wide, P("dp", "tp"), P(None), P(None)),
        check_vma=False,
    )
```

```python
import functools

import jax
import jax.numpy as jnp
from jax import lax
from jax.experimental import pallas as pl
from jax.experimental.pallas import tpu as pltpu
from jax.sharding import PartitionSpec as P

NORM_EPS = 1e-6
MTP_LAMBDA = 0.3
F32, BF16 = jnp.float32, jnp.bfloat16
DMA = pltpu.SemaphoreType.DMA
TWO = DMA((2,))
ANY = pl.BlockSpec(memory_space=pl.ANY)
VMEM = pl.BlockSpec(memory_space=pltpu.VMEM)
VMEM_LIMIT = 67043328
WINDOW = 9
LANES, FEATS = 128, 256
RING = 4
WAYS = (1, -1)
BOTH = range(2)
NT = (((1,), (1,)), ((), ()))
CHUNK = 1280
LEFT = 4096
SLICE = 24
SPREAD = 2 * RING * RING * SLICE
FIRST, WIDE = 128, 384
TASK = 512
KINDS = "nnnnnnnsn"
DONE = (0, 5, 8, 14, 16) + 4 * (20,)
ACTS = ("1m:f2", "1a:a1", "1t:f3", "2t:L0", "4t:C0", "2a:a2", "2d:r00,u0,L1", "3m:C1", "8t:a3", "9t:r01", "13t:f4", "4m:r02,L2", "4a:C2",
        "14t:a4", "4d:r03,f5,r10", "5m:r04,u1,L3", "5a:a5,C3", "5d:r05,r11", "6m:L4", "6a:a6,C4,r06", "7m:r12", "7a:a7", "8m:L5", "8a:a8,C5,r13")
TAIL = ("r14,g0,r15,r07,g1,r16,L7,C7,L6,C6,p80,q80,r08", "r17,p81,q81,n0,g2,r18,n1,z")


def ds(start, size, unit=8):
    return pl.ds(pl.multiple_of(start, unit), size)


def mod(p):
    return lax.rem(p + RING, RING)


def upto(n):
    return pl.ds(0, n)


def halves(n):
    return upto(n // 2), pl.ds(n // 2, n // 2)


def columns(row):
    return jnp.broadcast_to(row, (LANES, row.shape[1])).T


def near(src, dst, sem):
    return pltpu.make_async_copy(src, dst, sem)


def remote(src, dst, send, recv, to):
    return pltpu.make_async_remote_copy(src, dst, send, recv, device_id=to, device_id_type=pl.DeviceIdType.MESH)


def arrived(ref, sem):
    near(ref, ref, sem).wait()


def begin(copies):
    for c in copies:
        c.start()


def dot(a, b):
    return jnp.dot(a, b, preferred_element_type=F32)


def grad_logits(z, lse, rw, lab, col):
    lane = lax.broadcasted_iota(jnp.int32, z.shape, 1).astype(F32)
    p = jnp.exp(z - lse)
    return rw * jnp.where(lab - col == lane, p - 1.0, p)


class Torus:
    def __init__(self):
        self.tp, self.dp = lax.axis_index("tp"), lax.axis_index("dp")
        self.y, self.z = lax.rem(self.tp, RING), self.tp // RING
        self.x, self.core = self.dp // 2, lax.rem(self.dp, 2)
        self.mate = self.x + 1 - 2 * lax.rem(self.x, 2)
        self.far = RING - 1 - self.x
        self.opposite = RING - 1 - self.mate

    def side(self, swapped):
        return self.x // 2 if swapped else lax.rem((self.x + 1) // 2, 2)

    def chip(self, x, core=None):
        return {"tp": self.tp, "dp": 2 * x + (self.core if core is None else core)}

    def step(self, axis, d):
        y, z = (mod(self.y + d), self.z) if axis == 0 else (self.y, mod(self.z + d))
        return {"tp": z * RING + y, "dp": self.dp}

    def rings(self, s):
        ways = [functools.partial(self.step, a) for a in BOTH]
        return (self.y, ways[0], self.z, ways[1]) if s == 0 else (self.z, ways[1], self.y, ways[0])

    def others(self, axis):
        n, me = (lax.axis_size(axis), lax.axis_index(axis))
        return [{"tp": self.tp, "dp": self.dp, axis: lax.rem(me + d, n)} for d in range(1, n)]

    def greet(self):
        barrier = pltpu.get_barrier_semaphore()
        peers = self.others("tp") + self.others("dp")
        for peer in peers:
            pl.semaphore_signal(barrier, inc=1, device_id=peer, device_id_type=pl.DeviceIdType.MESH)
        return lambda: pl.semaphore_wait(barrier, len(peers))


class Exchange:
    def __init__(self, here, axis, src, land, send, recv):
        self.land, self.recv = land, recv
        me = lax.axis_index(axis)
        self.copies = lambda: [remote(src, land.at[me], send, recv, to) for to in here.others(axis)]
        self.rest = land.at[pl.ds(1, lax.axis_size(axis) - 1)]
        self.send, self.me = send, me

    def start(self, own):
        self.land[self.me] = own
        begin(self.copies())

    def blocks(self):
        arrived(self.rest, self.recv)
        return [self.land[i] for i in range(self.land.shape[0])]

    def drain(self):
        arrived(self.rest, self.send)


class Gather:
    def __init__(self, ref, rows, lanes, to, send, recv, own=None):
        self.ref, self.rows, self.to, self.send, self.recv = ref, rows, to, send, recv
        self.lanes = lanes
        self.own = ref.at[rows(0), lanes] if own is None else own
        self.size = rows(0).size

    def spread(self):
        dst = self.ref.at[self.rows(0), self.lanes]
        begin([remote(self.own, dst, self.send, self.recv.at[0], self.to(d)) for d in WAYS])

    def pass_on(self):
        arrived(self.ref.at[upto(2 * self.size), self.lanes], self.recv.at[0])
        n = self.lanes.size // 2
        for i, d in enumerate(WAYS):
            part = self.ref.at[self.rows(-d), pl.ds(self.lanes.start + i * n, n)]
            remote(part, part, self.send, self.recv.at[1], self.to(d)).start()

    def end(self):
        arrived(self.ref.at[upto(self.size), self.lanes], self.recv.at[1])


class Scatter:
    def __init__(self, src, rows, to, from_a, from_b, send, recv):
        self.src, self.rows, self.to, self.a, self.b, self.send, self.recv = src, rows, to, from_a, from_b, send, recv
        self.lanes = halves(src.shape[-1])

    def start(self):
        for i, d in enumerate(WAYS):
            remote(self.src.at[self.rows(2), self.lanes[i]], self.a.at[i], self.send, self.recv.at[0], self.to(d)).start()

    def rest(self):
        for i, d in enumerate(WAYS):
            other = self.lanes[1 - i]
            remote(self.src.at[self.rows(d), other], self.b.at[i, :, other], self.send, self.recv.at[1], self.to(d)).start()

    def middle(self, own):
        arrived(self.a, self.recv.at[0])
        for i, d in enumerate(WAYS):
            self.a[i] += own(i, d)
            remote(self.a.at[i], self.b.at[i, :, self.lanes[i]], self.send, self.recv.at[1], self.to(d)).start()

    def end(self):
        arrived(self.b, self.recv.at[1])


def slices(here, s):
    p1, _, p2, _ = here.rings(s)
    base = s * (SPREAD // 2)
    return (lambda o: ds(base + (p2 * RING + mod(p1 + o)) * SLICE, SLICE)), (lambda o: ds(base + mod(p2 + o) * RING * SLICE, RING * SLICE))


def plane_gather(here, ref, s, send, recv):
    _, to1, _, to2 = here.rings(s)
    one, many = slices(here, s)
    depth = ref.shape[-1]
    a = Gather(ref, one, upto(depth), to1, send.at[s], recv.at[s, 0])
    b, c = [Gather(ref, many, lanes, to2, send.at[s], recv.at[s, i + 1]) for i, lanes in enumerate(halves(depth))]

    def turn():
        a.end()
        b.spread()

    def end():
        b.end()
        c.end()

    def drain():
        arrived(ref.at[upto(3 * (RING + 1) * SLICE), :], send.at[s])

    return [a.spread, a.pass_on, turn, c.spread, b.pass_on, c.pass_on, end, drain]


def logits_kernel(hm, ht, gain_m, gain_t, lab_m, lab_t, wt_m, wt_t, w, z, u_out, up_out, far_u, du_out, st, lpart,
                  h_v, u_v, uf_v, got_v, w_v, z_v, e_v, x_v, m_v, s_v, t_v, lab_v, send_v, land, wsend, wland, pack,
                  sem_h, sem_u, sem_w, sem_z, sem_d, sem_k, es, er, ps, pr, gs, gr, xs, xr):
    seq, depth = hm.shape
    rows, vocab = z.shape
    steps = vocab // CHUNK
    here = Torus()
    mate, far = here.chip(here.mate), here.chip(here.far)

    def w_copy(i, slot):
        return near(w.at[:, ds(i * CHUNK, CHUNK, LANES)], w_v.at[slot], sem_w.at[slot])

    def z_copy(i, slot):
        return near(z_v.at[slot], z.at[:, ds(i * CHUNK, CHUNK, LANES)], sem_z.at[slot])

    loads = [near(src, h_v.at[pl.ds(i * seq, seq), :], sem_h.at[i]) for i, src in enumerate((hm, ht))]
    begin(loads + [w_copy(0, 0)])
    met = here.greet()
    m_v[:] = jnp.full_like(m_v, -jnp.inf)
    s_v[:] = jnp.zeros_like(s_v)
    t_v[:] = jnp.zeros_like(t_v)
    lab = jnp.concatenate([lab_m[:], lab_t[:]], axis=1).astype(F32) - (here.tp * vocab).astype(F32)
    lab_v[:] = columns(lab)
    top_row = lax.broadcasted_iota(jnp.int32, wsend.shape, 0) == 0
    wsend[:] = jnp.where(top_row, jnp.sum(wt_m[:]), jnp.sum(wt_t[:]))

    for half, gain in enumerate((gain_m, gain_t)):
        loads[half].wait()
        g = gain[:]

        @pl.loop(0, seq // LANES)
        def _(i):
            r = ds(half * seq + i * LANES, LANES)
            x = h_v[r, :].astype(F32)
            inv = lax.rsqrt(jnp.mean(x * x, axis=-1, keepdims=True) + NORM_EPS)
            u = (x * inv * g).astype(BF16)
            u_v[r, :] = u
            uf_v[r, :] = u.astype(F32)

    u_copy = near(u_v, u_out, sem_u)
    u_copy.start()
    with jax.named_scope("meet"):
        met()

    weights = Exchange(here, "dp", wsend, wland, es.at[0], er.at[0])
    weights.start(wsend[:])
    rest = pl.ds(SPREAD, rows - SPREAD)
    parts = [slices(here, s)[0](0) for s in BOTH] + [rest]

    def fetched(k, i):
        return remote(uf_v.at[parts[i], :], (got_v, far_u)[k].at[parts[i], :], xs.at[k, i], xr.at[k, i], (mate, far)[k])

    begin([fetched(k, i) for i in range(3) for k in BOTH])
    spread = [plane_gather(here, got_v, s, gs, gr) for s in BOTH]
    lane = lax.broadcasted_iota(jnp.int32, (rows, LANES), 1).astype(F32)

    @pl.loop(0, steps)
    def _(i):
        slot = lax.rem(i, 2)
        w_copy(i, slot).wait()

        @pl.when(i + 1 < steps)
        def _():
            w_copy(i + 1, 1 - slot).start()

        @pl.when(i >= 2)
        def _():
            z_copy(i - 2, slot).wait()

        m, s, t = m_v[:], s_v[:], t_v[:]
        rel = lab_v[:] - (i * CHUNK).astype(F32)
        for n in range(0, CHUNK, FEATS):
            for which, at in enumerate((0, 3 * FEATS)):
                for stage in range(3):
                    if n == at:
                        @pl.when(i == stage + 1)
                        def _():
                            if stage == 0:
                                arrived(got_v.at[parts[which], :], xr.at[0, which])
                            spread[which][stage]()
            zz = dot(u_v[:], w_v[slot, :, n:n + FEATS])
            z_v[slot, :, n:n + FEATS] = zz
            za, zb = zz[:, :LANES], zz[:, LANES:]
            new = jnp.maximum(m, jnp.maximum(za, zb))
            s = s * jnp.exp(m - new) + (jnp.exp(za - new) + jnp.exp(zb - new))
            t = jnp.where(rel == lane + n, za, t)
            t = jnp.where(rel == lane + (n + LANES), zb, t)
            m = new
        m_v[:], s_v[:], t_v[:] = m, s, t
        z_copy(i, slot).start()

    mt = m_v[:].T
    top = jnp.max(mt, axis=0, keepdims=True)
    total = jnp.sum(s_v[:].T * jnp.exp(mt - top), axis=0, keepdims=True)
    hit = jnp.sum(t_v[:].T, axis=0, keepdims=True)
    send_v[:] = jnp.where(lax.broadcasted_iota(jnp.int32, send_v.shape, 0) == 0, top + jnp.log(total), hit)
    stats = Exchange(here, "tp", send_v, land, es.at[1], er.at[1])
    stats.start(send_v[:])
    for stage in (3, 4):
        for which in BOTH:
            spread[which][stage]()
    sums = functools.reduce(jnp.add, weights.blocks())
    rw = jnp.concatenate([wt_m[:] * (1.0 / sums[0:1, 0:1]), wt_t[:] * (MTP_LAMBDA / sums[1:2, 0:1])], axis=1)
    with jax.named_scope("statwait"):
        blocks = stats.blocks()
    top = functools.reduce(jnp.maximum, blocks)
    lse = (top + jnp.log(functools.reduce(jnp.add, [jnp.exp(b - top) for b in blocks])))[0:1, :]
    hit = functools.reduce(jnp.add, blocks)[1:2, :]
    lpart[:] = jnp.broadcast_to(jnp.sum(rw * (lse - hit)), lpart.shape)
    row = lax.broadcasted_iota(jnp.int32, st.shape[1:], 0)
    st[1] = jnp.where(row == 0, lse, jnp.where(row == 1, rw, lab))
    pack[:] = st[1]
    swaps = [remote(pack, st.at[2 * k], ps.at[k], pr.at[k], to) for k, to in enumerate((mate, far))]
    begin(swaps)
    m_v[:] = columns(lse)
    s_v[:] = columns(rw)
    skip = LEFT - (steps - 2) * CHUNK
    at = 0
    for step, start in ((steps - 1, 0), (steps - 2, skip)):
        for c in range(start, CHUNK, LANES):
            e_v[:, at:at + LANES] = grad_logits(
                z_v[step % 2, :, c:c + LANES], m_v[:], s_v[:], lab_v[:], float(step * CHUNK + c)).astype(BF16)
            at += LANES

    def e_dot(r, cols):
        return (lax.dot_general(e_v[r, :CHUNK], w_v[(steps - 1) % 2, cols, :], NT, preferred_element_type=F32)
                + lax.dot_general(e_v[r, CHUNK:], w_v[(steps - 2) % 2, cols, skip:], NT, preferred_element_type=F32))

    for i in BOTH:
        for k in BOTH:
            fetched(k, i).wait_send()
    saves = []
    for dst, r in ((uf_v, slice(0, SPREAD)), (x_v, slice(SPREAD, rows))):
        for n in range(0, depth, TASK):
            dst[:r.stop - r.start, n:n + TASK] = e_dot(r, slice(n, n + TASK))
            src = dst.at[upto(r.stop - r.start), pl.ds(n, TASK)]
            saves.append(near(src, du_out.at[pl.ds(r.start, r.stop - r.start), pl.ds(n, TASK)], sem_d.at[len(saves)]))
            saves[-1].start()
            if len(saves) in (2, 3):
                spread[len(saves) - 2][5]()
    u_copy.wait()
    waits = [spread[0][6], spread[1][6], lambda: arrived(got_v.at[rest, :], xr.at[0, 2])]
    for i, wait in enumerate(waits):
        start = i * (SPREAD // 2)
        r = pl.ds(start, min(SPREAD // 2, rows - start))
        with jax.named_scope("land"):
            wait()

        @pl.loop(start // LANES, (start + r.size) // LANES)
        def _(j):
            part = ds(j * LANES, LANES)
            u_v[part, :] = got_v[part, :].astype(BF16)

        saves.append(near(u_v.at[r, :], up_out.at[r, :], sem_k.at[i]))
        saves[-1].start()
    for c in swaps:
        c.wait()
    for i in range(3):
        arrived(far_u.at[parts[i], :], xr.at[1, i])
    weights.drain()
    stats.drain()
    for k in BOTH:
        spread[k][7]()
        fetched(k, 2).wait_send()
        z_copy(steps - 2 + k, (steps + k) % 2).wait()
    for c in saves:
        c.wait()


def logits(hm, ht, gain_m, gain_t, lab_m, lab_t, wt_m, wt_t, w):
    seq, depth = hm.shape
    rows, vocab = 2 * seq, w.shape[1]
    n_tp, n_dp = lax.axis_size("tp"), lax.axis_size("dp")
    shape = jax.ShapeDtypeStruct
    stat = pltpu.VMEM((rows, LANES), F32)
    return pl.pallas_call(
        logits_kernel,
        out_shape=(shape((rows, vocab), F32), shape((rows, depth), BF16), shape((rows, depth), BF16), shape((rows, depth), F32),
                   shape((rows, depth), F32), shape((3, 8, rows), F32), shape((8, LANES), F32)),
        in_specs=[ANY, ANY] + [VMEM] * 6 + [ANY],
        out_specs=(ANY,) * 5 + (VMEM, VMEM),
        scratch_shapes=[
            pltpu.VMEM((rows, depth), BF16), pltpu.VMEM((rows, depth), BF16), pltpu.VMEM((rows, depth), F32), pltpu.VMEM((rows, depth), F32),
            pltpu.VMEM((2, depth, CHUNK), BF16), pltpu.VMEM((2, rows, CHUNK), F32), pltpu.VMEM((rows, vocab - LEFT), BF16),
            pltpu.VMEM((rows - SPREAD, depth), F32), stat, stat, stat, stat,
            pltpu.VMEM((2, rows), F32), pltpu.VMEM((n_tp, 2, rows), F32), pltpu.VMEM((8, LANES), F32), pltpu.VMEM((n_dp, 8, LANES), F32),
            pltpu.VMEM((8, rows), F32),
            TWO, DMA, TWO, TWO, DMA((2 * depth // TASK,)), DMA((3,)), TWO, TWO, TWO, TWO,
            TWO, DMA((2, 3, 2)), *[DMA((2, 3))] * 2,
        ],
        compiler_params=pltpu.CompilerParams(vmem_limit_bytes=VMEM_LIMIT, collective_id=0, has_side_effects=True),
        name="logits",
    )(hm, ht, gain_m, gain_t, lab_m, lab_t, wt_m, wt_t, w)


def chunk_table():
    out, at, used = [], 0, [0, 0]
    for i, kind in enumerate(KINDS):
        width, swapped = (WIDE if i else FIRST), int(kind == "s")
        out.append((at, width, swapped, used[swapped]))
        at, used[swapped] = at + width, used[swapped] + width
    return out, used


def column(here, used, swapped, other, offset):
    base = [2 * used[0] * s + abs(here.side(s) - other) * used[s] for s in BOTH]
    return jnp.where(swapped == 1, base[1], base[0]) + offset


def pick(values, k):
    if isinstance(k, int):
        return values[k]
    return functools.reduce(lambda out, i: jnp.where(k == i, values[i], out), range(1, len(values)), jnp.int32(values[0]))


def head_kernel(hm, ht, gain_m, gain_t, u_own, u_par, far_in, z, w, st, du_in, lpart,
                fin, gh, ghb, du, far_u, one, tot, u_v, w_v, z_v, et_v, g_v, own_v, sum_v, one_v, acc_v,
                lse_v, rw_v, lab_v, ra_v, rl_v, rb_v, rm_v, ra2_v, rb2_v, rh_v, gg_v, gland, tland, tsend,
                sem_u, sem_w, sem_z, sem_a, sem_o, sem_1, d_send, d_recv, b_send, b_recv, f_send, f_recv,
                gs, gr, ss, sr, sem_l, sem_x, es, er):
    del far_in
    rows, depth = u_own.shape
    seq = rows // 2
    here = Torus()
    x, core = here.x, here.core
    met = here.greet()
    table, used = chunk_table()
    starts, _, swaps, offsets = (list(t) for t in zip(*table))
    last = len(table) - 1

    def span(k):
        return upto(FIRST) if isinstance(k, int) and k == 0 else ds(FIRST + (k - 1) * WIDE, WIDE, LANES)

    def chips(k):
        s = pick(swaps, k) == 1
        return jnp.where(s, here.far, here.mate), jnp.where(s, here.mate, here.far)

    def block(i):
        return ds((2 * lax.rem(i, RING) + jnp.where(i < RING, 1 - core, core)) * FEATS, FEATS, FEATS)

    def feats(i):
        return pl.ds(i * FEATS, FEATS)

    def w_copies(col, width, slot):
        return [near(w.at[block(i), ds(col, width, LANES)], w_v.at[slot, feats(i), upto(width)], sem_w.at[slot]) for i in range(2 * RING)]

    def u_copies(k):
        src, r = ((u_par, upto(rows)), (u_own, pl.ds(rows, rows)))[k]
        return [near(src.at[:, block(i)], u_v.at[r, feats(i)], sem_u.at[k]) for i in range(2 * RING)]

    def u_wait(k):
        arrived(u_v.at[upto(rows), :], sem_u.at[k])

    def fetch(k, slot):
        width = span(k).size
        col = column(here, used, pick(swaps, k), 0, pick(offsets, k))
        begin(w_copies(col, width, slot) + [near(z.at[:, ds(col, width, LANES)], z_v.at[slot, :, upto(width)], sem_z.at[slot])])

    per = LEFT // TASK

    def piece(t):
        return t < 2 * per, t // per, lax.rem(t, per)

    def acc_copies(h, back):
        refs = [(acc_v.at[:, feats(i)], (du if back else du_in).at[ds(h * seq, seq), block(i)]) for i in range(2 * RING)]
        return [near(*(p if back else p[::-1]), sem_a) for p in refs]

    def task_fetch(t, slot):
        of_du, h, i = piece(t)

        @pl.when(of_du)
        def _():
            begin(w_copies(i * TASK, TASK, slot))
            near(z.at[ds(h * seq, seq), ds(i * TASK, TASK, LANES)], z_v.at[slot, upto(seq), :], sem_z.at[slot]).start()

        @pl.when(~of_du)
        def _():
            begin([near(far_u.at[:, block(2 * i + j)], z_v.at[slot, :, feats(j)], sem_z.at[slot]) for j in BOTH])

    def task(t, slot):
        of_du, h, i = piece(t)

        @pl.when(~of_du)
        def _():
            arrived(z_v.at[slot], sem_z.at[slot])
            u_v[pl.ds(2 * rows, rows), ds(i * TASK, TASK, LANES)] = z_v[slot].astype(BF16)

        @pl.when(of_du)
        def _():
            arrived(w_v.at[slot], sem_w.at[slot])
            arrived(z_v.at[slot, upto(seq), :], sem_z.at[slot])

            @pl.when(i == 0)
            def _():
                arrived(acc_v, sem_a)

            r = ds(rows + h * seq, seq)
            col = (i * TASK).astype(F32)
            for g in range(0, TASK, LANES):
                cols = slice(g, g + LANES)
                et_v[:, cols] = grad_logits(z_v[slot, :seq, cols], lse_v[r, :], rw_v[r, :], lab_v[r, :], col + g).astype(BF16)
            for m in range(0, depth, TASK):
                cols = slice(m, m + TASK)
                acc_v[:, cols] += lax.dot_general(et_v[:, :TASK], w_v[slot, cols, :], NT, preferred_element_type=F32)

            @pl.when(i == per - 1)
            def _():
                acc_v[:] = acc_v[:].astype(BF16).astype(F32)
                begin(acc_copies(h, True))
                arrived(acc_v, sem_a)

            @pl.when((i == per - 1) & (h == 0))
            def _():
                begin(acc_copies(1, False))

    def d_copy(k, part):
        lanes, width = pl.ds(part * TASK, TASK), span(k).size
        return remote(g_v.at[upto(width), lanes], sum_v.at[span(k), lanes], d_send, d_recv.at[k], here.chip(x, 1 - core))

    def b_copy(k, which):
        to = chips(k)[1]
        block_of = ds(jnp.where(which == 0, here.opposite, to) * FEATS, FEATS, FEATS)
        return remote(sum_v.at[span(k), block_of], one.at[which, span(k), :], b_send, b_recv.at[k, which], here.chip(to))

    def f_copy(k):
        mate = chips(k)[0]
        return remote(sum_v.at[span(k), ds(mate * FEATS, FEATS, FEATS)], fin.at[1, span(k), :], f_send, f_recv, here.chip(mate))

    def o_copy(k):
        return near(sum_v.at[span(k), ds(x * FEATS, FEATS, FEATS)], fin.at[0, span(k), :], sem_o)

    def make(k, slot, late=lambda: None, middle=lambda: None):
        width = span(k).size
        swapped = pick(swaps, k)
        col = column(here, used, swapped, 0, pick(offsets, k)).astype(F32)
        arrived(w_v.at[slot, :, upto(width)], sem_w.at[slot])
        arrived(z_v.at[slot, :, upto(width)], sem_z.at[slot])

        def put(zz, r, c, at):
            e = grad_logits(zz, lse_v[r, :], rw_v[r, :], lab_v[r, :], col + c)
            et_v[c:c + LANES, ds(at, rows, rows)] = e.T.astype(BF16)

        for c in range(0, width, LANES):
            put(z_v[slot, :, c:c + LANES], pl.ds(rows, rows), c, rows * (1 - swapped))
        late()
        other = ds(2 * rows * swapped, rows, rows)
        for n in range(0, width, FEATS):
            step = min(width - n, FEATS)
            zz = dot(u_v[other, :], w_v[slot, :, n:n + step])
            for c in range(0, step, LANES):
                put(zz[:, c:c + LANES], other, n + c, rows * swapped)
        middle()
        both = ds(rows * swapped, 2 * rows, rows)
        et = et_v[upto(width), :]
        for part in BOTH:
            lanes = pl.ds(part * TASK, TASK)
            g_v[upto(width), lanes] = dot(et, u_v[both, lanes])
            d_copy(k, part).start()
        own_v[upto(width), :] = dot(et, u_v[both, pl.ds(2 * TASK, 2 * TASK)])

    def add(k):
        arrived(sum_v.at[span(k), :], d_recv.at[k])
        sum_v[span(k), :] += own_v[upto(span(k).size), :]
        begin([b_copy(k, which) for which in BOTH])

    def landing(k, which):
        return near(one.at[which, span(k), :], one_v.at[which, upto(span(k).size), :], sem_1.at[which])

    def land(k, which):
        with jax.named_scope("bwait"):
            arrived(one.at[which, span(k), :], b_recv.at[k, which])
        landing(k, which).start()

    def close(k, which):
        landing(k, which).wait()
        chip = jnp.where(which == 0, chips(k)[0], x)
        sum_v[span(k), ds(chip * FEATS, FEATS, FEATS)] += one_v[which, upto(span(k).size), :]
        (o_copy if which else f_copy)(k).start()

    def ring(h, s):
        q = 2 * h + s
        p1, to1, p2, to2 = here.rings(s)
        big, small = seq // 2 // RING, seq // 2 // RING // RING
        base = h * seq + s * (seq // 2)
        one_of = lambda o: ds(base + mod(p1 + o) * big, big)
        two_of = lambda o: ds(base + p1 * big + mod(p2 + o) * small, small)
        sub = lambda o: ds(mod(p2 + o) * small, small)
        every = upto(depth)
        first = Scatter(du, one_of, to1, ra_v.at[q], rb_v.at[q], ss.at[q], sr.at[q, 0])
        second = Scatter(rm_v.at[q], sub, to2, ra2_v.at[q], rb2_v.at[q], ss.at[q], sr.at[q, 1])
        down = Gather(gh, two_of, every, to2, ss.at[q], sr.at[q, 2], rm_v.at[q, sub(0), :])
        up = Gather(gh, one_of, every, to1, ss.at[q], sr.at[q, 3])
        lanes = halves(depth)
        h_rows = ds(s * (seq // 2) + p1 * big + p2 * small, small)
        loads = lambda: [near(du.at[one_of(WAYS[i]), lanes[i]], rl_v.at[s, i], sem_l.at[s, i]) for i in BOTH] + [
            near(du.at[one_of(0), :], rm_v.at[q], sem_l.at[s, 2]), near((hm, ht)[h].at[h_rows, :], rh_v.at[q], sem_l.at[s, 3])]
        keep = lambda: near(rm_v.at[q, sub(0), :], gh.at[two_of(0), :], sem_x.at[q])
        return q, sub, lanes, first, second, down, up, loads, keep

    def event(h, stage):
        for s in BOTH:
            q, sub, lanes, first, second, down, up, loads, keep = ring(h, s)
            if stage == 0:
                first.start()
                begin(loads())
            if stage == 1:
                for c in loads():
                    c.wait()
                first.middle(lambda i, d: rl_v[s, i])
            if stage == 2:
                first.end()
                rm_v[q] += rb_v[q, 0] + rb_v[q, 1]
                second.start()
                second.rest()
            if stage == 3:
                second.middle(lambda i, d: rm_v[q, sub(d), lanes[i]])
            if stage == 4:
                second.end()
                gu = rm_v[q, sub(0), :] + (rb2_v[q, 0] + rb2_v[q, 1])
                xr = rh_v[q].astype(F32)
                inv = lax.rsqrt(jnp.mean(xr * xr, axis=-1, keepdims=True) + NORM_EPS)
                normed = xr * inv
                gn = gu * (gain_m, gain_t)[h][:]
                gx = inv * (gn - normed * jnp.mean(gn * normed, axis=-1, keepdims=True))
                rm_v[q, sub(0), :] = gx.astype(BF16).astype(F32)
                part = jnp.sum(gu * normed, axis=0, keepdims=True)
                gg_v[pl.ds(h, 1), :] = part if s == 0 else gg_v[pl.ds(h, 1), :] + part
                keep().start()
                down.spread()
            if stage == 5:
                down.pass_on()
            if stage == 6:
                keep().wait()
                down.end()
                up.spread()
            if stage == 7:
                up.pass_on()
            if stage == 8:
                up.end()

    def rest(h):
        for s in BOTH:
            ring(h, s)[3].rest()

    plane = Exchange(here, "tp", gg_v, gland, es.at[0], er.at[0])
    line = Exchange(here, "dp", tsend, tland, es.at[1], er.at[1])

    def sums(stage):
        if stage == 0:
            plane.start(gg_v[:])
        if stage == 1:
            total = functools.reduce(jnp.add, plane.blocks())
            tsend[:] = jnp.concatenate([total, jnp.broadcast_to(lpart[0:1, 0:1], total.shape)])
            line.start(tsend[:])
        if stage == 2:
            tot[:] = functools.reduce(jnp.add, line.blocks())

    def narrow(h):
        r = ds(h * seq, seq)
        c = near(gh.at[r, :], acc_v, sem_a)
        c.start()
        c.wait()
        u_v[r, :] = acc_v[:].astype(BF16)
        near(u_v.at[r, :], ghb.at[r, :], sem_x.at[h]).start()

    far_steps = [plane_gather(here, far_u, s, gs, gr) for s in BOTH]

    def far_event(stage):
        for s in BOTH:
            for i in ((stage - 1,), (2, 3), (4, 5), (6,))[max(stage - 2, 0)]:
                far_steps[s][i]()

    def drain():
        rows_sent = 6 * (seq // 2 // RING + seq // 2 // RING // RING)
        for q in range(4):
            arrived(du.at[upto(rows_sent), :], ss.at[q])
        for s in BOTH:
            far_steps[s][7]()
        plane.drain()
        line.drain()
        arrived(sum_v.at[:, upto(2 * FEATS)], b_send)
        arrived(g_v, d_send)

    def both(act):
        return lambda k: [act(k, which) for which in BOTH]

    verbs = {"r": event, "u": rest, "g": sums, "n": narrow, "f": far_event, "a": add, "L": both(land), "C": both(close), "p": land, "q": close, "z": drain}

    def run(text):
        for word in text.split(","):
            with jax.named_scope(word):
                verbs[word[0]](*(int(c) for c in word[1:]))

    def at_point(k, point):
        for at, text in (a.split(":") for a in ACTS):
            if at[-1] == point:
                @pl.when(k == int(at[:-1]))
                def _():
                    run(text)

    fetch(0, 0)
    begin(u_copies(0))

    def spread_stats(k):
        for i, ref in enumerate((lse_v, rw_v, lab_v)):
            ref[pl.ds(k * rows, rows), :] = columns(st[k, i:i + 1, :])

    spread_stats(1)

    def before_other():
        spread_stats(0)
        u_wait(0)
        begin(u_copies(1))

    def before_sends():
        u_wait(1)
        fetch(1, 1)
        begin(acc_copies(0, False))
        with jax.named_scope("meet"):
            met()
        far_event(1)

    with jax.named_scope("make0"):
        make(0, 0, before_other, before_sends)
    spread_stats(2)
    add(0)

    @pl.loop(1, last + 1)
    def _(k):
        lo, hi = pick(DONE[:1] + DONE[:-1], k), pick(DONE, k)
        slot = lax.rem(k + lo, 2)

        def more(t):
            @pl.when(t < hi)
            def _():
                task_fetch(t, lax.rem(k + 1 + t, 2))

            @pl.when((t == hi) & (k < last))
            def _():
                fetch(k + 1, lax.rem(k + 1 + t, 2))

        more(lo)

        def middle():
            at_point(k, "m")

            @pl.when(k == 1)
            def _():
                arrived(g_v.at[upto(FIRST), :], d_send)

            @pl.when(k > 1)
            def _():
                arrived(g_v, d_send)

        with jax.named_scope("make"):
            make(k, slot, middle=middle)

        at_point(k, "a")

        @pl.loop(lo, hi)
        def _(t):
            at_point(t, "t")
            more(t + 1)
            with jax.named_scope("task"):
                task(t, lax.rem(k + 1 + t, 2))

        at_point(k, "d")

    for text in TAIL:
        run(text)
    with jax.named_scope("tail"):
        arrived(fin.at[1], f_send)
        arrived(fin.at[1], f_recv)
        arrived(fin.at[0], sem_o)
        for h in BOTH:
            arrived(ghb.at[upto(seq), :], sem_x.at[h])


def head_grad(hm, ht, gain_m, gain_t, u_own, u_par, far_u, z, w, st, du_in, lpart):
    rows, depth = u_own.shape
    seq = rows // 2
    half = z.shape[1] // 2
    n_tp, n_dp, n = lax.axis_size("tp"), lax.axis_size("dp"), len(KINDS)
    big, small = seq // 2 // RING, seq // 2 // RING // RING
    shape = jax.ShapeDtypeStruct
    stat = pltpu.VMEM((3 * rows, LANES), F32)
    return pl.pallas_call(
        head_kernel,
        out_shape=(shape((2, half, FEATS), F32), shape((rows, depth), F32), shape((rows, depth), BF16), shape((rows, depth), F32),
                   shape((rows, depth), F32), shape((2, half, FEATS), F32), shape((4, depth), F32)),
        in_specs=[ANY, ANY, VMEM, VMEM] + [ANY] * 5 + [VMEM, ANY, VMEM],
        out_specs=(ANY,) * 6 + (VMEM,),
        scratch_shapes=[
            pltpu.VMEM((3 * rows, depth), BF16), pltpu.VMEM((2, depth, TASK), BF16), pltpu.VMEM((2, rows, TASK), F32),
            pltpu.VMEM((TASK, 2 * rows), BF16), pltpu.VMEM((WIDE, 2 * TASK), F32), pltpu.VMEM((WIDE, 2 * TASK), F32),
            pltpu.VMEM((half, 2 * TASK), F32), pltpu.VMEM((2, WIDE, FEATS), F32), pltpu.VMEM((seq, depth), F32),
            stat, stat, stat,
            pltpu.VMEM((4, 2, big, depth // 2), F32), pltpu.VMEM((2, 2, big, depth // 2), F32), pltpu.VMEM((4, 2, big, depth), F32),
            pltpu.VMEM((4, big, depth), F32), pltpu.VMEM((4, 2, small, depth // 2), F32), pltpu.VMEM((4, 2, small, depth), F32),
            pltpu.VMEM((4, small, depth), BF16),
            pltpu.VMEM((2, depth), F32), pltpu.VMEM((n_tp, 2, depth), F32), pltpu.VMEM((n_dp, 4, depth), F32), pltpu.VMEM((4, depth), F32),
            TWO, TWO, TWO, DMA, DMA, TWO, DMA, DMA((n,)), DMA, DMA((n, 2)), DMA, DMA,
            TWO, DMA((2, 3, 2)), DMA((4,)), DMA((4, 4, 2)), DMA((2, 4)), DMA((4,)), TWO, TWO,
        ],
        input_output_aliases={6: 4},
        compiler_params=pltpu.CompilerParams(vmem_limit_bytes=VMEM_LIMIT, collective_id=1, has_side_effects=True),
        name="head_grad",
    )(hm, ht, gain_m, gain_t, u_own, u_par, far_u, z, w, st, du_in, lpart)


def finish_kernel(fin, gh, tot, out, gm, gt, loss, ggm, ggt, f_v, o_v, g_v, sem_f, sem_o, sem_g):
    seq = gm.shape[0]
    table, used = chunk_table()
    jobs = [(k, *t) for t in table for k in BOTH]
    here = Torus()

    def f_in(i):
        k, at, width, _, _ = jobs[i]
        return near(fin.at[k, pl.ds(at, width), :], f_v.at[k, pl.ds(at, width), :], sem_f.at[i])

    def f_out(i):
        k, at, width, swapped, offset = jobs[i]
        return near(o_v.at[k, :, pl.ds(at, width)], out.at[:, ds(column(here, used, swapped, k, offset), width, LANES)], sem_o.at[i])

    g_in = [near(gh.at[pl.ds(h * seq, seq), :], g_v.at[h], sem_g.at[h]) for h in BOTH]
    begin([f_in(i) for i in range(WINDOW)])
    ggm[:], ggt[:], loss[:] = tot[0:1, :], tot[1:2, :], tot[2:3, 0:1]
    outs = [f_out(i) for i in range(len(jobs))] + [near(g_v.at[h], (gm, gt)[h], sem_g.at[h]) for h in BOTH]
    for i, (k, at, width, _, _) in enumerate(jobs):
        begin([f_in(i + WINDOW)] if i + WINDOW < len(jobs) else [g_in[i % 2]] if i + 2 >= len(jobs) else [])
        f_in(i).wait()
        o_v[k, :, pl.ds(at, width)] = f_v[k, pl.ds(at, width), :].T
        outs[i].start()
    for h in BOTH:
        g_in[h].wait()
        outs[h - 2].start()
    for c in outs:
        c.wait()


def finish(fin, gh, tot):
    _, half, block = fin.shape
    seq, depth = gh.shape[0] // 2, gh.shape[1]
    shape, row, jobs = jax.ShapeDtypeStruct, jax.ShapeDtypeStruct((1, depth), F32), DMA((2 * len(KINDS),))
    return pl.pallas_call(
        finish_kernel,
        out_shape=(shape((block, 2 * half), F32), shape((seq, depth), BF16), shape((seq, depth), BF16), shape((1, 1), F32), row, row),
        in_specs=[ANY, ANY, VMEM],
        out_specs=(ANY, ANY, ANY, VMEM, VMEM, VMEM),
        scratch_shapes=[pltpu.VMEM((2, half, block), F32), pltpu.VMEM((2, block, half), F32), pltpu.VMEM((2, seq, depth), BF16), jobs, jobs, TWO],
        compiler_params=pltpu.CompilerParams(vmem_limit_bytes=VMEM_LIMIT),
        name="finish",
    )(fin, gh, tot)


def solution(mesh):
    def local_step(h_main, h_mtp, labels_main, labels_mtp, weight_main, weight_mtp, gain_final, gain_mtp, w_out):
        hm, ht, gm, gt = h_main[0], h_mtp[0], gain_final[None], gain_mtp[None]
        z, u_own, u_par, far_u, du_in, st, lpart = logits(hm, ht, gm, gt, labels_main, labels_mtp, weight_main, weight_mtp, w_out)
        fin, _, gh, _, _, _, tot = head_grad(hm, ht, gm, gt, u_own, u_par, far_u, z, w_out, st, du_in, lpart)
        grad_w, gh_m, gh_t, loss, gg_m, gg_t = finish(fin, gh, tot)
        return loss[0, 0], gh_m[None], gh_t[None], grad_w, gg_m[0], gg_t[0]

    wide, row = P("dp", None, None), P("dp", None)
    return jax.shard_map(
        local_step,
        mesh=mesh,
        in_specs=(wide, wide, row, row, row, row, P(None), P(None), P(None, "tp")),
        out_specs=(P(), wide, wide, P("dp", "tp"), P(None), P(None)),
        check_vma=False,
    )
```

```python
import functools

import jax
import jax.numpy as jnp
from jax import lax
from jax.experimental import pallas as pl
from jax.experimental.pallas import tpu as pltpu
from jax.sharding import PartitionSpec as P

NORM_EPS = 1e-6
MTP_LAMBDA = 0.3
F32, BF16 = jnp.float32, jnp.bfloat16
DMA = pltpu.SemaphoreType.DMA
TWO = DMA((2,))
ANY = pl.BlockSpec(memory_space=pl.ANY)
VMEM = pl.BlockSpec(memory_space=pltpu.VMEM)
VMEM_LIMIT = 67043328
WINDOW = 17
LANES, FEATS = 128, 256
RING = 4
WAYS = (1, -1)
BOTH = range(2)
NT = (((1,), (1,)), ((), ()))
CHUNK = 1280
LEFT = 4096
SLICE = 24
SPREAD = 2 * RING * RING * SLICE
FIRST, WIDE = 128, 384
TASK = 512
KINDS = "nnnnnnnsn"
DONE = (0, 5, 8, 14, 16) + 4 * (20,)
ACTS = ("1m:f2", "1a:a1", "1t:f3", "2t:L0", "4t:C0", "2a:a2", "2d:r00,u0,L1", "3m:C1", "8t:a3", "9t:r01", "13t:f4", "4m:r02,L2", "4a:C2",
        "14t:a4", "4d:r03,f5,r10", "5m:r04,u1,L3", "5a:a5,C3", "5d:r05,r11", "6m:L4", "6a:a6,C4,r06", "7m:r12", "7a:a7", "8m:L5", "8a:a8,C5,r13")
TAIL = ("r14,g0,r15,r07,g1,r16,L7,C7,L6,C6,p80,q80,r08", "r17,p81,q81,n0,g2,r18,n1,z")


def ds(start, size, unit=8):
    return pl.ds(pl.multiple_of(start, unit), size)


def mod(p):
    return lax.rem(p + RING, RING)


def upto(n):
    return pl.ds(0, n)


def halves(n):
    return upto(n // 2), pl.ds(n // 2, n // 2)


def columns(row):
    return jnp.broadcast_to(row, (LANES, row.shape[1])).T


def near(src, dst, sem):
    return pltpu.make_async_copy(src, dst, sem)


def remote(src, dst, send, recv, to):
    return pltpu.make_async_remote_copy(src, dst, send, recv, device_id=to, device_id_type=pl.DeviceIdType.MESH)


def arrived(ref, sem):
    near(ref, ref, sem).wait()


def begin(copies):
    for c in copies:
        c.start()


def dot(a, b):
    return jnp.dot(a, b, preferred_element_type=F32)


def grad_logits(z, lse, rw, lab, col):
    lane = lax.broadcasted_iota(jnp.int32, z.shape, 1).astype(F32)
    p = jnp.exp(z - lse)
    return rw * jnp.where(lab - col == lane, p - 1.0, p)


class Torus:
    def __init__(self):
        self.tp, self.dp = lax.axis_index("tp"), lax.axis_index("dp")
        self.y, self.z = lax.rem(self.tp, RING), self.tp // RING
        self.x, self.core = self.dp // 2, lax.rem(self.dp, 2)
        self.mate = self.x + 1 - 2 * lax.rem(self.x, 2)
        self.far = RING - 1 - self.x
        self.opposite = RING - 1 - self.mate

    def side(self, swapped):
        return self.x // 2 if swapped else lax.rem((self.x + 1) // 2, 2)

    def chip(self, x, core=None):
        return {"tp": self.tp, "dp": 2 * x + (self.core if core is None else core)}

    def step(self, axis, d):
        y, z = (mod(self.y + d), self.z) if axis == 0 else (self.y, mod(self.z + d))
        return {"tp": z * RING + y, "dp": self.dp}

    def rings(self, s):
        ways = [functools.partial(self.step, a) for a in BOTH]
        return (self.y, ways[0], self.z, ways[1]) if s == 0 else (self.z, ways[1], self.y, ways[0])

    def others(self, axis):
        n, me = (lax.axis_size(axis), lax.axis_index(axis))
        return [{"tp": self.tp, "dp": self.dp, axis: lax.rem(me + d, n)} for d in range(1, n)]

    def greet(self):
        barrier = pltpu.get_barrier_semaphore()
        peers = self.others("tp") + self.others("dp")
        for peer in peers:
            pl.semaphore_signal(barrier, inc=1, device_id=peer, device_id_type=pl.DeviceIdType.MESH)
        return lambda: pl.semaphore_wait(barrier, len(peers))


class Exchange:
    def __init__(self, here, axis, src, land, send, recv):
        self.land, self.recv = land, recv
        me = lax.axis_index(axis)
        self.copies = lambda: [remote(src, land.at[me], send, recv, to) for to in here.others(axis)]
        self.rest = land.at[pl.ds(1, lax.axis_size(axis) - 1)]
        self.send, self.me = send, me

    def start(self, own):
        self.land[self.me] = own
        begin(self.copies())

    def blocks(self):
        arrived(self.rest, self.recv)
        return [self.land[i] for i in range(self.land.shape[0])]

    def drain(self):
        arrived(self.rest, self.send)


class Gather:
    def __init__(self, ref, rows, lanes, to, send, recv, own=None):
        self.ref, self.rows, self.to, self.send, self.recv = ref, rows, to, send, recv
        self.lanes = lanes
        self.own = ref.at[rows(0), lanes] if own is None else own
        self.size = rows(0).size

    def spread(self):
        dst = self.ref.at[self.rows(0), self.lanes]
        begin([remote(self.own, dst, self.send, self.recv.at[0], self.to(d)) for d in WAYS])

    def pass_on(self):
        arrived(self.ref.at[upto(2 * self.size), self.lanes], self.recv.at[0])
        n = self.lanes.size // 2
        for i, d in enumerate(WAYS):
            part = self.ref.at[self.rows(-d), pl.ds(self.lanes.start + i * n, n)]
            remote(part, part, self.send, self.recv.at[1], self.to(d)).start()

    def end(self):
        arrived(self.ref.at[upto(self.size), self.lanes], self.recv.at[1])


class Scatter:
    def __init__(self, src, rows, to, from_a, from_b, send, recv):
        self.src, self.rows, self.to, self.a, self.b, self.send, self.recv = src, rows, to, from_a, from_b, send, recv
        self.lanes = halves(src.shape[-1])

    def start(self):
        for i, d in enumerate(WAYS):
            remote(self.src.at[self.rows(2), self.lanes[i]], self.a.at[i], self.send, self.recv.at[0], self.to(d)).start()

    def rest(self):
        for i, d in enumerate(WAYS):
            other = self.lanes[1 - i]
            remote(self.src.at[self.rows(d), other], self.b.at[i, :, other], self.send, self.recv.at[1], self.to(d)).start()

    def middle(self, own):
        arrived(self.a, self.recv.at[0])
        for i, d in enumerate(WAYS):
            self.a[i] += own(i, d)
            remote(self.a.at[i], self.b.at[i, :, self.lanes[i]], self.send, self.recv.at[1], self.to(d)).start()

    def end(self):
        arrived(self.b, self.recv.at[1])


def slices(here, s):
    p1, _, p2, _ = here.rings(s)
    base = s * (SPREAD // 2)
    return (lambda o: ds(base + (p2 * RING + mod(p1 + o)) * SLICE, SLICE)), (lambda o: ds(base + mod(p2 + o) * RING * SLICE, RING * SLICE))


def plane_gather(here, ref, s, send, recv):
    _, to1, _, to2 = here.rings(s)
    one, many = slices(here, s)
    depth = ref.shape[-1]
    a = Gather(ref, one, upto(depth), to1, send.at[s], recv.at[s, 0])
    b, c = [Gather(ref, many, lanes, to2, send.at[s], recv.at[s, i + 1]) for i, lanes in enumerate(halves(depth))]

    def turn():
        a.end()
        b.spread()

    def end():
        b.end()
        c.end()

    def drain():
        arrived(ref.at[upto(3 * (RING + 1) * SLICE), :], send.at[s])

    return [a.spread, a.pass_on, turn, c.spread, b.pass_on, c.pass_on, end, drain]


def logits_kernel(hm, ht, gain_m, gain_t, lab_m, lab_t, wt_m, wt_t, w, z, u_out, up_out, far_u, du_out, st, lpart,
                  h_v, u_v, uf_v, got_v, w_v, z_v, e_v, x_v, m_v, s_v, t_v, lab_v, send_v, land, wsend, wland, pack,
                  sem_h, sem_u, sem_w, sem_z, sem_d, sem_k, es, er, ps, pr, gs, gr, xs, xr):
    seq, depth = hm.shape
    rows, vocab = z.shape
    steps = vocab // CHUNK
    here = Torus()
    mate, far = here.chip(here.mate), here.chip(here.far)

    def w_copy(i, slot):
        return near(w.at[:, ds(i * CHUNK, CHUNK, LANES)], w_v.at[slot], sem_w.at[slot])

    def z_copy(i, slot):
        return near(z_v.at[slot], z.at[:, ds(i * CHUNK, CHUNK, LANES)], sem_z.at[slot])

    loads = [near(src, h_v.at[pl.ds(i * seq, seq), :], sem_h.at[i]) for i, src in enumerate((hm, ht))]
    begin(loads + [w_copy(0, 0)])
    met = here.greet()
    m_v[:] = jnp.full_like(m_v, -jnp.inf)
    s_v[:] = jnp.zeros_like(s_v)
    t_v[:] = jnp.zeros_like(t_v)
    lab = jnp.concatenate([lab_m[:], lab_t[:]], axis=1).astype(F32) - (here.tp * vocab).astype(F32)
    lab_v[:] = columns(lab)
    top_row = lax.broadcasted_iota(jnp.int32, wsend.shape, 0) == 0
    wsend[:] = jnp.where(top_row, jnp.sum(wt_m[:]), jnp.sum(wt_t[:]))

    for half, gain in enumerate((gain_m, gain_t)):
        loads[half].wait()
        g = gain[:]

        @pl.loop(0, seq // LANES)
        def _(i):
            r = ds(half * seq + i * LANES, LANES)
            x = h_v[r, :].astype(F32)
            inv = lax.rsqrt(jnp.mean(x * x, axis=-1, keepdims=True) + NORM_EPS)
            u = (x * inv * g).astype(BF16)
            u_v[r, :] = u
            uf_v[r, :] = u.astype(F32)

    u_copy = near(u_v, u_out, sem_u)
    u_copy.start()
    with jax.named_scope("meet"):
        met()

    weights = Exchange(here, "dp", wsend, wland, es.at[0], er.at[0])
    weights.start(wsend[:])
    rest = pl.ds(SPREAD, rows - SPREAD)
    parts = [slices(here, s)[0](0) for s in BOTH] + [rest]

    def fetched(k, i):
        return remote(uf_v.at[parts[i], :], (got_v, far_u)[k].at[parts[i], :], xs.at[k, i], xr.at[k, i], (mate, far)[k])

    begin([fetched(k, i) for i in range(3) for k in BOTH])
    spread = [plane_gather(here, got_v, s, gs, gr) for s in BOTH]
    lane = lax.broadcasted_iota(jnp.int32, (rows, LANES), 1).astype(F32)

    @pl.loop(0, steps)
    def _(i):
        slot = lax.rem(i, 2)
        w_copy(i, slot).wait()

        @pl.when(i + 1 < steps)
        def _():
            w_copy(i + 1, 1 - slot).start()

        @pl.when(i >= 2)
        def _():
            z_copy(i - 2, slot).wait()

        m, s, t = m_v[:], s_v[:], t_v[:]
        rel = lab_v[:] - (i * CHUNK).astype(F32)
        for n in range(0, CHUNK, FEATS):
            for which, at in enumerate((0, 3 * FEATS)):
                for stage in range(3):
                    if n == at:
                        @pl.when(i == stage + 1)
                        def _():
                            if stage == 0:
                                arrived(got_v.at[parts[which], :], xr.at[0, which])
                            spread[which][stage]()
            zz = dot(u_v[:], w_v[slot, :, n:n + FEATS])
            z_v[slot, :, n:n + FEATS] = zz
            za, zb = zz[:, :LANES], zz[:, LANES:]
            new = jnp.maximum(m, jnp.maximum(za, zb))
            s = s * jnp.exp(m - new) + (jnp.exp(za - new) + jnp.exp(zb - new))
            t = jnp.where(rel == lane + n, za, t)
            t = jnp.where(rel == lane + (n + LANES), zb, t)
            m = new
        m_v[:], s_v[:], t_v[:] = m, s, t
        z_copy(i, slot).start()

    mt = m_v[:].T
    top = jnp.max(mt, axis=0, keepdims=True)
    total = jnp.sum(s_v[:].T * jnp.exp(mt - top), axis=0, keepdims=True)
    hit = jnp.sum(t_v[:].T, axis=0, keepdims=True)
    send_v[:] = jnp.where(lax.broadcasted_iota(jnp.int32, send_v.shape, 0) == 0, top + jnp.log(total), hit)
    stats = Exchange(here, "tp", send_v, land, es.at[1], er.at[1])
    stats.start(send_v[:])
    for stage in (3, 4):
        for which in BOTH:
            spread[which][stage]()
    sums = functools.reduce(jnp.add, weights.blocks())
    rw = jnp.concatenate([wt_m[:] * (1.0 / sums[0:1, 0:1]), wt_t[:] * (MTP_LAMBDA / sums[1:2, 0:1])], axis=1)
    with jax.named_scope("statwait"):
        blocks = stats.blocks()
    top = functools.reduce(jnp.maximum, blocks)
    lse = (top + jnp.log(functools.reduce(jnp.add, [jnp.exp(b - top) for b in blocks])))[0:1, :]
    hit = functools.reduce(jnp.add, blocks)[1:2, :]
    lpart[:] = jnp.broadcast_to(jnp.sum(rw * (lse - hit)), lpart.shape)
    row = lax.broadcasted_iota(jnp.int32, st.shape[1:], 0)
    st[1] = jnp.where(row == 0, lse, jnp.where(row == 1, rw, lab))
    pack[:] = st[1]
    swaps = [remote(pack, st.at[2 * k], ps.at[k], pr.at[k], to) for k, to in enumerate((mate, far))]
    begin(swaps)
    m_v[:] = columns(lse)
    s_v[:] = columns(rw)
    skip = LEFT - (steps - 2) * CHUNK
    at = 0
    for step, start in ((steps - 1, 0), (steps - 2, skip)):
        for c in range(start, CHUNK, LANES):
            e_v[:, at:at + LANES] = grad_logits(
                z_v[step % 2, :, c:c + LANES], m_v[:], s_v[:], lab_v[:], float(step * CHUNK + c)).astype(BF16)
            at += LANES

    def e_dot(r, cols):
        return (lax.dot_general(e_v[r, :CHUNK], w_v[(steps - 1) % 2, cols, :], NT, preferred_element_type=F32)
                + lax.dot_general(e_v[r, CHUNK:], w_v[(steps - 2) % 2, cols, skip:], NT, preferred_element_type=F32))

    for i in BOTH:
        for k in BOTH:
            fetched(k, i).wait_send()
    saves = []
    for dst, r in ((uf_v, slice(0, SPREAD)), (x_v, slice(SPREAD, rows))):
        for n in range(0, depth, TASK):
            dst[:r.stop - r.start, n:n + TASK] = e_dot(r, slice(n, n + TASK))
            src = dst.at[upto(r.stop - r.start), pl.ds(n, TASK)]
            saves.append(near(src, du_out.at[pl.ds(r.start, r.stop - r.start), pl.ds(n, TASK)], sem_d.at[len(saves)]))
            saves[-1].start()
            if len(saves) in (2, 3):
                spread[len(saves) - 2][5]()
    u_copy.wait()
    waits = [spread[0][6], spread[1][6], lambda: arrived(got_v.at[rest, :], xr.at[0, 2])]
    for i, wait in enumerate(waits):
        start = i * (SPREAD // 2)
        r = pl.ds(start, min(SPREAD // 2, rows - start))
        with jax.named_scope("land"):
            wait()

        @pl.loop(start // LANES, (start + r.size) // LANES)
        def _(j):
            part = ds(j * LANES, LANES)
            u_v[part, :] = got_v[part, :].astype(BF16)

        saves.append(near(u_v.at[r, :], up_out.at[r, :], sem_k.at[i]))
        saves[-1].start()
    for c in swaps:
        c.wait()
    for i in range(3):
        arrived(far_u.at[parts[i], :], xr.at[1, i])
    weights.drain()
    stats.drain()
    for k in BOTH:
        spread[k][7]()
        fetched(k, 2).wait_send()
        z_copy(steps - 2 + k, (steps + k) % 2).wait()
    for c in saves:
        c.wait()


def logits(hm, ht, gain_m, gain_t, lab_m, lab_t, wt_m, wt_t, w):
    seq, depth = hm.shape
    rows, vocab = 2 * seq, w.shape[1]
    n_tp, n_dp = lax.axis_size("tp"), lax.axis_size("dp")
    shape = jax.ShapeDtypeStruct
    stat = pltpu.VMEM((rows, LANES), F32)
    return pl.pallas_call(
        logits_kernel,
        out_shape=(shape((rows, vocab), F32), shape((rows, depth), BF16), shape((rows, depth), BF16), shape((rows, depth), F32),
                   shape((rows, depth), F32), shape((3, 8, rows), F32), shape((8, LANES), F32)),
        in_specs=[ANY, ANY] + [VMEM] * 6 + [ANY],
        out_specs=(ANY,) * 5 + (VMEM, VMEM),
        scratch_shapes=[
            pltpu.VMEM((rows, depth), BF16), pltpu.VMEM((rows, depth), BF16), pltpu.VMEM((rows, depth), F32), pltpu.VMEM((rows, depth), F32),
            pltpu.VMEM((2, depth, CHUNK), BF16), pltpu.VMEM((2, rows, CHUNK), F32), pltpu.VMEM((rows, vocab - LEFT), BF16),
            pltpu.VMEM((rows - SPREAD, depth), F32), stat, stat, stat, stat,
            pltpu.VMEM((2, rows), F32), pltpu.VMEM((n_tp, 2, rows), F32), pltpu.VMEM((8, LANES), F32), pltpu.VMEM((n_dp, 8, LANES), F32),
            pltpu.VMEM((8, rows), F32),
            TWO, DMA, TWO, TWO, DMA((2 * depth // TASK,)), DMA((3,)), TWO, TWO, TWO, TWO,
            TWO, DMA((2, 3, 2)), *[DMA((2, 3))] * 2,
        ],
        compiler_params=pltpu.CompilerParams(vmem_limit_bytes=VMEM_LIMIT, collective_id=0, has_side_effects=True),
        name="logits",
    )(hm, ht, gain_m, gain_t, lab_m, lab_t, wt_m, wt_t, w)


def chunk_table():
    out, at, used = [], 0, [0, 0]
    for i, kind in enumerate(KINDS):
        width, swapped = (WIDE if i else FIRST), int(kind == "s")
        out.append((at, width, swapped, used[swapped]))
        at, used[swapped] = at + width, used[swapped] + width
    return out, used


def column(here, used, swapped, other, offset):
    base = [2 * used[0] * s + abs(here.side(s) - other) * used[s] for s in BOTH]
    return jnp.where(swapped == 1, base[1], base[0]) + offset


def pick(values, k):
    if isinstance(k, int):
        return values[k]
    return functools.reduce(lambda out, i: jnp.where(k == i, values[i], out), range(1, len(values)), jnp.int32(values[0]))


def head_kernel(hm, ht, gain_m, gain_t, u_own, u_par, far_in, z, w, st, du_in, lpart,
                fin, gh, ghb, du, far_u, one, tot, u_v, w_v, z_v, et_v, g_v, own_v, sum_v, one_v, acc_v,
                lse_v, rw_v, lab_v, ra_v, rl_v, rb_v, rm_v, ra2_v, rb2_v, rh_v, gg_v, gland, tland, tsend,
                sem_u, sem_w, sem_z, sem_a, sem_o, sem_1, d_send, d_recv, b_send, b_recv, f_send, f_recv,
                gs, gr, ss, sr, sem_l, sem_x, es, er):
    del far_in
    rows, depth = u_own.shape
    seq = rows // 2
    here = Torus()
    x, core = here.x, here.core
    met = here.greet()
    table, used = chunk_table()
    starts, _, swaps, offsets = (list(t) for t in zip(*table))
    last = len(table) - 1

    def span(k):
        return upto(FIRST) if isinstance(k, int) and k == 0 else ds(FIRST + (k - 1) * WIDE, WIDE, LANES)

    def chips(k):
        s = pick(swaps, k) == 1
        return jnp.where(s, here.far, here.mate), jnp.where(s, here.mate, here.far)

    def block(i):
        return ds((2 * lax.rem(i, RING) + jnp.where(i < RING, 1 - core, core)) * FEATS, FEATS, FEATS)

    def feats(i):
        return pl.ds(i * FEATS, FEATS)

    def w_copies(col, width, slot):
        return [near(w.at[block(i), ds(col, width, LANES)], w_v.at[slot, feats(i), upto(width)], sem_w.at[slot]) for i in range(2 * RING)]

    def u_copies(k):
        src, r = ((u_par, upto(rows)), (u_own, pl.ds(rows, rows)))[k]
        return [near(src.at[:, block(i)], u_v.at[r, feats(i)], sem_u.at[k]) for i in range(2 * RING)]

    def u_wait(k):
        arrived(u_v.at[upto(rows), :], sem_u.at[k])

    def fetch(k, slot):
        width = span(k).size
        col = column(here, used, pick(swaps, k), 0, pick(offsets, k))
        begin(w_copies(col, width, slot) + [near(z.at[:, ds(col, width, LANES)], z_v.at[slot, :, upto(width)], sem_z.at[slot])])

    per = LEFT // TASK

    def piece(t):
        return t < 2 * per, t // per, lax.rem(t, per)

    def acc_copies(h, back):
        refs = [(acc_v.at[:, feats(i)], (du if back else du_in).at[ds(h * seq, seq), block(i)]) for i in range(2 * RING)]
        return [near(*(p if back else p[::-1]), sem_a) for p in refs]

    def task_fetch(t, slot):
        of_du, h, i = piece(t)

        @pl.when(of_du)
        def _():
            begin(w_copies(i * TASK, TASK, slot))
            near(z.at[ds(h * seq, seq), ds(i * TASK, TASK, LANES)], z_v.at[slot, upto(seq), :], sem_z.at[slot]).start()

        @pl.when(~of_du)
        def _():
            begin([near(far_u.at[:, block(2 * i + j)], z_v.at[slot, :, feats(j)], sem_z.at[slot]) for j in BOTH])

    def task(t, slot):
        of_du, h, i = piece(t)

        @pl.when(~of_du)
        def _():
            arrived(z_v.at[slot], sem_z.at[slot])
            u_v[pl.ds(2 * rows, rows), ds(i * TASK, TASK, LANES)] = z_v[slot].astype(BF16)

        @pl.when(of_du)
        def _():
            arrived(w_v.at[slot], sem_w.at[slot])
            arrived(z_v.at[slot, upto(seq), :], sem_z.at[slot])

            @pl.when(i == 0)
            def _():
                arrived(acc_v, sem_a)

            r = ds(rows + h * seq, seq)
            col = (i * TASK).astype(F32)
            for g in range(0, TASK, LANES):
                cols = slice(g, g + LANES)
                et_v[:, cols] = grad_logits(z_v[slot, :seq, cols], lse_v[r, :], rw_v[r, :], lab_v[r, :], col + g).astype(BF16)
            for m in range(0, depth, TASK):
                cols = slice(m, m + TASK)
                acc_v[:, cols] += lax.dot_general(et_v[:, :TASK], w_v[slot, cols, :], NT, preferred_element_type=F32)

            @pl.when(i == per - 1)
            def _():
                acc_v[:] = acc_v[:].astype(BF16).astype(F32)
                begin(acc_copies(h, True))
                arrived(acc_v, sem_a)

            @pl.when((i == per - 1) & (h == 0))
            def _():
                begin(acc_copies(1, False))

    def d_copy(k, part):
        lanes, width = pl.ds(part * TASK, TASK), span(k).size
        return remote(g_v.at[upto(width), lanes], sum_v.at[span(k), lanes], d_send, d_recv.at[k], here.chip(x, 1 - core))

    def b_copy(k, which):
        to = chips(k)[1]
        block_of = ds(jnp.where(which == 0, here.opposite, to) * FEATS, FEATS, FEATS)
        return remote(sum_v.at[span(k), block_of], one.at[which, span(k), :], b_send, b_recv.at[k, which], here.chip(to))

    def f_copy(k):
        mate = chips(k)[0]
        return remote(sum_v.at[span(k), ds(mate * FEATS, FEATS, FEATS)], fin.at[1, span(k), :], f_send, f_recv, here.chip(mate))

    def o_copy(k):
        return near(sum_v.at[span(k), ds(x * FEATS, FEATS, FEATS)], fin.at[0, span(k), :], sem_o)

    def make(k, slot, late=lambda: None, middle=lambda: None):
        width = span(k).size
        swapped = pick(swaps, k)
        col = column(here, used, swapped, 0, pick(offsets, k)).astype(F32)
        arrived(w_v.at[slot, :, upto(width)], sem_w.at[slot])
        arrived(z_v.at[slot, :, upto(width)], sem_z.at[slot])

        def put(zz, r, c, at):
            e = grad_logits(zz, lse_v[r, :], rw_v[r, :], lab_v[r, :], col + c)
            et_v[c:c + LANES, ds(at, rows, rows)] = e.T.astype(BF16)

        for c in range(0, width, LANES):
            put(z_v[slot, :, c:c + LANES], pl.ds(rows, rows), c, rows * (1 - swapped))
        late()
        other = ds(2 * rows * swapped, rows, rows)
        for n in range(0, width, FEATS):
            step = min(width - n, FEATS)
            zz = dot(u_v[other, :], w_v[slot, :, n:n + step])
            for c in range(0, step, LANES):
                put(zz[:, c:c + LANES], other, n + c, rows * swapped)
        middle()
        both = ds(rows * swapped, 2 * rows, rows)
        et = et_v[upto(width), :]
        for part in BOTH:
            lanes = pl.ds(part * TASK, TASK)
            g_v[upto(width), lanes] = dot(et, u_v[both, lanes])
            d_copy(k, part).start()
        own_v[upto(width), :] = dot(et, u_v[both, pl.ds(2 * TASK, 2 * TASK)])

    def add(k):
        arrived(sum_v.at[span(k), :], d_recv.at[k])
        sum_v[span(k), :] += own_v[upto(span(k).size), :]
        begin([b_copy(k, which) for which in BOTH])

    def landing(k, which):
        return near(one.at[which, span(k), :], one_v.at[which, upto(span(k).size), :], sem_1.at[which])

    def land(k, which):
        with jax.named_scope("bwait"):
            arrived(one.at[which, span(k), :], b_recv.at[k, which])
        landing(k, which).start()

    def close(k, which):
        landing(k, which).wait()
        chip = jnp.where(which == 0, chips(k)[0], x)
        sum_v[span(k), ds(chip * FEATS, FEATS, FEATS)] += one_v[which, upto(span(k).size), :]
        (o_copy if which else f_copy)(k).start()

    def ring(h, s):
        q = 2 * h + s
        p1, to1, p2, to2 = here.rings(s)
        big, small = seq // 2 // RING, seq // 2 // RING // RING
        base = h * seq + s * (seq // 2)
        one_of = lambda o: ds(base + mod(p1 + o) * big, big)
        two_of = lambda o: ds(base + p1 * big + mod(p2 + o) * small, small)
        sub = lambda o: ds(mod(p2 + o) * small, small)
        every = upto(depth)
        first = Scatter(du, one_of, to1, ra_v.at[q], rb_v.at[q], ss.at[q], sr.at[q, 0])
        second = Scatter(rm_v.at[q], sub, to2, ra2_v.at[q], rb2_v.at[q], ss.at[q], sr.at[q, 1])
        down = Gather(gh, two_of, every, to2, ss.at[q], sr.at[q, 2], rm_v.at[q, sub(0), :])
        up = Gather(gh, one_of, every, to1, ss.at[q], sr.at[q, 3])
        lanes = halves(depth)
        h_rows = ds(s * (seq // 2) + p1 * big + p2 * small, small)
        loads = lambda: [near(du.at[one_of(WAYS[i]), lanes[i]], rl_v.at[s, i], sem_l.at[s, i]) for i in BOTH] + [
            near(du.at[one_of(0), :], rm_v.at[q], sem_l.at[s, 2]), near((hm, ht)[h].at[h_rows, :], rh_v.at[q], sem_l.at[s, 3])]
        keep = lambda: near(rm_v.at[q, sub(0), :], gh.at[two_of(0), :], sem_x.at[q])
        return q, sub, lanes, first, second, down, up, loads, keep

    def event(h, stage):
        for s in BOTH:
            q, sub, lanes, first, second, down, up, loads, keep = ring(h, s)
            if stage == 0:
                first.start()
                begin(loads())
            if stage == 1:
                for c in loads():
                    c.wait()
                first.middle(lambda i, d: rl_v[s, i])
            if stage == 2:
                first.end()
                rm_v[q] += rb_v[q, 0] + rb_v[q, 1]
                second.start()
                second.rest()
            if stage == 3:
                second.middle(lambda i, d: rm_v[q, sub(d), lanes[i]])
            if stage == 4:
                second.end()
                gu = rm_v[q, sub(0), :] + (rb2_v[q, 0] + rb2_v[q, 1])
                xr = rh_v[q].astype(F32)
                inv = lax.rsqrt(jnp.mean(xr * xr, axis=-1, keepdims=True) + NORM_EPS)
                normed = xr * inv
                gn = gu * (gain_m, gain_t)[h][:]
                gx = inv * (gn - normed * jnp.mean(gn * normed, axis=-1, keepdims=True))
                rm_v[q, sub(0), :] = gx.astype(BF16).astype(F32)
                part = jnp.sum(gu * normed, axis=0, keepdims=True)
                gg_v[pl.ds(h, 1), :] = part if s == 0 else gg_v[pl.ds(h, 1), :] + part
                keep().start()
                down.spread()
            if stage == 5:
                down.pass_on()
            if stage == 6:
                keep().wait()
                down.end()
                up.spread()
            if stage == 7:
                up.pass_on()
            if stage == 8:
                up.end()

    def rest(h):
        for s in BOTH:
            ring(h, s)[3].rest()

    plane = Exchange(here, "tp", gg_v, gland, es.at[0], er.at[0])
    line = Exchange(here, "dp", tsend, tland, es.at[1], er.at[1])

    def sums(stage):
        if stage == 0:
            plane.start(gg_v[:])
        if stage == 1:
            total = functools.reduce(jnp.add, plane.blocks())
            tsend[:] = jnp.concatenate([total, jnp.broadcast_to(lpart[0:1, 0:1], total.shape)])
            line.start(tsend[:])
        if stage == 2:
            tot[:] = functools.reduce(jnp.add, line.blocks())

    def narrow(h):
        r = ds(h * seq, seq)
        c = near(gh.at[r, :], acc_v, sem_a)
        c.start()
        c.wait()
        u_v[r, :] = acc_v[:].astype(BF16)
        near(u_v.at[r, :], ghb.at[r, :], sem_x.at[h]).start()

    far_steps = [plane_gather(here, far_u, s, gs, gr) for s in BOTH]

    def far_event(stage):
        for s in BOTH:
            for i in ((stage - 1,), (2, 3), (4, 5), (6,))[max(stage - 2, 0)]:
                far_steps[s][i]()

    def drain():
        rows_sent = 6 * (seq // 2 // RING + seq // 2 // RING // RING)
        for q in range(4):
            arrived(du.at[upto(rows_sent), :], ss.at[q])
        for s in BOTH:
            far_steps[s][7]()
        plane.drain()
        line.drain()
        arrived(sum_v.at[:, upto(2 * FEATS)], b_send)
        arrived(g_v, d_send)

    def both(act):
        return lambda k: [act(k, which) for which in BOTH]

    verbs = {"r": event, "u": rest, "g": sums, "n": narrow, "f": far_event, "a": add, "L": both(land), "C": both(close), "p": land, "q": close, "z": drain}

    def run(text):
        for word in text.split(","):
            with jax.named_scope(word):
                verbs[word[0]](*(int(c) for c in word[1:]))

    def at_point(k, point):
        for at, text in (a.split(":") for a in ACTS):
            if at[-1] == point:
                @pl.when(k == int(at[:-1]))
                def _():
                    run(text)

    fetch(0, 0)
    begin(u_copies(0))

    def spread_stats(k):
        for i, ref in enumerate((lse_v, rw_v, lab_v)):
            ref[pl.ds(k * rows, rows), :] = columns(st[k, i:i + 1, :])

    spread_stats(1)

    def before_other():
        spread_stats(0)
        u_wait(0)
        begin(u_copies(1))

    def before_sends():
        u_wait(1)
        fetch(1, 1)
        begin(acc_copies(0, False))
        with jax.named_scope("meet"):
            met()
        far_event(1)

    with jax.named_scope("make0"):
        make(0, 0, before_other, before_sends)
    spread_stats(2)
    add(0)

    @pl.loop(1, last + 1)
    def _(k):
        lo, hi = pick(DONE[:1] + DONE[:-1], k), pick(DONE, k)
        slot = lax.rem(k + lo, 2)

        def more(t):
            @pl.when(t < hi)
            def _():
                task_fetch(t, lax.rem(k + 1 + t, 2))

            @pl.when((t == hi) & (k < last))
            def _():
                fetch(k + 1, lax.rem(k + 1 + t, 2))

        more(lo)

        def middle():
            at_point(k, "m")

            @pl.when(k == 1)
            def _():
                arrived(g_v.at[upto(FIRST), :], d_send)

            @pl.when(k > 1)
            def _():
                arrived(g_v, d_send)

        with jax.named_scope("make"):
            make(k, slot, middle=middle)

        at_point(k, "a")

        @pl.loop(lo, hi)
        def _(t):
            at_point(t, "t")
            more(t + 1)
            with jax.named_scope("task"):
                task(t, lax.rem(k + 1 + t, 2))

        at_point(k, "d")

    for text in TAIL:
        run(text)
    with jax.named_scope("tail"):
        arrived(fin.at[1], f_send)
        arrived(fin.at[1], f_recv)
        arrived(fin.at[0], sem_o)
        for h in BOTH:
            arrived(ghb.at[upto(seq), :], sem_x.at[h])


def head_grad(hm, ht, gain_m, gain_t, u_own, u_par, far_u, z, w, st, du_in, lpart):
    rows, depth = u_own.shape
    seq = rows // 2
    half = z.shape[1] // 2
    n_tp, n_dp, n = lax.axis_size("tp"), lax.axis_size("dp"), len(KINDS)
    big, small = seq // 2 // RING, seq // 2 // RING // RING
    shape = jax.ShapeDtypeStruct
    stat = pltpu.VMEM((3 * rows, LANES), F32)
    return pl.pallas_call(
        head_kernel,
        out_shape=(shape((2, half, FEATS), F32), shape((rows, depth), F32), shape((rows, depth), BF16), shape((rows, depth), F32),
                   shape((rows, depth), F32), shape((2, half, FEATS), F32), shape((4, depth), F32)),
        in_specs=[ANY, ANY, VMEM, VMEM] + [ANY] * 5 + [VMEM, ANY, VMEM],
        out_specs=(ANY,) * 6 + (VMEM,),
        scratch_shapes=[
            pltpu.VMEM((3 * rows, depth), BF16), pltpu.VMEM((2, depth, TASK), BF16), pltpu.VMEM((2, rows, TASK), F32),
            pltpu.VMEM((TASK, 2 * rows), BF16), pltpu.VMEM((WIDE, 2 * TASK), F32), pltpu.VMEM((WIDE, 2 * TASK), F32),
            pltpu.VMEM((half, 2 * TASK), F32), pltpu.VMEM((2, WIDE, FEATS), F32), pltpu.VMEM((seq, depth), F32),
            stat, stat, stat,
            pltpu.VMEM((4, 2, big, depth // 2), F32), pltpu.VMEM((2, 2, big, depth // 2), F32), pltpu.VMEM((4, 2, big, depth), F32),
            pltpu.VMEM((4, big, depth), F32), pltpu.VMEM((4, 2, small, depth // 2), F32), pltpu.VMEM((4, 2, small, depth), F32),
            pltpu.VMEM((4, small, depth), BF16),
            pltpu.VMEM((2, depth), F32), pltpu.VMEM((n_tp, 2, depth), F32), pltpu.VMEM((n_dp, 4, depth), F32), pltpu.VMEM((4, depth), F32),
            TWO, TWO, TWO, DMA, DMA, TWO, DMA, DMA((n,)), DMA, DMA((n, 2)), DMA, DMA,
            TWO, DMA((2, 3, 2)), DMA((4,)), DMA((4, 4, 2)), DMA((2, 4)), DMA((4,)), TWO, TWO,
        ],
        input_output_aliases={6: 4},
        compiler_params=pltpu.CompilerParams(vmem_limit_bytes=VMEM_LIMIT, collective_id=1, has_side_effects=True),
        name="head_grad",
    )(hm, ht, gain_m, gain_t, u_own, u_par, far_u, z, w, st, du_in, lpart)


def finish_kernel(fin, gh, tot, out, gm, gt, loss, ggm, ggt, f_v, o_v, g_v, sem_f, sem_o, sem_g):
    seq = gm.shape[0]
    table, used = chunk_table()
    jobs = [(k, *t) for t in table for k in BOTH]
    here = Torus()

    def f_in(i):
        k, at, width, _, _ = jobs[i]
        return near(fin.at[k, pl.ds(at, width), :], f_v.at[k, pl.ds(at, width), :], sem_f.at[i])

    def f_out(i):
        k, at, width, swapped, offset = jobs[i]
        return near(o_v.at[k, :, pl.ds(at, width)], out.at[:, ds(column(here, used, swapped, k, offset), width, LANES)], sem_o.at[i])

    g_in = [near(gh.at[pl.ds(h * seq, seq), :], g_v.at[h], sem_g.at[h]) for h in BOTH]
    begin(g_in + [f_in(i) for i in range(WINDOW)])
    ggm[:], ggt[:], loss[:] = tot[0:1, :], tot[1:2, :], tot[2:3, 0:1]
    outs = [f_out(i) for i in range(len(jobs))] + [near(g_v.at[h], (gm, gt)[h], sem_g.at[h]) for h in BOTH]
    for i, (k, at, width, _, _) in enumerate(jobs):
        begin([f_in(i + WINDOW)] if i + WINDOW < len(jobs) else [])
        if i < 2:
            g_in[i].wait()
            outs[i - 2].start()
        f_in(i).wait()
        o_v[k, :, pl.ds(at, width)] = f_v[k, pl.ds(at, width), :].T
        outs[i].start()
    for c in outs:
        c.wait()


def finish(fin, gh, tot):
    _, half, block = fin.shape
    seq, depth = gh.shape[0] // 2, gh.shape[1]
    shape, row, jobs = jax.ShapeDtypeStruct, jax.ShapeDtypeStruct((1, depth), F32), DMA((2 * len(KINDS),))
    return pl.pallas_call(
        finish_kernel,
        out_shape=(shape((block, 2 * half), F32), shape((seq, depth), BF16), shape((seq, depth), BF16), shape((1, 1), F32), row, row),
        in_specs=[ANY, ANY, VMEM],
        out_specs=(ANY, ANY, ANY, VMEM, VMEM, VMEM),
        scratch_shapes=[pltpu.VMEM((2, half, block), F32), pltpu.VMEM((2, block, half), F32), pltpu.VMEM((2, seq, depth), BF16), jobs, jobs, TWO],
        compiler_params=pltpu.CompilerParams(vmem_limit_bytes=VMEM_LIMIT),
        name="finish",
    )(fin, gh, tot)


def solution(mesh):
    def local_step(h_main, h_mtp, labels_main, labels_mtp, weight_main, weight_mtp, gain_final, gain_mtp, w_out):
        hm, ht, gm, gt = h_main[0], h_mtp[0], gain_final[None], gain_mtp[None]
        z, u_own, u_par, far_u, du_in, st, lpart = logits(hm, ht, gm, gt, labels_main, labels_mtp, weight_main, weight_mtp, w_out)
        fin, _, gh, _, _, _, tot = head_grad(hm, ht, gm, gt, u_own, u_par, far_u, z, w_out, st, du_in, lpart)
        grad_w, gh_m, gh_t, loss, gg_m, gg_t = finish(fin, gh, tot)
        return loss[0, 0], gh_m[None], gh_t[None], grad_w, gg_m[0], gg_t[0]

    wide, row = P("dp", None, None), P("dp", None)
    return jax.shard_map(
        local_step,
        mesh=mesh,
        in_specs=(wide, wide, row, row, row, row, P(None), P(None), P(None, "tp")),
        out_specs=(P(), wide, wide, P("dp", "tp"), P(None), P(None)),
        check_vma=False,
    )
```
